32 devices in a mesh: seq: 4 (over y, x), ctx: 4 (over z), mp: 2 (over core).
Axes of the slice: x: 2, y: 2, z: 4, core: 2. Of those that a mesh axis runs over, the one named last changes fastest.
Arguments:
- tokens: bfloat16 [4, 512, 2048], P('seq', 'ctx'), may hold values from -5.75 to 6.25
- positions: int32 [4, 512], P('seq', 'ctx'), may hold values from 0 to 255, as said below
- routes: int32 [4, 512, 8], P('seq', 'ctx'), may hold values from 0 to 15, as said below
- cotangent: bfloat16 [4, 512, 2048], P('seq', 'ctx'), may hold values from -6 to 6
- attention_gain: bfloat16 [2048], P(('seq', 'ctx')), may hold values from 0.099609375 to 1.8984375
- query_weight: bfloat16 [2048, 2048], P(('seq', 'ctx'), 'mp'), may hold values from -0.125 to 0.125
- key_weight: bfloat16 [2048, 2048], P(('seq', 'ctx'), 'mp'), may hold values from -0.125 to 0.125
- value_weight: bfloat16 [2048, 2048], P(('seq', 'ctx'), 'mp'), may hold values from -0.125 to 0.125
- query_gain: bfloat16 [16, 128], P('mp', ('seq', 'ctx')), may hold values from 0.59765625 to 2
- key_gain: bfloat16 [16, 128], P('mp', ('seq', 'ctx')), may hold values from 0.59765625 to 2
- output_weight: bfloat16 [2048, 2048], P('mp', ('seq', 'ctx')), may hold values from -0.5 to 0.5
- ffn_gain: bfloat16 [2048], P(('seq', 'ctx')), may hold values from 0.099609375 to 1.8984375
- router_weight: bfloat16 [2048, 16], P(('seq', 'ctx')), may hold values from -0.093830323 to 0.06629126
- gate_weight: bfloat16 [16, 2048, 1024], P(('seq', 'ctx'), None, 'mp'), may hold values from -0.125 to 0.125
- up_weight: bfloat16 [16, 2048, 1024], P(('seq', 'ctx'), None, 'mp'), may hold values from -0.125 to 0.125
- down_weight: bfloat16 [16, 1024, 2048], P(('seq', 'ctx'), 'mp'), may hold values from -1.5 to 1.5
Outputs:
- layer_output: bfloat16 [4, 512, 2048], P('seq', 'ctx')
- tokens_grad: float32 [4, 512, 2048], P('seq', 'ctx')
- attention_gain_grad: float32 [2048], P(('seq', 'ctx'))
- query_weight_grad: float32 [2048, 2048], P(('seq', 'ctx'), 'mp')
- key_weight_grad: float32 [2048, 2048], P(('seq', 'ctx'), 'mp')
- value_weight_grad: float32 [2048, 2048], P(('seq', 'ctx'), 'mp')
- query_gain_grad: float32 [16, 128], P('mp', ('seq', 'ctx'))
- key_gain_grad: float32 [16, 128], P('mp', ('seq', 'ctx'))
- output_weight_grad: float32 [2048, 2048], P('mp', ('seq', 'ctx'))
- ffn_gain_grad: float32 [2048], P(('seq', 'ctx'))
- router_weight_grad: float32 [2048, 16], P(('seq', 'ctx'))
- gate_weight_grad: float32 [16, 2048, 1024], P(('seq', 'ctx'), None, 'mp')
- up_weight_grad: float32 [16, 2048, 1024], P(('seq', 'ctx'), None, 'mp')
- down_weight_grad: float32 [16, 1024, 2048], P(('seq', 'ctx'), 'mp')
The draws below stay inside these ranges and needn't reach their ends.
Inputs may be any that keep to these rules, and one draw needn't show every extreme that they name: `positions`: within each sequence a position counts up by one from the previous token, or restarts at 0 where a packed document begins. Documents begin at the first token and at token 256, and nowhere else in the first half of a sequence. `routes`: each token names 8 different experts. Among the 1024 choices of one sequence block (one device's rows), no expert is named more than 96 times.
All inputs are finite; a program needn't handle non-finite values.
Results may differ from the reference program's by a relative error of at most 0.02.
Values may be sent and summed in bfloat16 or wider, within the bound.
A program may use at most 256 MiB of HBM per device.

```python
import math
import jax
import jax.numpy as jnp
from jax import lax

D = 2048
HEADS = 16
HEAD_DIM = 128
FF = 1024
TOP = 8
EXPERTS = 16
TOK_DEV = 128
SEQ_LEN = 512
SEQS = 4
HQ = 2048
CAP = 96
N_SEQ = 4
N_CTX = 4


def draw_positions(key, part):
    index = jnp.arange(SEQ_LEN, dtype=jnp.int32)
    half_len = SEQ_LEN // 2
    starts = jax.random.randint(key, (SEQS, SEQ_LEN), 0, 256)
    starts = jnp.where(index[None, :] < half_len, 1, starts)
    starts = jnp.where(index[None, :] % half_len == 0, 0, starts)
    marks = jnp.where(starts == 0, index[None, :], 0).astype(jnp.int32)
    begin = lax.cummax(marks, axis=1)
    return (index[None, :] - begin).astype(jnp.int32)


def draw_tokens(key, part):
    base_key = jax.random.fold_in(key, 5)
    noise_part = jnp.clip(jax.random.normal(base_key, (SEQS, SEQ_LEN, D), jnp.float32), -6.0, 6.0)
    return (noise_part + 0.25).astype(jnp.bfloat16)


def draw_router_weight(key, part):
    base_key = jax.random.fold_in(key, 11)
    key_noise, key_pick, key_depth = jax.random.split(base_key, 3)
    spread = (4.0 * D) ** (-0.5)
    noise_part = jnp.clip(jax.random.normal(key_noise, (D, EXPERTS), jnp.float32), -6.0, 6.0)
    expert_order = jax.random.permutation(key_pick, EXPERTS)
    lowered = expert_order < max(1, EXPERTS // 8)
    depth_scale = jax.random.uniform(key_depth, (EXPERTS,), jnp.float32, 0.8, 1.2)
    offset = jnp.where(lowered, -47.0 / D, 0.0) * depth_scale
    return (noise_part * spread + offset[None, :]).astype(jnp.bfloat16)


def draw_routes(key, part):
    blocks = SEQS * SEQ_LEN // TOK_DEV
    block_keys = jax.random.split(jax.random.fold_in(key, 23), blocks)
    slots_all = EXPERTS * CAP

    def one_block(block_key):
        key_order, key_heavy, key_pool, key_rows, key_turn = jax.random.split(block_key, 5)
        expert_order = jax.random.permutation(key_order, EXPERTS).astype(jnp.int32)
        heavy_count = jax.random.randint(key_heavy, (), max(1, EXPERTS // 8), EXPERTS // 4 + 1)
        slot_index = jnp.arange(slots_all, dtype=jnp.int32)
        slot_rank = slot_index // CAP
        shuffle = jax.random.permutation(key_pool, slots_all).astype(jnp.int32)
        slot_score = jnp.where(slot_rank < heavy_count, slot_index, slots_all + shuffle)
        picked = jnp.sort(jnp.argsort(slot_score, stable=True)[:TOK_DEV * TOP]).astype(jnp.int32)
        listed = expert_order[picked // CAP]
        choice_table = listed.reshape(TOP, TOK_DEV).T
        rows_order = jax.random.permutation(key_rows, TOK_DEV)
        choice_table = choice_table[rows_order]
        turn_score = jax.random.randint(key_turn, (TOK_DEV, TOP), 0, 1 << 20) * TOP + jnp.arange(TOP, dtype=jnp.int32)[None, :]
        turn_order = jnp.argsort(turn_score, axis=1, stable=True)
        return jnp.take_along_axis(choice_table, turn_order, axis=1)
    return jax.vmap(one_block)(block_keys).reshape(SEQS, SEQ_LEN, TOP).astype(jnp.int32)


def steps_of(key, extent, shards, low, largest):
    def one(axis_at, blocks):
        heights = jax.random.uniform(jax.random.fold_in(jax.random.fold_in(key, 6), axis_at), (blocks,), jnp.float32, low / len(shards), largest / len(shards))
        return jnp.repeat(jnp.exp(heights), extent[axis_at] // blocks).reshape((-1,) + (1,) * (len(extent) - axis_at - 1))

    level = one(*shards[0])
    for cut in shards[1:]:
        level = level * one(*cut)
    return level


def normal_values(stream_key, extent, scale, reach, cuts=(), kind=jnp.bfloat16):
    values = jax.random.normal(stream_key, extent, jnp.float32) * scale
    if len(cuts) > 0:
        values = steps_of(stream_key, extent, cuts, -0.22, 0.18) * values
    return jnp.clip(values, min=-reach, max=reach).astype(kind)


def setup_inputs(seed: int = 0) -> dict:
    key_of = jax.random.split(jax.random.key(seed), 17)
    return {
        "tokens": draw_tokens(jax.random.fold_in(key_of[16], 71), 0),
        "positions": draw_positions(jax.random.fold_in(key_of[16], 71), 0),
        "routes": draw_routes(jax.random.fold_in(key_of[16], 71), 0),
        "cotangent": normal_values(key_of[3], (SEQS, SEQ_LEN, D), 1.0, 6.0, ((0, 4), (1, 4))),
        "attention_gain": jnp.clip(1.0 + 0.18 * jax.random.normal(key_of[4], (D,), jnp.float32), 0.099609375, 1.8984375).astype(jnp.bfloat16),
        "query_weight": normal_values(key_of[5], (D, HQ), D ** -0.5, 0.125, ((0, 16), (1, 2))),
        "key_weight": normal_values(key_of[6], (D, HQ), D ** -0.5, 0.125, ((0, 16), (1, 2))),
        "value_weight": normal_values(key_of[7], (D, HQ), D ** -0.5, 0.125, ((0, 16), (1, 2))),
        "query_gain": jnp.clip(jnp.exp(math.log(2.0) - 1.2078867 * jax.random.uniform(key_of[8], (HEADS, HEAD_DIM), jnp.float32) ** steps_of(key_of[8], (HEADS, HEAD_DIM), ((0, 2), (1, 16)), -0.2, 0.2)), 0.59765625, 2.0).astype(jnp.bfloat16),
        "key_gain": jnp.clip(jnp.exp(math.log(2.0) - 1.2078867 * jax.random.uniform(key_of[9], (HEADS, HEAD_DIM), jnp.float32) ** steps_of(key_of[9], (HEADS, HEAD_DIM), ((0, 2), (1, 16)), -0.2, 0.2)), 0.59765625, 2.0).astype(jnp.bfloat16),
        "output_weight": normal_values(key_of[10], (HQ, D), (HQ // 16) ** -0.5, 0.5, ((0, 2), (1, 16))),
        "ffn_gain": jnp.clip(1.0 + 0.18 * jax.random.normal(key_of[11], (D,), jnp.float32), 0.099609375, 1.8984375).astype(jnp.bfloat16),
        "router_weight": draw_router_weight(jax.random.fold_in(key_of[16], 71), 0),
        "gate_weight": normal_values(key_of[13], (EXPERTS, D, FF), D ** -0.5, 0.125, ((0, 16), (2, 2))),
        "up_weight": normal_values(key_of[14], (EXPERTS, D, FF), D ** -0.5, 0.125, ((0, 16), (2, 2))),
        "down_weight": normal_values(key_of[15], (EXPERTS, FF, D), (FF // 64) ** -0.5, 1.5, ((0, 16), (1, 2))),
    }


eps = 1e-05
neg_big = -1e+30

def to_half(values):
    return lax.optimization_barrier(values.astype(jnp.bfloat16))

def rms_scale(rows, gain):
    return rows * lax.rsqrt(lax.optimization_barrier(jnp.mean(rows * rows, axis=-1, keepdims=True)) + eps) * gain

def rope_tables(positions):
    half = HEAD_DIM // 2
    freq = 10000.0 ** (-(jnp.arange(half).astype(jnp.float32) * 2.0 / HEAD_DIM))
    angle = positions.astype(jnp.float32)[:, None] * freq[None, :]
    return (jnp.cos(angle), jnp.sin(angle))

def head_prepare(proj, gain, cosine, sine, factor):
    count = proj.shape[0]
    heads = gain.shape[0]
    width = gain.shape[1]
    unit = proj * lax.rsqrt(lax.optimization_barrier(jnp.mean(proj * proj, axis=-1, keepdims=True)) + eps)
    normed = unit.reshape(count, heads, width) * gain
    first = normed[..., :width // 2]
    second = normed[..., width // 2:]
    cos_rows = cosine[:, None, :]
    sin_rows = sine[:, None, :]
    turned = jnp.concatenate([first * cos_rows - second * sin_rows, second * cos_rows + first * sin_rows], axis=-1)
    return (turned * factor).reshape(count, heads * width)

def attend_sequence(parts):
    query, keys, values = parts
    query3 = query.astype(jnp.float32).reshape(SEQ_LEN, HEADS, HEAD_DIM)
    keys3 = keys.astype(jnp.float32).reshape(SEQ_LEN, HEADS, HEAD_DIM)
    values3 = values.astype(jnp.float32).reshape(SEQ_LEN, HEADS, HEAD_DIM)
    block = min(512, SEQ_LEN)
    count = SEQ_LEN // block
    key_index = jnp.arange(SEQ_LEN, dtype=jnp.int32)

    def one_block(index):
        start = (index * block).astype(jnp.int32)
        query_block = lax.dynamic_slice_in_dim(query3, start, block, 0)
        scores = jnp.einsum('qhd,khd->hqk', query_block, keys3)
        allowed = key_index[None, :] <= (start + jnp.arange(block, dtype=jnp.int32))[:, None]
        scores = jnp.where(allowed[None], scores, neg_big)
        top = lax.optimization_barrier(jnp.max(scores, axis=-1))
        weights = jnp.where(allowed[None], jnp.exp(scores - top[..., None]), 0.0)
        total = lax.optimization_barrier(jnp.sum(weights, axis=-1))
        summed = jnp.einsum('hqk,khd->qhd', to_half(weights).astype(jnp.float32), values3)
        result = to_half(summed / total.T[:, :, None]).reshape(block, HQ)
        return (result, top + jnp.log(total))
    outs, lses = lax.map(one_block, jnp.arange(count, dtype=jnp.int32))
    return (outs.reshape(SEQ_LEN, HQ), lses.transpose(1, 0, 2).reshape(HEADS, SEQ_LEN))

def attend_back(parts):
    query, keys, values, mixed, lse, grad_mixed = parts
    query3 = query.astype(jnp.float32).reshape(SEQ_LEN, HEADS, HEAD_DIM)
    keys3 = keys.astype(jnp.float32).reshape(SEQ_LEN, HEADS, HEAD_DIM)
    values3 = values.astype(jnp.float32).reshape(SEQ_LEN, HEADS, HEAD_DIM)
    mixed3 = mixed.astype(jnp.float32).reshape(SEQ_LEN, HEADS, HEAD_DIM)
    grad3 = grad_mixed.astype(jnp.float32).reshape(SEQ_LEN, HEADS, HEAD_DIM)
    delta = lax.optimization_barrier(jnp.sum(grad3 * mixed3, axis=-1)).T
    block = min(512, SEQ_LEN)
    count = SEQ_LEN // block
    key_index = jnp.arange(SEQ_LEN, dtype=jnp.int32)

    def one_block(carry, index):
        key_acc, value_acc = carry
        start = (index * block).astype(jnp.int32)
        query_block = lax.dynamic_slice_in_dim(query3, start, block, 0)
        grad_block = lax.dynamic_slice_in_dim(grad3, start, block, 0)
        lse_block = lax.dynamic_slice_in_dim(lse, start, block, 1)
        delta_block = lax.dynamic_slice_in_dim(delta, start, block, 1)
        scores = jnp.einsum('qhd,khd->hqk', query_block, keys3)
        allowed = key_index[None, :] <= (start + jnp.arange(block, dtype=jnp.int32))[:, None]
        scores = jnp.where(allowed[None], scores, neg_big)
        prob = jnp.where(allowed[None], jnp.exp(scores - lse_block[..., None]), 0.0)
        value_acc = value_acc + jnp.einsum('hqk,qhd->khd', to_half(prob).astype(jnp.float32), grad_block)
        grad_prob = jnp.einsum('qhd,khd->hqk', grad_block, values3)
        grad_scores = to_half(prob * (grad_prob - delta_block[..., None])).astype(jnp.float32)
        query_grad = jnp.einsum('hqk,khd->qhd', grad_scores, keys3)
        key_acc = key_acc + jnp.einsum('hqk,qhd->khd', grad_scores, query_block)
        return ((key_acc, value_acc), query_grad.reshape(block, HQ))
    zero = jnp.zeros((SEQ_LEN, HEADS, HEAD_DIM), jnp.float32)
    (key_acc, value_acc), query_grads = lax.scan(one_block, (zero, zero), jnp.arange(count, dtype=jnp.int32))
    return (query_grads.reshape(SEQ_LEN, HQ), key_acc.reshape(SEQ_LEN, HQ), value_acc.reshape(SEQ_LEN, HQ))

def contract_last(left, right):
    return lax.dot_general(left, right, (((1,), (1,)), ((), ())), preferred_element_type=jnp.float32)

def contract_first(left, right):
    return lax.dot_general(left, right, (((0,), (0,)), ((), ())), preferred_element_type=jnp.float32)

def reference(tokens, positions, routes, cotangent, attention_gain, query_weight, key_weight, value_weight, query_gain, key_gain, output_weight, ffn_gain, router_weight, gate_weight, up_weight, down_weight):
    total_rows = SEQS * SEQ_LEN
    flat = tokens.reshape(total_rows, D).astype(jnp.float32)
    grad_top = cotangent.reshape(total_rows, D).astype(jnp.float32)
    gain_one = attention_gain.astype(jnp.float32)
    gain_two = ffn_gain.astype(jnp.float32)
    query_gain_f = query_gain.astype(jnp.float32)
    key_gain_f = key_gain.astype(jnp.float32)
    factor = HEAD_DIM ** (-0.5)
    normed_one = to_half(rms_scale(flat, gain_one))
    query_raw = jnp.dot(normed_one, query_weight, preferred_element_type=jnp.float32)
    key_raw = jnp.dot(normed_one, key_weight, preferred_element_type=jnp.float32)
    value_rows = to_half(jnp.dot(normed_one, value_weight, preferred_element_type=jnp.float32))
    cosine, sine = rope_tables(positions.reshape(total_rows))
    query_rows = to_half(head_prepare(query_raw, query_gain_f, cosine, sine, factor))
    key_rows = to_half(head_prepare(key_raw, key_gain_f, cosine, sine, 1.0))
    shaped = (query_rows.reshape(SEQS, SEQ_LEN, HQ), key_rows.reshape(SEQS, SEQ_LEN, HQ), value_rows.reshape(SEQS, SEQ_LEN, HQ))
    mixed, lse = lax.map(attend_sequence, shaped)
    mixed_flat = mixed.reshape(total_rows, HQ)
    hidden = flat + jnp.dot(mixed_flat, output_weight, preferred_element_type=jnp.float32)
    normed_two = to_half(rms_scale(hidden, gain_two))
    logits = jnp.dot(normed_two, router_weight, preferred_element_type=jnp.float32)
    probs = jax.nn.softmax(logits, axis=-1)
    route_flat = routes.reshape(total_rows, TOP)
    choose = (route_flat[:, :, None] == jnp.arange(EXPERTS, dtype=jnp.int32)[None, None, :]).astype(jnp.float32)
    share = lax.optimization_barrier(jnp.sum(choose * probs[:, None, :], axis=-1))
    assign = total_rows * TOP
    blocks = N_SEQ * N_CTX
    expert_of = route_flat.reshape(assign).astype(jnp.int32)
    onehot = (expert_of[:, None] == jnp.arange(EXPERTS, dtype=jnp.int32)[None, :]).astype(jnp.int32)
    running = jnp.cumsum(onehot.reshape(blocks, TOK_DEV * TOP, EXPERTS), axis=1).reshape(assign, EXPERTS).astype(jnp.int32)
    rank = (lax.optimization_barrier(jnp.sum(onehot * running, axis=1)) - 1).astype(jnp.int32)
    block_of = jnp.arange(assign, dtype=jnp.int32) // (TOK_DEV * TOP)
    place = (expert_of * (blocks * CAP) + block_of * CAP + rank).astype(jnp.int32)
    table = jnp.full((EXPERTS * blocks * CAP,), assign, jnp.int32).at[place].set(jnp.arange(assign, dtype=jnp.int32))
    table = table.reshape(EXPERTS, blocks * CAP)
    share_flat = share.reshape(assign)

    def expert_step(carry, parts):
        moe_sum, grad_share, grad_norm = carry
        slots, gate_w, up_w, down_w = parts
        valid = slots < assign
        safe = jnp.minimum(slots, assign - 1).astype(jnp.int32)
        row = (safe // TOP).astype(jnp.int32)
        inputs = jnp.where(valid[:, None], normed_two[row], jnp.zeros((), jnp.bfloat16))
        gate = jnp.dot(inputs, gate_w, preferred_element_type=jnp.float32)
        up = jnp.dot(inputs, up_w, preferred_element_type=jnp.float32)
        sig = jax.nn.sigmoid(gate)
        act = to_half(gate * sig * up)
        result = jnp.dot(act, down_w, preferred_element_type=jnp.float32)
        weight = jnp.where(valid, share_flat[safe], 0.0)
        moe_sum = moe_sum.at[row].add(weight[:, None] * result)
        grad_share = grad_share.at[safe].add(jnp.where(valid, lax.optimization_barrier(jnp.sum(grad_top[row] * result, axis=-1)), 0.0))
        grad_result = to_half(weight[:, None] * grad_top[row])
        grad_act = contract_last(grad_result, down_w)
        grad_down = contract_first(act, grad_result)
        grad_gate = to_half(grad_act * up * sig * (1.0 + gate * (1.0 - sig)))
        grad_up = to_half(grad_act * gate * sig)
        grad_gate_w = contract_first(inputs, grad_gate)
        grad_up_w = contract_first(inputs, grad_up)
        back = contract_last(grad_gate, gate_w) + contract_last(grad_up, up_w)
        grad_norm = grad_norm.at[row].add(jnp.where(valid[:, None], back, 0.0))
        return ((moe_sum, grad_share, grad_norm), (grad_gate_w, grad_up_w, grad_down))
    start_carry = (jnp.zeros((total_rows, D), jnp.float32), jnp.zeros((assign,), jnp.float32), jnp.zeros((total_rows, D), jnp.float32))
    (moe_sum, grad_share, grad_norm_moe), (gate_grads, up_grads, down_grads) = lax.scan(expert_step, start_carry, (table, gate_weight, up_weight, down_weight))
    layer_output = (hidden + moe_sum).astype(jnp.bfloat16).reshape(SEQS, SEQ_LEN, D)
    grad_prob = lax.optimization_barrier(jnp.sum(choose * grad_share.reshape(total_rows, TOP)[:, :, None], axis=1))
    grad_logits = to_half(probs * (grad_prob - lax.optimization_barrier(jnp.sum(probs * grad_prob, axis=-1, keepdims=True))))
    router_grad = contract_first(normed_two, grad_logits)
    grad_normed_two = grad_norm_moe + contract_last(grad_logits, router_weight)
    _, pull_two = jax.vjp(rms_scale, hidden, gain_two)
    grad_hidden_part, ffn_gain_grad = pull_two(grad_normed_two)
    grad_hidden = grad_top + grad_hidden_part
    grad_attn = to_half(grad_hidden)
    output_grad = contract_first(mixed_flat, grad_attn)
    grad_mixed = to_half(contract_last(grad_attn, output_weight))
    back_parts = (shaped[0], shaped[1], shaped[2], mixed, lse, grad_mixed.reshape(SEQS, SEQ_LEN, HQ))
    grad_queries, grad_keys, grad_values = lax.map(attend_back, back_parts)
    grad_queries = grad_queries.reshape(total_rows, HQ)
    grad_keys = grad_keys.reshape(total_rows, HQ)
    grad_values = grad_values.reshape(total_rows, HQ)
    _, pull_query = jax.vjp(lambda proj, gain: head_prepare(proj, gain, cosine, sine, factor), query_raw, query_gain_f)
    grad_query_raw, query_gain_grad = pull_query(grad_queries)
    _, pull_key = jax.vjp(lambda proj, gain: head_prepare(proj, gain, cosine, sine, 1.0), key_raw, key_gain_f)
    grad_key_raw, key_gain_grad = pull_key(grad_keys)
    query_half = to_half(grad_query_raw)
    key_half = to_half(grad_key_raw)
    value_half = to_half(grad_values)
    query_grad = contract_first(normed_one, query_half)
    key_grad = contract_first(normed_one, key_half)
    value_grad = contract_first(normed_one, value_half)
    grad_normed_one = contract_last(query_half, query_weight) + contract_last(key_half, key_weight) + contract_last(value_half, value_weight)
    _, pull_one = jax.vjp(rms_scale, flat, gain_one)
    grad_flat_part, attention_gain_grad = pull_one(grad_normed_one)
    tokens_grad = (grad_hidden + grad_flat_part).reshape(SEQS, SEQ_LEN, D)
    return (layer_output, tokens_grad, attention_gain_grad, query_grad, key_grad, value_grad, query_gain_grad, key_gain_grad, output_grad, ffn_gain_grad, router_grad, gate_grads, up_grads, down_grads)
```

```python
import functools

import jax
import jax.numpy as jnp
import numpy as np
from jax import lax
from jax.experimental import pallas as pl
from jax.experimental.pallas import tpu as pltpu
from jax.sharding import PartitionSpec as P

MESH = pl.DeviceIdType.MESH
BF = jnp.bfloat16
F32 = jnp.float32


def place():
    s = lax.axis_index("seq")
    z = lax.axis_index("ctx")
    m = lax.axis_index("mp")
    return s, z, m


def flip_x(s):
    return s + 1 - 2 * lax.rem(s, 2)


def flip_y(s):
    return s + 2 - 4 * lax.div(s, 2)


def remote(src, dst, send, recv, device):
    return pltpu.make_async_remote_copy(
        src_ref=src, dst_ref=dst, send_sem=send, recv_sem=recv,
        device_id=device, device_id_type=MESH,
    )


def signal(device):
    pl.semaphore_signal(
        pltpu.get_barrier_semaphore(), inc=1, device_id=device, device_id_type=MESH
    )


def when(cond, fn):
    if cond is True:
        fn()
    else:
        pl.when(cond)(fn)


def near_planes(z):
    return (z, flip_x(z), 2 - lax.div(z, 2), 3 - 3 * lax.div(z, 2))


def far_planes(z):
    return (3 - 3 * lax.div(z, 2), lax.rem(2 + 3 * z, 5), 1 + lax.rem(z, 2), z)


def span(start, size):
    return pl.ds(pl.multiple_of(start, size), size)


class Part:
    def __init__(self, kind, source, target):
        self.kind = kind
        self.source = source
        self.target = target
        self.whole = kind == "small"

    def own(self, m):
        if self.kind == "rows":
            width = self.source.shape[1] // 2
            return self.source.at[:, span(m * width, width)]
        return self.source

    def piece(self, row, plane, core, half=None):
        ref = self.target
        if self.kind == "small":
            return ref.at[plane * 4 + row, core]
        if self.kind == "line":
            rows = self.source.shape[0]
            return ref.at[span(core * rows, rows), span(plane * 128, 128)]
        if self.kind == "cols":
            rows = self.source.shape[1] // 2
            base = (row * 4 + plane) * 2 * rows + core * rows
            if half is None:
                return ref.at[span(base, rows), :]
            return ref.at[span(base + half * (rows // 2), rows // 2), :]
        if self.kind == "rows":
            rows, width = self.source.shape[0], self.source.shape[1] // 2
            cols = span(core * width, width)
            base = (plane * 4 + row) * rows
        elif self.kind == "chips":
            rows, width = self.source.shape[0], self.source.shape[1] // 2
            cols = span(core * width, width)
            base = (row * 4 + plane) * rows
        else:
            rows = self.source.shape[0]
            cols = span((row * 4 + plane) * 128, 128)
            base = core * rows
        if half is None:
            return ref.at[span(base, rows), cols]
        return ref.at[span(base + half * (rows // 2), rows // 2), cols]

    def mirrored(self):
        return self.kind in ("rows", "chips", "cols")


class Gather:
    Z, X, Y, DX, DY, PO, PX, PY, P0, P1, UP, DN = range(12)

    def __init__(self, parts, send, recv):
        self.parts, self.send, self.recv = parts, send, recv
        s, z, m = place()
        self.s, self.z, self.m = s, z, m
        self.lines = (s, flip_x(s), flip_y(s), 3 - s)
        self.xn, self.yn, self.pn = (self.lines[1], z, m), (self.lines[2], z, m), (s, z, 1 - m)
        self.planes = near_planes(z)
        self.pending = []

    def own(self, k):
        part = self.parts[k]
        if part.kind == "chips":
            width = part.source.shape[1] // 2
            return part.source.at[:, span(self.m * width, width)]
        return part.own(self.m)

    def push(self, cond, k, kind, at, source, target, device, out=None):
        out = kind if out is None else out
        copy = lambda: remote(source, target, self.send.at[k, out, at], self.recv.at[k, kind, at], device)
        when(cond, lambda: copy().start())
        self.pending.append((cond, copy))

    def landed(self, k, kind, at, target):
        remote(target, target, self.send.at[k, kind, at], self.recv.at[k, kind, at], self.pn).wait_recv()

    def fan(self, k, at, source):
        target = self.parts[k].piece(self.s, at, self.m)
        self.push(True, k, self.X, at, source, target, self.xn)
        self.push(True, k, self.Y, at, source, target, self.yn)

    def start(self):
        z, at = self.z, self.z
        for k, part in enumerate(self.parts):
            source, target = self.own(k), part.piece(self.s, at, self.m)
            self.push(z < 3, k, self.Z, at, source, target, (self.s, z + 1, self.m), self.UP)
            self.push(z > 0, k, self.Z, at, source, target, (self.s, z - 1, self.m), self.DN)
            self.fan(k, at, source)
            if not part.mirrored():
                self.push(True, k, self.PO, at, source, target, self.pn)

    def along(self, step):
        z, at = self.z, self.planes[step]
        goal = 3 - z if step == 1 else 3 * z - 3
        inner = jnp.logical_and(z > 0, z < 3)
        for k, part in enumerate(self.parts):
            target = part.piece(self.s, at, self.m)
            self.landed(k, self.Z, at, target)
            self.push(inner, k, self.Z, at, target, target, (self.s, goal, self.m), self.UP)
            self.fan(k, at, target)
            self.push(True, k, self.PO, at, target, target, self.pn)

    def across(self, step):
        at = self.planes[step]
        for k, part in enumerate(self.parts):
            whole = part.piece(self.lines[1], at, self.m)
            half = whole if part.whole else part.piece(self.lines[1], at, self.m, 0)
            self.landed(k, self.X, at, whole)
            self.push(True, k, self.DY, at, half, half, self.yn)
            self.push(True, k, self.PX, at, whole, whole, self.pn)
            whole = part.piece(self.lines[2], at, self.m)
            self.landed(k, self.Y, at, whole)
            if not part.whole:
                half = part.piece(self.lines[2], at, self.m, 1)
                self.push(True, k, self.DX, at, half, half, self.xn)
            self.push(True, k, self.PY, at, whole, whole, self.pn)

    def corner(self, step):
        at, far = self.planes[step], self.lines[3]
        for k, part in enumerate(self.parts):
            half = part.piece(far, at, self.m, None if part.whole else 0)
            self.landed(k, self.DY, at, half)
            self.push(True, k, self.P0, at, half, half, self.pn)
            if not part.whole:
                half = part.piece(far, at, self.m, 1)
                self.landed(k, self.DX, at, half)
                self.push(True, k, self.P1, at, half, half, self.pn)

    def ready(self, step):
        at, other = self.planes[step], 1 - self.m
        for k, part in enumerate(self.parts):
            if step > 0 or not part.mirrored():
                self.landed(k, self.PO, at, part.piece(self.s, at, other))
            self.landed(k, self.PX, at, part.piece(self.lines[1], at, other))
            self.landed(k, self.PY, at, part.piece(self.lines[2], at, other))
            self.landed(k, self.P0, at, part.piece(self.lines[3], at, other, None if part.whole else 0))
            if not part.whole:
                self.landed(k, self.P1, at, part.piece(self.lines[3], at, other, 1))

    def finish(self):
        for cond, copy in self.pending:
            when(cond, lambda copy=copy: copy().wait_send())


class Line(Gather):
    def fan(self, k, at, source):
        pass

    def ready(self, step):
        at = self.planes[step]
        for k, part in enumerate(self.parts):
            self.landed(k, self.PO, at, part.piece(self.s, at, 1 - self.m))


class Spread(Gather):
    def block(self, plane):
        source = self.parts[0].source
        rows = source.shape[1] // 2
        return source.at[plane, span(self.m * rows, rows), :]

    def start(self):
        z = self.z
        target = self.parts[0].piece(self.s, z, self.m)
        for step in (1, 2, 3):
            plane = lax.rem(z + step, 4)
            out = (self.UP, self.DN, self.Z)[step - 1]
            self.push(True, 0, self.Z, z, self.block(plane), target, (self.s, plane, self.m), out)
        self.fan(0, z, self.block(z))

    def along(self, step):
        at = self.planes[step]
        target = self.parts[0].piece(self.s, at, self.m)
        self.landed(0, self.Z, at, target)
        self.fan(0, at, target)
        self.push(True, 0, self.PO, at, target, target, self.pn)


def meet_chips():
    s, z, m = place()
    c = s * 4 + z
    for step in range(1, 16):
        j = lax.rem(c + step, 16)
        signal((lax.div(j, 4), lax.rem(j, 4), m))
    signal((s, z, 1 - m))
    pl.semaphore_wait(pltpu.get_barrier_semaphore(), 16)


def add_rows(put, sources, count, step=16):
    def run(r, _):
        at = span(r * step, step)
        total = sources[0](at)
        for source in sources[1:]:
            total = total + source(at)
        put(at, total)
        return 0
    lax.fori_loop(0, count // step, run, 0)


def shifted(at, base, step=16):
    return pl.ds(pl.multiple_of(at.start + base, step), step)


class Reduce:
    def __init__(self, pair, by_plane, src, acc, out, bufs, sems):
        self.pair, self.by_plane, self.src, self.acc, self.out = pair, by_plane, src, acc, out
        (self.buf0, self.bufx, self.bufy, self.bufx2, self.bufy2, self.zbuf, self.zsend, self.fin) = bufs
        self.send, self.recv = sems
        s, z, m = place()
        self.s, self.z, self.m = s, z, m
        self.xn, self.yn, self.pn = (flip_x(s), z, m), (flip_y(s), z, m), (s, z, 1 - m)
        self.lines = (s, flip_x(s), flip_y(s), 3 - s)
        self.rows = self.fin.shape[0]
        self.half = self.rows // 2
        self.width = self.fin.shape[1]
        self.mine = span(m * self.width, self.width)
        self.cols = self.mine if acc.shape[1] > self.width else slice(None)
        self.other = span((1 - m) * self.width, self.width)
        self.pending = []

    def push(self, kind, at, source, target, device):
        copy = lambda: remote(source, target, self.send.at[kind, at], self.recv.at[kind, at], device)
        copy().start()
        self.pending.append(copy)

    def landed(self, kind, at, target):
        remote(target, target, self.send.at[kind, at], self.recv.at[kind, at], self.pn).wait_recv()

    def base(self, at, q, by_plane=None):
        by_plane = self.by_plane if by_plane is None else by_plane
        row = self.lines[q]
        return (at * 4 + row if by_plane else row * 4 + at) * self.rows

    def held(self, at, q):
        return self.base(at, q, self.pair or self.by_plane)

    def swap(self, at):
        for q in (3, 1, 2, 0):
            self.push(q, at, self.src.at[span(self.base(at, q), self.rows), self.other],
                      self.buf0.at[at, q], self.pn)

    def block(self, at, q, lo):
        return self.acc.at[pl.ds(pl.multiple_of(self.held(at, q) + lo, self.half), self.half), self.cols]

    def first(self, at):
        for q in (3, 1, 2, 0):
            if self.pair:
                self.landed(q, at, self.buf0.at[at, q])
                base = self.base(at, q)
                held = self.held(at, q)

                def put(r, v, held=held):
                    self.acc[shifted(r, held), self.cols] = v.astype(BF)
                add_rows(put, [
                    lambda r, base=base: self.src[shifted(r, base), self.mine].astype(F32),
                    lambda r, q=q: self.buf0[at, q, r].astype(F32)], self.rows)
            if q == 3:
                self.push(4, at, self.block(at, 3, 0), self.bufx.at[at, 1], self.xn)
                self.push(5, at, self.block(at, 3, self.half), self.bufy.at[at, 1], self.yn)
            if q == 1:
                self.push(6, at, self.block(at, 1, 0), self.bufx.at[at, 0], self.xn)
            if q == 2:
                self.push(7, at, self.block(at, 2, self.half), self.bufy.at[at, 0], self.yn)

    def local(self, at, q, lo):
        held = self.held(at, q) + lo
        return lambda r: self.acc[shifted(r, held), self.cols].astype(F32)

    def second(self, at):
        self.landed(4, at, self.bufx.at[at, 1])

        def put_x(r, v):
            self.bufx[at, 1, r] = v.astype(BF)
        add_rows(put_x, [self.local(at, 2, 0), lambda r: self.bufx[at, 1, r].astype(F32)], self.half)
        self.push(8, at, self.bufx.at[at, 1], self.bufy2.at[at], self.yn)
        self.landed(5, at, self.bufy.at[at, 1])

        def put_y(r, v):
            self.bufy[at, 1, r] = v.astype(BF)
        add_rows(put_y, [self.local(at, 1, self.half), lambda r: self.bufy[at, 1, r].astype(F32)], self.half)
        self.push(9, at, self.bufy.at[at, 1], self.bufx2.at[at], self.xn)

    def settle(self, at, put_low, put_high):
        half = self.half
        self.landed(6, at, self.bufx.at[at, 0])
        self.landed(8, at, self.bufy2.at[at])
        self.landed(7, at, self.bufy.at[at, 0])
        self.landed(9, at, self.bufx2.at[at])
        add_rows(put_low, [self.local(at, 0, 0), lambda r: self.bufx[at, 0, r].astype(F32),
                           lambda r: self.bufy2[at, r].astype(F32)], half)
        add_rows(put_high, [self.local(at, 0, half), lambda r: self.bufy[at, 0, r].astype(F32),
                            lambda r: self.bufx2[at, r].astype(F32)], half)

    def third(self, at, slot):
        half = self.half

        def low(r, v):
            self.zsend[slot, r] = v.astype(BF)

        def high(r, v):
            self.zsend[slot, shifted(r, half)] = v.astype(BF)
        self.settle(at, low, high)
        copy = lambda: remote(self.zsend.at[slot], self.zbuf.at[self.z], self.send.at[12, slot],
                              self.recv.at[10, self.z], (self.s, at, self.m))
        copy().start()
        self.pending.append(copy)

    def keep(self):
        half = self.half

        def low(r, v):
            self.fin[r] = v

        def high(r, v):
            self.fin[shifted(r, half)] = v
        self.settle(self.z, low, high)

    def close(self):
        mine, other = self.mine, self.other
        others = [lax.rem(self.z + step, 4) for step in (1, 2, 3)]
        for at in others:
            self.landed(10, at, self.zbuf.at[at])

        def put(r, v):
            self.out[r, mine] = v.astype(BF)
        add_rows(put, [lambda r: self.fin[r]] + [
            lambda r, at=at: self.zbuf[at, r].astype(F32) for at in others], self.rows)
        self.push(13, 0, self.out.at[:, mine], self.out.at[:, mine], self.pn)

    def landing(self):
        self.landed(13, 0, self.out.at[:, self.other])

    def finish(self):
        for copy in self.pending:
            copy().wait_send()


def reduce_buffers(pair, rows, width):
    half = rows // 2
    return [
        pltpu.VMEM((4, 4, rows, width) if pair else (1, 1, 16, width), BF),
        pltpu.VMEM((4, 2, half, width), BF),
        pltpu.VMEM((4, 2, half, width), BF),
        pltpu.VMEM((4, half, width), BF),
        pltpu.VMEM((4, half, width), BF),
        pltpu.VMEM((4, rows, width), BF),
        pltpu.VMEM((3, rows, width), BF),
        pltpu.VMEM((rows, width), F32),
        pltpu.SemaphoreType.DMA((14, 4)),
        pltpu.SemaphoreType.DMA((14, 4)),
    ]


def experts_body(two_ref, share_ref, top_ref, gate_ref, up_ref, down_ref,
                 back_out, prob_out, moe_out, dgate_out, dup_out, ddown_out,
                 two_all, shares, top_all, pair_w, down_w, pull, pair_v,
                 acts, dpair, back, prob_v, stage, dstage,
                 buf0, bufx, bufy, bufx2, bufy2, zbuf, zsend, fin, rsend, rrecv,
                 gsend, grecv, psend, precv, load, store, dstore):
    s, z, m = place()
    c = s * 4 + z
    rows = two_ref.shape[0]
    width = two_ref.shape[1]
    hidden = down_w.shape[0]
    block = 4 * rows
    loads = [
        pltpu.make_async_copy(top_ref, top_all, load.at[0]),
        pltpu.make_async_copy(down_ref, down_w, load.at[1]),
        pltpu.make_async_copy(gate_ref, pair_w.at[:, pl.ds(0, hidden)], load.at[2]),
        pltpu.make_async_copy(up_ref, pair_w.at[:, pl.ds(hidden, hidden)], load.at[3]),
    ]
    for copy in loads:
        copy.start()
    meet_chips()
    work = Gather([Part("rows", two_ref, two_all), Part("small", share_ref, shares)], gsend, grecv)
    work.start()
    two_all[span((z * 4 + s) * rows, rows), :] = two_ref[...]
    shares[z * 4 + s, m] = share_ref[...]
    total = Reduce(True, True, back, back, back_out,
                   (buf0, bufx, bufy, bufx2, bufy2, zbuf, zsend, fin), (rsend, rrecv))
    planes = work.planes

    def tiles(count, size, fn):
        def run(i, _):
            fn(span(i * size, size))
            return 0
        lax.fori_loop(0, count // size, run, 0)

    def pulls(i):
        at = pl.ds(i * block, block)

        def tile(cols):
            pull[at, cols] = contract_last(top_all[at, :], down_w[cols, :])
        tiles(hidden, 512, tile)

    def enter(side, k):
        at = span(planes[k] * block, block)
        cols = pl.ds(side * hidden, hidden)
        pair_v[:, cols] = jnp.dot(two_all[at, :], pair_w[:, cols], preferred_element_type=F32)

    def middle(k):
        def one(row, _):
            slot = planes[k] * 4 + row
            wide = jnp.broadcast_to(shares[slot, m, pl.ds(c, 1), :], (rows, rows))
            column = jnp.transpose(wide)[:, 0:1]
            base = span(slot * rows, rows)
            here = span(row * rows, rows)
            gate = pair_v[here, pl.ds(0, hidden)]
            up = pair_v[here, pl.ds(hidden, hidden)]
            drawn = pull[base, :]
            sig = jax.nn.sigmoid(gate)
            act = gate * sig * up
            acts[base, :] = (act * column).astype(BF)
            grad = drawn * column
            dpair[base, pl.ds(0, hidden)] = (grad * up * sig * (1.0 + gate * (1.0 - sig))).astype(BF)
            dpair[base, pl.ds(hidden, hidden)] = (grad * gate * sig).astype(BF)
            prob = jnp.sum(act * drawn, axis=1, keepdims=True)
            prob_v[slot] = jnp.transpose(jnp.broadcast_to(prob, (rows, rows)))[0:8, :]
            return 0
        lax.fori_loop(0, 4, one, 0)

    def backs(k):
        at = span(planes[k] * block, block)

        def tile(cols):
            back[at, cols] = contract_last(dpair[at, :], pair_w[cols, :]).astype(BF)
        tiles(width, 1024, tile)
        total.swap(planes[k])

    def saves(i, t):
        cols = pl.ds(t * 1024, 1024)
        return pltpu.make_async_copy(
            stage.at[t], moe_out.at[pl.ds(i * block, block), cols], store.at[t])

    def moes(i):
        at = pl.ds(i * block, block)
        for t in (0, 1):
            if i >= 1:
                saves(i - 1, t).wait()
            cols = pl.ds(t * 1024, 1024)
            stage[t] = jnp.dot(acts[at, :], down_w[:, cols], preferred_element_type=F32).astype(BF)
            saves(i, t).start()

    def keep(i):
        rows_at = span(i * 512, 512)
        slot = lax.rem(i, 2)
        return [
            pltpu.make_async_copy(
                dstage.at[slot, :, pl.ds(side * hidden, hidden)],
                (dgate_out, dup_out)[side].at[rows_at, :],
                dstore.at[slot, side],
            )
            for side in (0, 1)
        ]

    def keep_down(i):
        return pltpu.make_async_copy(
            dstage.at[i], ddown_out.at[:, pl.ds(i * 1024, 1024)], dstore.at[i, 2])

    def grads(low, high):
        def one(i, _):
            def settle():
                for copy in keep(i - 2):
                    copy.wait()
            pl.when(i >= 2)(settle)
            cols = span(i * 512, 512)
            dstage[lax.rem(i, 2)] = contract_first(two_all[:, cols], dpair[...])
            for copy in keep(i):
                copy.start()
            return 0
        lax.fori_loop(low, high, one, 0)

    def downs():
        for i in (2, 3):
            for copy in keep(i):
                copy.wait()
        for i in (0, 1):
            dstage[i] = contract_first(acts[...], top_all[:, pl.ds(i * 1024, 1024)])
            keep_down(i).start()

    loads[0].wait()
    loads[1].wait()
    pulls(0)
    work.along(1)
    work.across(0)
    pulls(1)
    work.along(2)
    work.across(1)
    pulls(2)
    work.along(3)
    work.corner(0)
    pulls(3)
    work.across(2)
    loads[2].wait()
    loads[3].wait()
    work.ready(0)
    enter(0, 0)
    work.corner(1)
    enter(1, 0)
    work.across(3)
    middle(0)
    work.corner(2)
    backs(0)
    work.ready(1)
    enter(0, 1)
    work.corner(3)
    enter(1, 1)
    total.first(planes[0])
    middle(1)
    backs(1)
    total.second(planes[0])
    work.ready(2)
    enter(0, 2)
    total.first(planes[1])
    enter(1, 2)
    middle(2)
    backs(2)
    total.second(planes[1])
    work.ready(3)
    enter(0, 3)
    total.first(planes[2])
    enter(1, 3)
    middle(3)

    def dev(j):
        return (lax.div(j, 4), lax.rem(j, 4), m)

    def send_prob(step):
        j = lax.rem(c + step, 16)
        slot = lax.rem(j, 4) * 4 + lax.div(j, 4)
        return remote(prob_v.at[slot], prob_out.at[m, c], psend.at[step], precv.at[step], dev(j))
    for step in range(1, 16):
        send_prob(step).start()
    prob_out[m, c] = prob_v[z * 4 + s]
    backs(3)
    total.second(planes[2])
    moes(0)
    total.first(planes[3])
    total.keep()
    moes(1)
    total.third(planes[1], 0)
    moes(2)
    total.second(planes[3])
    total.third(planes[2], 1)
    moes(3)
    grads(0, 1)
    total.third(planes[3], 2)
    grads(1, 3)
    for step in range(1, 16):
        j = lax.rem(c + 16 - step, 16)
        target = prob_out.at[m, j]
        remote(target, target, psend.at[step], precv.at[step], dev(j)).wait_recv()
    pair = remote(prob_out.at[m], prob_out.at[m], psend.at[0], precv.at[0], (s, z, 1 - m))
    pair.start()
    grads(3, 4)
    downs()
    total.close()
    for i in (0, 1):
        keep_down(i).wait()
    for t in (0, 1):
        saves(3, t).wait()
    total.landing()
    other = prob_out.at[1 - m]
    remote(other, other, psend.at[0], precv.at[0], (s, z, 1 - m)).wait_recv()
    pair.wait_send()
    for step in range(1, 16):
        send_prob(step).wait_send()
    work.finish()
    total.finish()


def experts(ident, two, share, top, gate, up, down):
    rows, width = two.shape
    hidden = gate.shape[1]
    every = 16 * rows
    block = 4 * rows
    vmem = pl.BlockSpec(memory_space=pltpu.VMEM)
    hbm = pl.BlockSpec(memory_space=pl.ANY)
    return pl.pallas_call(
        experts_body,
        out_shape=(
            jax.ShapeDtypeStruct((rows, width), BF),
            jax.ShapeDtypeStruct((2, 16, 8, rows), F32),
            jax.ShapeDtypeStruct((every, width), BF),
            jax.ShapeDtypeStruct((width, hidden), F32),
            jax.ShapeDtypeStruct((width, hidden), F32),
            jax.ShapeDtypeStruct((hidden, width), F32),
        ),
        in_specs=[vmem, vmem, hbm, hbm, hbm, hbm],
        out_specs=(vmem, vmem, hbm, hbm, hbm, hbm),
        scratch_shapes=[
            pltpu.VMEM((every, width), BF),
            pltpu.VMEM((16, 2) + share.shape, F32),
            pltpu.VMEM((every, width), BF),
            pltpu.VMEM((width, 2 * hidden), BF),
            pltpu.VMEM((hidden, width), BF),
            pltpu.VMEM((every, hidden), F32),
            pltpu.VMEM((block, 2 * hidden), F32),
            pltpu.VMEM((every, hidden), BF),
            pltpu.VMEM((every, 2 * hidden), BF),
            pltpu.VMEM((every, width), BF),
            pltpu.VMEM((16, 8, rows), F32),
            pltpu.VMEM((2, block, 1024), BF),
            pltpu.VMEM((2, 512, 2 * hidden), F32),
        ]
        + reduce_buffers(True, rows, width // 2)
        + [
            pltpu.SemaphoreType.DMA((2, 12, 4)),
            pltpu.SemaphoreType.DMA((2, 12, 4)),
            pltpu.SemaphoreType.DMA((16,)),
            pltpu.SemaphoreType.DMA((16,)),
            pltpu.SemaphoreType.DMA((4,)),
            pltpu.SemaphoreType.DMA((2,)),
            pltpu.SemaphoreType.DMA((2, 3)),
        ],
        compiler_params=pltpu.CompilerParams(collective_id=ident, has_side_effects=True,
                                             vmem_limit_bytes=66900000),
        name="experts_%d" % ident,
    )(two, share, top, gate, up, down)


class Hand:
    def __init__(self, source, target, send, recv):
        s, z, m = place()
        self.c, self.m, self.pn = s * 4 + z, m, (s, z, 1 - m)
        self.source, self.target, self.send, self.recv = source, target, send, recv

    def dev(self, j):
        return (lax.div(j, 4), lax.rem(j, 4), self.m)

    def copy(self, step):
        j = lax.rem(self.c + step, 16)
        return remote(self.source(j), self.target(self.c), self.send.at[step], self.recv.at[step], self.dev(j))

    def start(self):
        for step in range(1, 16):
            self.copy(step).start()

    def collect(self):
        for step in range(1, 16):
            j = lax.rem(self.c + 16 - step, 16)
            remote(self.target(j), self.target(j), self.send.at[step], self.recv.at[step], self.pn).wait_recv()

    def finish(self):
        for step in range(1, 16):
            self.copy(step).wait_send()


class Chips:
    def __init__(self, source, target, send, recv, fsend, frecv, local):
        s, z, m = place()
        self.c, self.m, self.pn = s * 4 + z, m, (s, z, 1 - m)
        self.first = lax.div(self.c, 8) == m
        self.source, self.target = source, target
        self.send, self.recv, self.fsend, self.frecv, self.local = send, recv, fsend, frecv, local

    def copy(self, i):
        j = 8 * self.m + i
        return remote(self.source(i), self.target.at[self.c], self.send.at[i], self.recv.at[self.c],
                      (lax.div(j, 4), lax.rem(j, 4), self.m))

    def mine(self):
        return pltpu.make_async_copy(
            self.source(lax.rem(self.c, 8)), self.target.at[self.c], self.local.at[0])

    def each(self, fn):
        for step in range(8):
            i = lax.rem(self.c + 1 + step, 8)
            pl.when(8 * self.m + i != self.c)(lambda i=i: fn(self.copy(i)))

    def start(self):
        self.each(lambda copy: copy.start())
        pl.when(self.first)(lambda: self.mine().start())

    def forward(self, j):
        return remote(self.target.at[j], self.target.at[j], self.fsend.at[j], self.frecv.at[j], self.pn)

    def collect(self):
        def take():
            self.mine().wait()
            self.forward(self.c).start()
            for step in range(1, 16):
                j = lax.rem(self.c + 16 - step, 16)
                remote(self.target.at[j], self.target.at[j], self.send.at[0], self.recv.at[j],
                       self.pn).wait_recv()
                self.forward(j).start()
        pl.when(self.first)(take)

    def follow(self):
        def wait():
            for j in range(16):
                self.forward(j).wait_recv()
        pl.when(jnp.logical_not(self.first))(wait)

    def finish(self):
        def wait():
            for j in range(16):
                self.forward(j).wait_send()
        pl.when(self.first)(wait)
        self.each(lambda copy: copy.wait_send())


def chips_semaphores():
    return [pltpu.SemaphoreType.DMA((8,))] + [pltpu.SemaphoreType.DMA((16,))] * 3 + [
        pltpu.SemaphoreType.DMA((1,))]


def front_body(tok_ref, one_ref, second_ref, place_ref, router_ref, qg_ref, kg_ref, routes_ref,
               qw_ref, kw_ref, vw_ref, wo_ref, cot_ref, freq_ref,
               n1_out, wo_out, cot_out, w3, info, raw, rows3, squares, mixed, lse, trig, own_mixed,
               hidden, two, probs_out, chosen_out, share_out, heads_out, gain_out,
               info_ref, packed_ref, n1_own, n1_all, wo_all, wide_mixed, gathered, sums, line,
               nsend, nrecv, osend, orecv, csend, crecv,
               isend, irecv, qsend, qrecv, pairs, *chips_sems):
    s, z, m = place()
    c = s * 4 + z
    pn = (s, z, 1 - m)
    rows, width = tok_ref.shape
    dim = 128
    planes = near_planes(z)
    lane = lax.broadcasted_iota(jnp.int32, (rows, dim), 1)
    info_ref[...] = jnp.zeros_like(info_ref)
    info_ref[0:1, :] = one_ref[...].astype(F32)
    info_ref[1:2, :] = second_ref[...].astype(F32)
    info_ref[2:3, :] = place_ref[...].astype(F32)
    info_ref[4:20, :] = router_ref[...].astype(F32)
    info_ref[24:32, 0:8] = qg_ref[...].astype(F32)
    info_ref[32:40, 0:8] = kg_ref[...].astype(F32)
    for i in range(8):
        for n, ref in enumerate((qw_ref, kw_ref, vw_ref)):
            packed_ref[i, :, pl.ds(n * dim, dim)] = ref[:, pl.ds(i * dim, dim)]
    meet_chips()
    hand = Hand(lambda j: info_ref, lambda j: info.at[m, j], isend, irecv)
    hand.start()
    weights = Chips(lambda i: packed_ref.at[i], w3, *chips_sems[:5])
    weights.start()
    info[m, c] = info_ref[...]

    def square_sum(r, _):
        at = span(r * 16, 16)
        x = tok_ref[at, :].astype(F32)
        mean = jnp.sum(x * x, axis=1, keepdims=True) / width
        line[at, :] = jnp.broadcast_to(lax.rsqrt(mean + eps), (16, dim))
        return 0
    lax.fori_loop(0, rows // 16, square_sum, 0)
    hand.collect()
    swap = remote(info.at[m], info.at[m], pairs.at[0], pairs.at[1], pn)
    swap.start()

    def normalize(j, _):
        at = span(j * dim, dim)
        n1_own[:, at] = (tok_ref[:, at].astype(F32) * line[...] * info[m, j, 0:1, :]).astype(BF)
        return 0
    lax.fori_loop(0, 16, normalize, 0)
    first = Gather([Part("rows", n1_own, n1_all)], nsend, nrecv)
    first.start()
    n1_all[span((z * 4 + s) * rows, rows), :] = n1_own[...]

    def tables(b, _):
        spot = jnp.broadcast_to(info[m, 8 * m + b, 2:3, :], (rows, dim))
        angle = jnp.transpose(spot) * freq_ref[0:1, :]
        trig[0, b] = jnp.cos(angle)
        trig[1, b] = jnp.where(lane < dim // 2, -jnp.sin(angle), jnp.sin(angle))
        return 0
    lax.fori_loop(0, 8, tables, 0)
    other = info.at[1 - m]
    remote(other, other, pairs.at[0], pairs.at[1], pn).wait_recv()

    first.along(1)
    first.across(0)
    weights.collect()
    first.along(2)
    first.across(1)
    first.along(3)
    first.corner(0)
    weights.follow()
    first.across(2)
    first.ready(0)

    def project(k):
        value = jnp.dot(n1_all[span((planes[k] * 4 + 2 * m) * rows, 2 * rows), :],
                        w3[...].reshape(width, 3 * dim), preferred_element_type=F32)
        for e in (0, 1):
            part = value[e * rows : (e + 1) * rows, :]
            base = span((e * 4 + planes[k]) * rows, rows)
            raw[base, :] = part[:, : 2 * dim]
            rows3[base, pl.ds(2 * dim, dim)] = part[:, 2 * dim :].astype(BF)
    project(0)
    first.corner(1)
    first.across(3)
    outer = Gather([Part("heads", wo_ref, wo_all)], osend, orecv)
    outer.start()
    first.ready(1)
    project(1)
    first.corner(2)
    first.ready(2)
    project(2)
    first.corner(3)
    first.ready(3)
    project(3)

    def norms(b, total):
        at = span(b * rows, rows)
        q = raw[at, pl.ds(0, dim)]
        k = raw[at, pl.ds(dim, dim)]
        total = jnp.where(lane == b, jnp.sum(q * q, axis=1, keepdims=True), total)
        return jnp.where(lane == b + 8, jnp.sum(k * k, axis=1, keepdims=True), total)
    total = lax.fori_loop(0, 8, norms, jnp.zeros((rows, dim), F32))
    sums[...] = jnp.transpose(total)[0:16, :]
    share = Hand(lambda j: sums, lambda j: gathered.at[j], qsend, qrecv)
    share.start()
    gathered[c] = sums[...]
    save_n1 = pltpu.make_async_copy(n1_all, n1_out, pairs.at[2])
    save_n1.start()
    wo_own = pltpu.make_async_copy(wo_ref, outer.parts[0].piece(s, z, m), pairs.at[3])
    wo_own.start()
    share.collect()

    def add_up(j, acc):
        return acc + gathered[j]
    summed = lax.fori_loop(1, 16, add_up, gathered[0])
    squares[...] = summed
    wide = jnp.concatenate([lax.rsqrt(summed / width + eps), jnp.zeros((rows - 16, dim), F32)], axis=0)
    line[...] = jnp.transpose(wide)
    outer.along(1)

    def head_gain(which):
        total = jnp.zeros((8, dim), F32)
        lane8 = lax.broadcasted_iota(jnp.int32, (8, dim), 1)
        for j in range(16):
            row = info[lax.div(c, 8), j, pl.ds(24 + 8 * which + lax.rem(c, 8), 1), :]
            moved = pltpu.roll(jnp.broadcast_to(row, (8, dim)), 8 * j, 1)
            total = jnp.where(lax.div(lane8, 8) == j, moved, total)
        return total[0:1, :]
    gains = (head_gain(0), head_gain(1))
    heads_out[...] = jnp.concatenate([gains[0], gains[1], jnp.zeros((6, dim), F32)], axis=0)

    def turn(b, _):
        at = span(b * rows, rows)
        for which, factor in ((0, dim ** (-0.5)), (1, 1.0)):
            pick = jnp.where(lane == b + 8 * which, line[...], 0.0)
            inverse = jnp.sum(pick, axis=1, keepdims=True)
            value = raw[at, pl.ds(which * dim, dim)] * inverse * gains[which]
            value = value * trig[0, b] + pltpu.roll(value, dim // 2, 1) * trig[1, b]
            rows3[at, pl.ds(which * dim, dim)] = (value * factor).astype(BF)
        return 0
    lax.fori_loop(0, 8, turn, 0)
    outer.across(0)
    outer.along(2)

    def attend(b, _):
        seq = span(lax.div(b, 4) * 4 * rows, 4 * rows)
        at = span(b * rows, rows)
        scores = contract_last(rows3[at, pl.ds(0, dim)], rows3[seq, pl.ds(dim, dim)])
        here = lax.broadcasted_iota(jnp.int32, scores.shape, 0) + lax.rem(b, 4) * rows
        allowed = lax.broadcasted_iota(jnp.int32, scores.shape, 1) <= here
        scores = jnp.where(allowed, scores, neg_big)
        top = jnp.max(scores, axis=1, keepdims=True)
        weight = jnp.where(allowed, jnp.exp(scores - top), 0.0)
        count = jnp.sum(weight, axis=1, keepdims=True)
        value = jnp.dot(weight.astype(BF), rows3[seq, pl.ds(2 * dim, dim)], preferred_element_type=F32)
        mixed[b] = (value / count).astype(BF)
        lse[b] = jnp.transpose(jnp.broadcast_to(top + jnp.log(count), (rows, dim)))[0:8, :]
        return 0
    lax.fori_loop(0, 8, attend, 0)
    back = Chips(lambda i: mixed.at[i], own_mixed, *chips_sems[5:])
    back.start()
    outer.across(1)
    outer.along(3)
    outer.corner(0)
    outer.across(2)
    back.collect()
    outer.corner(1)
    outer.across(3)
    cots = Gather([Part("rows", cot_ref, cot_out)], csend, crecv)
    cots.start()
    cot_own = pltpu.make_async_copy(cot_ref, cot_out.at[span((z * 4 + s) * rows, rows)], pairs.at[4])
    cot_own.start()
    outer.corner(2)
    back.follow()
    outer.corner(3)
    wo_own.wait()
    for step in range(4):
        outer.ready(step)
    save_wo = pltpu.make_async_copy(wo_all, wo_out, pairs.at[5])
    save_wo.start()
    cots.along(1)
    cots.across(0)
    for j in range(16):
        wide_mixed[:, pl.ds(j * dim, dim)] = own_mixed[j]

    def outward(j, _):
        at = span(j * 512, 512)
        hidden[:, at] = tok_ref[:, at].astype(F32) + jnp.dot(
            wide_mixed[...], wo_all[:, at], preferred_element_type=F32)
        return 0
    lax.fori_loop(0, 4, outward, 0)
    cots.along(2)
    cots.across(1)

    def square_two(r, _):
        at = span(r * 8, 8)
        x = hidden[at, :]
        mean = jnp.sum(x * x, axis=1, keepdims=True) / width
        line[at, :] = jnp.broadcast_to(lax.rsqrt(mean + eps), (8, dim))
        return 0
    lax.fori_loop(0, rows // 8, square_two, 0)

    def normalize_two(j, _):
        at = span(j * dim, dim)
        two[:, at] = (hidden[:, at] * line[...] * info[m, j, 1:2, :]).astype(BF)
        return 0
    lax.fori_loop(0, 16, normalize_two, 0)
    logits = jnp.zeros((16, rows), F32)
    for j in range(16):
        logits = logits + contract_last(info[m, j, 4:20, :].astype(BF), two[:, pl.ds(j * dim, dim)])
        gain_out[0:1, pl.ds(j * dim, dim)] = info[m, j, 0:1, :]
        gain_out[1:2, pl.ds(j * dim, dim)] = info[m, j, 1:2, :]
    gain_out[2:8, :] = jnp.zeros((6, width), F32)
    logits = jnp.exp(logits - jnp.max(logits, axis=0, keepdims=True))
    probs = logits / jnp.sum(logits, axis=0, keepdims=True)
    picks = jnp.transpose(jnp.concatenate(
        [routes_ref[...].astype(F32), jnp.full((rows, dim - 8), -1.0, F32)], axis=1))
    row16 = lax.broadcasted_iota(jnp.int32, (16, rows), 0).astype(F32)
    chosen = jnp.zeros((16, rows), F32)
    for k in range(8):
        chosen = jnp.where(row16 == picks[k : k + 1, :], 1.0, chosen)
    probs_out[...] = probs
    chosen_out[...] = chosen
    share_out[...] = probs * chosen
    cots.along(3)
    cots.corner(0)
    cots.across(2)
    cots.corner(1)
    cots.across(3)
    cots.corner(2)
    cots.corner(3)
    for step in range(4):
        cots.ready(step)
    for copy in (save_n1, save_wo, cot_own):
        copy.wait()
    swap.wait_send()
    for work in (hand, weights, share, back, first, outer, cots):
        work.finish()


def front(ident, *arrays):
    rows, width = arrays[0].shape
    every = 16 * rows
    mine = every // 2
    vmem = pl.BlockSpec(memory_space=pltpu.VMEM)
    hbm = pl.BlockSpec(memory_space=pl.ANY)

    def shape(*sizes, dtype=F32):
        return jax.ShapeDtypeStruct(sizes, dtype)
    return pl.pallas_call(
        front_body,
        out_shape=(
            shape(every, width, dtype=BF),
            shape(every, width, dtype=BF),
            shape(every, width, dtype=BF),
            shape(16, rows, 384, dtype=BF),
            shape(2, 16, 40, 128),
            shape(mine, 256),
            shape(mine, 384, dtype=BF),
            shape(16, 128),
            shape(8, rows, 128, dtype=BF),
            shape(8, 8, rows),
            shape(2, 8, rows, 128),
            shape(16, rows, 128, dtype=BF),
            shape(rows, width),
            shape(rows, width, dtype=BF),
            shape(16, rows),
            shape(16, rows),
            shape(16, rows),
            shape(8, 128),
            shape(8, width),
        ),
        in_specs=[vmem] * 14,
        out_specs=(hbm, hbm, hbm) + (vmem,) * 16,
        scratch_shapes=[
            pltpu.VMEM((40, 128), F32),
            pltpu.VMEM((8, rows, 384), BF),
            pltpu.VMEM((rows, width), BF),
            pltpu.VMEM((every, width), BF),
            pltpu.VMEM((every, width), BF),
            pltpu.VMEM((rows, width), BF),
            pltpu.VMEM((16, 16, 128), F32),
            pltpu.VMEM((16, 128), F32),
            pltpu.VMEM((rows, 128), F32),
        ]
        + [pltpu.SemaphoreType.DMA((1, 12, 4))] * 6
        + [pltpu.SemaphoreType.DMA((16,))] * 4
        + [pltpu.SemaphoreType.DMA((6,))]
        + chips_semaphores() * 2,
        compiler_params=pltpu.CompilerParams(collective_id=ident, has_side_effects=True,
                                             vmem_limit_bytes=56 << 20),
        name="front_%d" % ident,
    )(*arrays)


class Cores:
    def __init__(self, source, target, send, recv, local):
        s, z, m = place()
        self.c, self.m = s * 4 + z, m
        self.high, self.low = lax.div(self.c, 8), lax.rem(self.c, 8)
        self.same = self.high == m
        self.source, self.target, self.send, self.recv, self.local = source, target, send, recv, local

    def dev(self, i):
        j = 8 * self.m + i
        return (lax.div(j, 4), lax.rem(j, 4), self.high)

    def away(self, i):
        return jnp.logical_not(jnp.logical_and(self.same, self.low == i))

    def copy(self, i):
        return remote(self.source.at[i], self.target.at[self.low], self.send.at[i],
                      self.recv.at[self.low], self.dev(i))

    def mine(self):
        return pltpu.make_async_copy(self.source.at[self.low], self.target.at[self.low], self.local.at[0])

    def start(self, low=0, high=8):
        for i in range(low, high):
            pl.when(self.away(i))(lambda i=i: self.copy(i).start())

            def keep():
                self.mine().start()
            pl.when(jnp.logical_not(self.away(i)))(keep)

    def collect(self):
        for i in range(8):
            pl.when(self.away(i))(lambda i=i: remote(
                self.target.at[i], self.target.at[i], self.send.at[0], self.recv.at[i],
                self.dev(i)).wait_recv())
        pl.when(self.same)(lambda: self.mine().wait())

    def finish(self):
        for i in range(8):
            pl.when(self.away(i))(lambda i=i: self.copy(i).wait_send())


def cores_semaphores():
    return [pltpu.SemaphoreType.DMA((8,))] * 2 + [pltpu.SemaphoreType.DMA((1,))]


def meet_all():
    s, z, m = place()
    c = s * 4 + z
    high = lax.div(c, 8)
    for step in range(1, 16):
        j = lax.rem(c + step, 16)
        signal((lax.div(j, 4), lax.rem(j, 4), m))
    signal((s, z, 1 - m))

    def cross():
        for i in range(8):
            j = 8 * m + i
            signal((lax.div(j, 4), lax.rem(j, 4), high))
        pl.semaphore_wait(pltpu.get_barrier_semaphore(), 24)
    pl.when(high != m)(cross)
    pl.when(high == m)(lambda: pl.semaphore_wait(pltpu.get_barrier_semaphore(), 16))


def rear_body(back_ref, prob_ref, probs_ref, chosen_ref, two_ref, out_ref, cot_ref, info,
              mixed_ref, rows3, raw, squares, lse, trig, gains, w3, tok_ref, gain_ref,
              wo_ref, n1_ref, moe_ref,
              gn_out, moe_out, q_out, k_out, v_out, out_grad, tok_out, tail_out,
              got, ga_ref, hidden_ref, wo_half, n1_half, moe, gn_part, mixed_line, ga_blocks, ga_plane, gm_send, gm, wsend, backs,
              dq, dk, dv, sums, gathered, line, dots, tail, out_mine, out_all,
              a0, a1, a2, a3, a4, a5, a6, a7, asend, arecv,
              b0, b1, b2, b3, b4, b5, b6, b7, bsend, brecv,
              msend, mrecv, csend, crecv, hsend, hrecv, tsend, trecv, psend, precv, osend, orecv, load, *rest):
    s, z, m = place()
    c = s * 4 + z
    pn = (s, z, 1 - m)
    rows, width = tok_ref.shape
    cut = width // 2
    dim = 128
    factor = dim ** (-0.5)
    loads = [
        pltpu.make_async_copy(wo_ref.at[span(m * cut, cut), :], wo_half, load.at[0]),
        pltpu.make_async_copy(moe_ref, moe, load.at[1]),
        pltpu.make_async_copy(n1_ref.at[:, span(m * cut, cut)], n1_half, load.at[2]),
        pltpu.make_async_copy(mixed_ref, mixed_line.at[span(m * cut, cut), span(z * dim, dim)], load.at[3]),
    ]
    for copy in loads:
        copy.start()
    prob = jnp.concatenate(
        [prob_ref[0, j, 0:1, :] + prob_ref[1, j, 0:1, :] for j in range(16)], axis=0)
    prob = prob * chosen_ref[...]
    probs = probs_ref[...]
    logits = (probs * (prob - jnp.sum(probs * prob, axis=0, keepdims=True))).astype(BF)
    tail[...] = jnp.zeros_like(tail)
    for j in range(16):
        at = pl.ds(j * dim, dim)
        tail[j, 3:19, :] = jnp.dot(logits, two_ref[:, at], preferred_element_type=F32)
        hidden_ref[:, at] = back_ref[:, at].astype(F32) + contract_first(
            logits, info[m, j, 4:20, :].astype(BF))

    def second_norm(r, acc):
        at = span(r * 16, 16)
        x = out_ref[at, :]
        grad = hidden_ref[at, :]
        inverse = lax.rsqrt(jnp.sum(x * x, axis=1, keepdims=True) / width + eps)
        scaled = grad * gain_ref[1:2, :]
        dot = jnp.sum(x * scaled, axis=1, keepdims=True) / width
        value = cot_ref[at, :].astype(F32) + (
            inverse * scaled - x * (inverse * inverse * inverse * dot))
        hidden_ref[at, :] = value
        ga_ref[at, :] = value.astype(BF)
        part = grad * x * inverse
        return acc + part[0:8] + part[8:16]
    acc = lax.fori_loop(0, rows // 16, second_norm, jnp.zeros((8, width), F32))
    acc = jnp.sum(acc, axis=0, keepdims=True)
    for j in range(16):
        tail[j, 1:2, :] = acc[:, j * dim : (j + 1) * dim]
    meet_all()
    lane = lax.broadcasted_iota(jnp.int32, (rows, dim), 1)
    order = far_planes(z)
    give = Cores(gm_send, gm, *rest[:3])
    loads[0].wait()
    for t in range(2):
        value = contract_last(ga_ref[...], wo_half[pl.ds(t * 512, 512), :]).astype(BF)
        for i in range(4):
            gm_send[t * 4 + i] = value[:, i * dim : (i + 1) * dim]
        give.start(t * 4, t * 4 + 4)
    strip = Line([Part("line", mixed_ref, mixed_line)], msend, mrecv)
    spread = Spread([Part("cols", ga_blocks, ga_plane)], csend, crecv)
    loads[1].wait()
    outer = Reduce(True, True, moe, moe, moe_out, (a0, a1, a2, a3, a4, a5, a6, a7), (asend, arecv))
    inner = Reduce(False, True, gn_part, gn_part, gn_out, (b0, b1, b2, b3, b4, b5, b6, b7), (bsend, brecv))
    for at in order:
        outer.swap(at)

    wide = jnp.concatenate(
        [lax.rsqrt(squares[...] / width + eps), jnp.zeros((rows - 16, dim), F32)], axis=0)
    line[...] = jnp.transpose(wide)
    dk[...] = jnp.zeros_like(dk)
    dv[...] = jnp.zeros_like(dv)
    outer.first(order[0])
    outer.first(order[1])
    give.collect()
    outer.first(order[2])
    outer.first(order[3])

    def attend(b, _):
        seq = span(lax.div(b, 4) * 4 * rows, 4 * rows)
        at = span(b * rows, rows)
        query = rows3[at, pl.ds(0, dim)]
        key = rows3[seq, pl.ds(dim, dim)]
        value = rows3[seq, pl.ds(2 * dim, dim)]
        grad = gm[b]
        top = jnp.transpose(jnp.broadcast_to(lse[b, 0:1, :], (rows, dim)))[:, 0:1]
        delta = jnp.sum(grad.astype(F32) * mixed_ref[at, :].astype(F32), axis=1, keepdims=True)
        scores = contract_last(query, key)
        here = lax.broadcasted_iota(jnp.int32, scores.shape, 0) + lax.rem(b, 4) * rows
        allowed = lax.broadcasted_iota(jnp.int32, scores.shape, 1) <= here
        prob = jnp.where(allowed, jnp.exp(jnp.where(allowed, scores, neg_big) - top), 0.0)
        back = (prob * (contract_last(grad, value) - delta)).astype(BF)
        dv[seq, :] += contract_first(prob.astype(BF), grad)
        dk[seq, :] += contract_first(back, query)
        dq[at, :] = jnp.dot(back, key, preferred_element_type=F32) * factor
        return 0
    lax.fori_loop(0, 4, attend, 0)
    outer.second(order[0])
    outer.second(order[1])
    lax.fori_loop(4, 8, attend, 0)

    def column(source, r):
        return jnp.sum(jnp.where(lane == r, source, 0.0), axis=1, keepdims=True)

    def unturn(b, carry):
        total, gain_q, gain_k = carry
        at = span(b * rows, rows)
        out = []
        for which, grads in ((0, dq), (1, dk)):
            value = grads[at, :]
            value = value * trig[0, b] + pltpu.roll(value * trig[1, b], dim // 2, 1)
            plain = raw[at, pl.ds(which * dim, dim)]
            unit = plain * column(line[...], b + 8 * which)
            out.append(jnp.sum(value * unit, axis=0, keepdims=True))
            value = value * gains[which : which + 1, :]
            grads[at, :] = value
            dot = jnp.sum(plain * value, axis=1, keepdims=True)
            total = jnp.where(lane == b + 8 * which, dot, total)
        return total, gain_q + out[0], gain_k + out[1]
    zero = jnp.zeros((1, dim), F32)
    total, gain_q, gain_k = lax.fori_loop(0, 8, unturn, (jnp.zeros((rows, dim), F32), zero, zero))
    for j in range(16):
        tail[j, 2:3, :] = gain_q
        tail[j, 19:20, :] = gain_k
    sums[...] = jnp.transpose(total)[0:16, :]
    hand = Hand(lambda j: sums, lambda j: gathered.at[j], hsend, hrecv)
    hand.start()
    gathered[c] = sums[...]
    strip.start()
    for p in range(4):
        for q in range(4):
            ga_blocks[p, :, pl.ds(q * dim, dim)] = ga_ref[:, pl.ds((q * 4 + p) * dim, dim)]
    spread.start()
    ga_plane[span(c * rows, rows), :] = ga_blocks[z]
    outer.second(order[2])
    outer.third(order[0], 0)
    outer.second(order[3])
    outer.third(order[1], 1)
    hand.collect()
    summed = lax.fori_loop(1, 16, lambda j, acc: acc + gathered[j], gathered[0])
    dots[...] = jnp.transpose(jnp.concatenate([summed, jnp.zeros((rows - 16, dim), F32)], axis=0))

    def finish_rows(b, _):
        at = span(b * rows, rows)
        base = span((lax.rem(b, 4) * 4 + 2 * m + lax.div(b, 4)) * rows, rows)
        for which, grads in ((0, dq), (1, dk)):
            inverse = column(line[...], b + 8 * which)
            dot = column(dots[...], b + 8 * which)
            value = inverse * grads[at, :] - raw[at, pl.ds(which * dim, dim)] * (
                inverse * inverse * inverse * dot / width)
            backs[base, pl.ds(which * dim, dim)] = value.astype(BF)
        backs[base, pl.ds(2 * dim, dim)] = dv[at, :].astype(BF)
        return 0
    lax.fori_loop(0, 8, finish_rows, 0)

    def pair(at, core):
        part = backs.at[span((at * 4 + 2 * core) * rows, 2 * rows), :]
        return remote(part, part, psend.at[at], precv.at[at], pn)
    for at in range(4):
        pair(at, m).start()
    outer.third(order[2], 2)
    for at in range(4):
        pair(at, 1 - m).wait_recv()
    for at in order:
        here = span(at * 4 * rows, 4 * rows)
        gn_part[here, :] = contract_last(
            backs[here, :], w3[span(m * 8, 8)].reshape(cut, 3 * dim)).astype(BF)
        inner.first(at)
    outer.keep()
    strip.along(1)
    spread.along(1)
    loads[2].wait()

    def weight_tile(t):
        value = contract_first(n1_half[:, pl.ds(t * 256, 256)], backs[...]).astype(BF)
        wsend[2 * t] = value[:rows]
        wsend[2 * t + 1] = value[rows:]
    weight_tile(0)
    weight_tile(1)
    inner.second(order[0])
    weight_tile(2)
    inner.third(order[0], 0)
    inner.second(order[1])
    weight_tile(3)
    outer.close()
    weights = Cores(wsend, got, *rest[3:6])
    weights.start()
    strip.along(2)
    spread.along(2)
    spread.across(0)
    inner.third(order[1], 1)
    inner.second(order[2])
    inner.third(order[2], 2)
    inner.second(order[3])
    inner.keep()
    strip.along(3)
    spread.along(3)
    spread.across(1)
    spread.corner(0)
    inner.close()
    inner.landing()

    def last(r, acc):
        at = span(r * 16, 16)
        x = tok_ref[at, :].astype(F32)
        grad = gn_out[at, :].astype(F32)
        inverse = lax.rsqrt(jnp.sum(x * x, axis=1, keepdims=True) / width + eps)
        scaled = grad * gain_ref[0:1, :]
        dot = jnp.sum(x * scaled, axis=1, keepdims=True) / width
        tok_out[at, :] = hidden_ref[at, :] + inverse * scaled - x * (inverse * inverse * inverse * dot)
        part = grad * x * inverse
        return acc + part[0:8] + part[8:16]
    acc = lax.fori_loop(0, rows // 16, last, jnp.zeros((8, width), F32))
    acc = jnp.sum(acc, axis=0, keepdims=True)
    for j in range(16):
        tail[j, 0:1, :] = acc[:, j * dim : (j + 1) * dim]
    finale = Hand(lambda j: tail.at[j], lambda j: tail_out.at[m, j], tsend, trecv)
    finale.start()
    tail_out[m, c] = tail[c]
    spread.across(2)
    spread.corner(1)
    spread.across(3)
    spread.corner(2)
    spread.corner(3)
    loads[3].wait()
    for step in (1, 2, 3):
        strip.ready(step)
    strip_own = mixed_line.at[span((1 - m) * cut, cut), span(z * dim, dim)]
    strip.landed(0, strip.PO, z, strip_own)
    for step in range(4):
        spread.ready(step)

    value = contract_first(mixed_line[:, span(m * 256, 256)], ga_plane[...]).astype(BF)
    for q in range(4):
        out_mine[q] = value[:, q * dim : (q + 1) * dim]
    high = lax.div(c, 8)
    lower = lax.rem(s, 2)
    cross = remote(out_mine, out_all.at[m], osend.at[0], orecv.at[0], pn)

    def landing(q, core):
        return out_grad.at[q, core]

    def away(step, core):
        q = (None, flip_x(s), flip_y(s), 3 - s)[step]
        source = out_mine if core is None else out_all.at[1 - m]
        who = m if core is None else 1 - m
        at = step * 2 + (0 if core is None else 1)
        return remote(source.at[q], landing(lower, who), osend.at[at], orecv.at[at], (q, z, m))

    def lead():
        for step in (1, 2, 3):
            away(step, None).start()
        out_grad[lower, m] = out_mine[s]
        remote(out_all.at[1 - m], out_all.at[1 - m], osend.at[0], orecv.at[0], pn).wait_recv()
        for step in (1, 2, 3):
            away(step, 1).start()
        out_grad[lower, 1 - m] = out_all[1 - m, s]
    pl.when(high == m)(lead)
    pl.when(high != m)(lambda: cross.start())
    finale.collect()
    pair_tail = remote(tail_out.at[m], tail_out.at[m], osend.at[8], orecv.at[8], pn)
    pair_tail.start()
    weights.collect()
    for j in range(8):
        for n, ref in enumerate((q_out, k_out, v_out)):
            ref[:, pl.ds(j * dim, dim)] = got[j, :, pl.ds(n * dim, dim)].astype(F32)

    def arrive(step):
        q = (None, flip_x(s), flip_y(s), 3 - s)[step]

        def take():
            for second in (0, 1):
                who = 1 - m if second else m
                at = step * 2 + second
                target = landing(lax.rem(q, 2), who)
                remote(target, target, osend.at[at], orecv.at[at], pn).wait_recv()
        pl.when(lax.div(q, 2) == m)(take)
    for step in (1, 2, 3):
        arrive(step)
    other = tail_out.at[1 - m]
    remote(other, other, osend.at[8], orecv.at[8], pn).wait_recv()
    pair_tail.wait_send()
    pl.when(high != m)(lambda: cross.wait_send())

    def sent():
        for step in (1, 2, 3):
            away(step, None).wait_send()
            away(step, 1).wait_send()
    pl.when(high == m)(sent)
    outer.landing()
    for at in range(4):
        pair(at, m).wait_send()
    for work in (give, outer, inner, hand, finale, weights, strip, spread):
        work.finish()


def rear(ident, *arrays):
    rows, width = arrays[0].shape
    every = 16 * rows
    cut = width // 2
    vmem = pl.BlockSpec(memory_space=pltpu.VMEM)
    hbm = pl.BlockSpec(memory_space=pl.ANY)
    return pl.pallas_call(
        rear_body,
        out_shape=(
            jax.ShapeDtypeStruct((rows, width), BF),
            jax.ShapeDtypeStruct((rows, width), BF),
            jax.ShapeDtypeStruct((rows, cut), F32),
            jax.ShapeDtypeStruct((rows, cut), F32),
            jax.ShapeDtypeStruct((rows, cut), F32),
            jax.ShapeDtypeStruct((2, 2, 256, 128), BF),
            jax.ShapeDtypeStruct((rows, width), F32),
            jax.ShapeDtypeStruct((2, 16, 24, 128), F32),
        ),
        in_specs=[vmem] * 18 + [hbm] * 3,
        out_specs=(vmem,) * 8,
        scratch_shapes=[
            pltpu.VMEM((8, rows, 384), BF),
            pltpu.VMEM((rows, width), BF),
            pltpu.VMEM((rows, width), F32),
            pltpu.VMEM((cut, width), BF),
            pltpu.VMEM((every, cut), BF),
            pltpu.VMEM((every, width), BF),
            pltpu.VMEM((every, cut), BF),
            pltpu.VMEM((every, 512), BF),
            pltpu.VMEM((4, rows, 512), BF),
            pltpu.VMEM((every, 512), BF),
            pltpu.VMEM((8, rows, 128), BF),
            pltpu.VMEM((8, rows, 128), BF),
            pltpu.VMEM((8, rows, 384), BF),
            pltpu.VMEM((every, 384), BF),
            pltpu.VMEM((every // 2, 128), F32),
            pltpu.VMEM((every // 2, 128), F32),
            pltpu.VMEM((every // 2, 128), F32),
            pltpu.VMEM((16, 128), F32),
            pltpu.VMEM((16, 16, 128), F32),
            pltpu.VMEM((rows, 128), F32),
            pltpu.VMEM((rows, 128), F32),
            pltpu.VMEM((16, 24, 128), F32),
            pltpu.VMEM((4, 256, 128), BF),
            pltpu.VMEM((2, 4, 256, 128), BF),
        ]
        + reduce_buffers(True, rows, cut)
        + reduce_buffers(False, rows, cut)
        + [pltpu.SemaphoreType.DMA((1, 12, 4))] * 4
        + [pltpu.SemaphoreType.DMA((16,))] * 4
        + [pltpu.SemaphoreType.DMA((4,))] * 2
        + [pltpu.SemaphoreType.DMA((9,))] * 2
        + [pltpu.SemaphoreType.DMA((4,))]
        + cores_semaphores()
        + cores_semaphores(),
        compiler_params=pltpu.CompilerParams(collective_id=ident, has_side_effects=True,
                                             vmem_limit_bytes=66900000),
        name="rear_%d" % ident,
    )(*arrays)


HEADS = 16
HEAD_DIM = 128


eps = 1e-05
neg_big = -1e30


def rms_scale(rows, gain):
    return rows * lax.rsqrt(jnp.mean(rows * rows, axis=-1, keepdims=True) + eps) * gain


def rope_tables(positions):
    half = HEAD_DIM // 2
    freq = 10000.0 ** (-(jnp.arange(half).astype(jnp.float32) * 2.0 / HEAD_DIM))
    angle = positions.astype(jnp.float32)[:, None] * freq[None, :]
    return (jnp.cos(angle), jnp.sin(angle))


def rope_turn(normed, cosine, sine, factor):
    count = normed.shape[0]
    heads = normed.shape[1]
    width = normed.shape[2]
    first = normed[..., : width // 2]
    second = normed[..., width // 2 :]
    cos_rows = cosine[:, None, :]
    sin_rows = sine[:, None, :]
    turned = jnp.concatenate(
        [first * cos_rows - second * sin_rows, second * cos_rows + first * sin_rows], axis=-1
    )
    return (turned * factor).reshape(count, heads * width)


def contract_last(left, right):
    return lax.dot_general(
        left, right, (((1,), (1,)), ((), ())), preferred_element_type=jnp.float32
    )


def contract_first(left, right):
    return lax.dot_general(
        left, right, (((0,), (0,)), ((), ())), preferred_element_type=jnp.float32
    )


def sum_halves(part):
    return lax.psum(part.astype(jnp.bfloat16), "mp").astype(jnp.float32)


def general_body(
    tokens,
    positions,
    routes,
    cotangent,
    attention_gain,
    query_weight,
    key_weight,
    value_weight,
    query_gain,
    key_gain,
    output_weight,
    ffn_gain,
    router_weight,
    gate_weight,
    up_weight,
    down_weight,
):
    gathered = (
        lax.all_gather(query_weight, ("seq", "ctx"), axis=0, tiled=True),
        lax.all_gather(key_weight, ("seq", "ctx"), axis=0, tiled=True),
        lax.all_gather(value_weight, ("seq", "ctx"), axis=0, tiled=True),
        lax.all_gather(output_weight, ("seq", "ctx"), axis=1, tiled=True),
        lax.all_gather(router_weight, ("seq", "ctx"), axis=0, tiled=True),
        lax.all_gather(attention_gain, ("seq", "ctx"), axis=0, tiled=True),
        lax.all_gather(ffn_gain, ("seq", "ctx"), axis=0, tiled=True),
        lax.all_gather(query_gain, ("seq", "ctx"), axis=1, tiled=True),
        lax.all_gather(key_gain, ("seq", "ctx"), axis=1, tiled=True),
    )
    (
        query_full,
        key_full,
        value_full,
        output_full,
        router_full,
        gain_one_half,
        gain_two_half,
        query_gain_full,
        key_gain_full,
    ) = gathered
    rows = tokens.shape[1]
    width = tokens.shape[2]
    heads_here = query_gain.shape[0]
    local_width = query_weight.shape[1]
    all_columns = HEADS * HEAD_DIM
    factor = HEAD_DIM ** (-0.5)
    flat = tokens[0].astype(jnp.float32)
    grad_top = cotangent[0].astype(jnp.float32)
    gain_one = gain_one_half.astype(jnp.float32)
    gain_two = gain_two_half.astype(jnp.float32)
    query_gain_f = query_gain_full.astype(jnp.float32)
    key_gain_f = key_gain_full.astype(jnp.float32)
    normed_one = rms_scale(flat, gain_one).astype(jnp.bfloat16)
    query_raw = jnp.dot(normed_one, query_full, preferred_element_type=jnp.float32)
    key_raw = jnp.dot(normed_one, key_full, preferred_element_type=jnp.float32)
    value_rows = jnp.dot(normed_one, value_full, preferred_element_type=jnp.float32).astype(
        jnp.bfloat16
    )
    query_sq, key_sq = lax.psum(
        (jnp.sum(query_raw * query_raw, axis=-1), jnp.sum(key_raw * key_raw, axis=-1)), "mp"
    )
    query_inv = lax.rsqrt(query_sq / all_columns + eps)
    key_inv = lax.rsqrt(key_sq / all_columns + eps)
    query_unit = (query_raw * query_inv[:, None]).reshape(rows, heads_here, HEAD_DIM)
    key_unit = (key_raw * key_inv[:, None]).reshape(rows, heads_here, HEAD_DIM)
    cosine, sine = rope_tables(positions[0])
    query_rows = rope_turn(query_unit * query_gain_f, cosine, sine, factor).astype(jnp.bfloat16)
    key_rows = rope_turn(key_unit * key_gain_f, cosine, sine, 1.0).astype(jnp.bfloat16)
    keys_all, values_all = (
        lax.all_gather(key_rows, "ctx", axis=0, tiled=True),
        lax.all_gather(value_rows, "ctx", axis=0, tiled=True),
    )
    ctx_count = lax.axis_size("ctx")
    length = rows * ctx_count
    first_row = lax.axis_index("ctx") * rows
    last_row = first_row + rows - 1
    query_pos = first_row + jnp.arange(rows, dtype=jnp.int32)
    block = min(512, length)
    blocks = length // block
    query3 = query_rows.reshape(rows, heads_here, HEAD_DIM)

    def forward_block(carry, index):
        start = index * block

        def forward_work(state):
            top, total, acc = state
            keys = lax.dynamic_slice_in_dim(keys_all, start, block, 0).reshape(
                block, heads_here, HEAD_DIM
            )
            values = lax.dynamic_slice_in_dim(values_all, start, block, 0).reshape(
                block, heads_here, HEAD_DIM
            )
            scores = jnp.einsum("qhd,khd->hqk", query3, keys, preferred_element_type=jnp.float32)
            allowed = (start + jnp.arange(block, dtype=jnp.int32))[None, :] <= query_pos[:, None]
            scores = jnp.where(allowed[None], scores, neg_big)
            new_top = jnp.maximum(top, jnp.max(scores, axis=-1))
            weights = jnp.where(allowed[None], jnp.exp(scores - new_top[..., None]), 0.0)
            fade = jnp.exp(top - new_top)
            total = total * fade + jnp.sum(weights, axis=-1)
            acc = acc * fade[..., None] + jnp.einsum(
                "hqk,khd->hqd",
                weights.astype(jnp.bfloat16),
                values,
                preferred_element_type=jnp.float32,
            )
            return (new_top, total, acc)

        return (lax.cond(start <= last_row, forward_work, lambda state: state, carry), None)

    start_state = (
        jnp.full((heads_here, rows), neg_big, jnp.float32),
        jnp.zeros((heads_here, rows), jnp.float32),
        jnp.zeros((heads_here, rows, HEAD_DIM), jnp.float32),
    )
    (top, total, acc), _ = lax.scan(forward_block, start_state, jnp.arange(blocks, dtype=jnp.int32))
    mixed = (
        (acc / total[..., None]).transpose(1, 0, 2).reshape(rows, local_width).astype(jnp.bfloat16)
    )
    lse = top + jnp.log(total)
    attn = lax.psum(jnp.dot(mixed, output_full, preferred_element_type=jnp.float32), "mp")
    hidden = flat + attn
    normed_two = rms_scale(hidden, gain_two).astype(jnp.bfloat16)
    logits = jnp.dot(normed_two, router_full, preferred_element_type=jnp.float32)
    probs = jax.nn.softmax(logits, axis=-1)
    route_rows = routes[0]
    experts = router_full.shape[1]
    top_count = route_rows.shape[1]
    choose = (route_rows[:, :, None] == jnp.arange(experts, dtype=jnp.int32)[None, None, :]).astype(
        jnp.float32
    )
    share = jnp.sum(choose * probs[:, None, :], axis=-1)
    assign = rows * top_count
    capacity = assign * 3 // (2 * experts)
    expert_of = route_rows.reshape(assign)
    onehot = (expert_of[:, None] == jnp.arange(experts, dtype=jnp.int32)[None, :]).astype(jnp.int32)
    rank = jnp.sum(onehot * jnp.cumsum(onehot, axis=0), axis=1) - 1
    place = expert_of * capacity + rank
    table = (
        jnp.full((experts * capacity,), assign, jnp.int32)
        .at[place]
        .set(jnp.arange(assign, dtype=jnp.int32))
    )
    valid = table < assign
    safe = jnp.minimum(table, assign - 1)
    outgoing = jnp.where(
        valid[:, None], normed_two[safe // top_count], jnp.zeros((), jnp.bfloat16)
    ).reshape(experts, capacity, width)
    gate_here = gate_weight[0]
    up_here = up_weight[0]
    down_here = down_weight[0]
    received = lax.all_to_all(outgoing, ("seq", "ctx"), split_axis=0, concat_axis=0, tiled=True)
    sources = received.shape[0]
    slots = received.shape[1]
    inputs = received.reshape(sources * slots, width)
    gate = jnp.dot(inputs, gate_here, preferred_element_type=jnp.float32)
    up = jnp.dot(inputs, up_here, preferred_element_type=jnp.float32)
    act = (gate * jax.nn.sigmoid(gate) * up).astype(jnp.bfloat16)
    result = jnp.dot(act, down_here, preferred_element_type=jnp.float32).reshape(
        sources, slots, width
    )
    result = sum_halves(result)
    returned = lax.all_to_all(
        result.astype(jnp.bfloat16), ("seq", "ctx"), split_axis=0, concat_axis=0, tiled=True
    ).astype(result.dtype)
    per_assign = returned.reshape(experts * capacity, width)[place].reshape(rows, top_count, width)
    combined = jnp.sum(share[:, :, None] * per_assign, axis=1)
    layer_output = (hidden + combined).astype(jnp.bfloat16)[None]
    grad_share_part = jnp.sum(per_assign * grad_top[:, None, :], axis=-1)
    grad_result = (
        (share[:, :, None] * grad_top[:, None, :]).astype(jnp.bfloat16).reshape(assign, width)
    )
    grad_slots = jnp.where(valid[:, None], grad_result[safe], jnp.zeros((), jnp.bfloat16)).reshape(
        experts, capacity, width
    )
    incoming_rows, incoming_grads = (
        lax.all_to_all(outgoing, ("seq", "ctx"), split_axis=0, concat_axis=0, tiled=True),
        lax.all_to_all(grad_slots, ("seq", "ctx"), split_axis=0, concat_axis=0, tiled=True),
    )
    sources = incoming_rows.shape[0]
    inputs = incoming_rows.reshape(sources * capacity, width)
    grads_in = incoming_grads.reshape(sources * capacity, width)
    gate = jnp.dot(inputs, gate_here, preferred_element_type=jnp.float32)
    up = jnp.dot(inputs, up_here, preferred_element_type=jnp.float32)
    sig = jax.nn.sigmoid(gate)
    act = (gate * sig * up).astype(jnp.bfloat16)
    grad_act = contract_last(grads_in, down_here)
    down_grad = contract_first(act, grads_in)
    grad_gate = (grad_act * up * sig * (1.0 + gate * (1.0 - sig))).astype(jnp.bfloat16)
    grad_up = (grad_act * gate * sig).astype(jnp.bfloat16)
    gate_grad = contract_first(inputs, grad_gate)
    up_grad = contract_first(inputs, grad_up)
    back = (contract_last(grad_gate, gate_here) + contract_last(grad_up, up_here)).reshape(
        sources, capacity, width
    )
    back_home = lax.all_to_all(
        back.astype(jnp.bfloat16), ("seq", "ctx"), split_axis=0, concat_axis=0, tiled=True
    ).astype(back.dtype)
    moe_part = jnp.sum(
        back_home.reshape(experts * capacity, width)[place].reshape(rows, top_count, width), axis=1
    )
    share_send = jnp.zeros_like(grad_share_part)
    grad_norm_moe, share_summed = lax.psum((moe_part, share_send), "mp")
    grad_share = grad_share_part + share_summed
    grad_prob = jnp.sum(choose * grad_share[:, :, None], axis=1)
    grad_logits = (probs * (grad_prob - jnp.sum(probs * grad_prob, axis=-1, keepdims=True))).astype(
        jnp.bfloat16
    )
    router_grad = contract_first(normed_two, grad_logits)
    grad_normed_two = grad_norm_moe + contract_last(grad_logits, router_full)
    _, pull_two = jax.vjp(rms_scale, hidden, gain_two)
    grad_hidden_part, ffn_gain_grad = pull_two(grad_normed_two)
    grad_hidden = grad_top + grad_hidden_part
    grad_attn = grad_hidden.astype(jnp.bfloat16)
    output_grad = contract_first(mixed, grad_attn)
    grad_mixed = contract_last(grad_attn, output_full).astype(jnp.bfloat16)
    grad3 = grad_mixed.reshape(rows, heads_here, HEAD_DIM)
    delta = jnp.sum(
        grad3.astype(jnp.float32) * mixed.reshape(rows, heads_here, HEAD_DIM).astype(jnp.float32),
        axis=-1,
    ).T

    def backward_block(query_acc, index):
        start = index * block

        def backward_work(acc_now):
            keys = lax.dynamic_slice_in_dim(keys_all, start, block, 0).reshape(
                block, heads_here, HEAD_DIM
            )
            values = lax.dynamic_slice_in_dim(values_all, start, block, 0).reshape(
                block, heads_here, HEAD_DIM
            )
            scores = jnp.einsum("qhd,khd->hqk", query3, keys, preferred_element_type=jnp.float32)
            allowed = (start + jnp.arange(block, dtype=jnp.int32))[None, :] <= query_pos[:, None]
            scores = jnp.where(allowed[None], scores, neg_big)
            prob = jnp.where(allowed[None], jnp.exp(scores - lse[..., None]), 0.0)
            value_part = jnp.einsum(
                "hqk,qhd->khd", prob.astype(jnp.bfloat16), grad3, preferred_element_type=jnp.float32
            )
            grad_prob_block = jnp.einsum(
                "qhd,khd->hqk", grad3, values, preferred_element_type=jnp.float32
            )
            grad_scores = (prob * (grad_prob_block - delta[..., None])).astype(jnp.bfloat16)
            acc_now = acc_now + jnp.einsum(
                "hqk,khd->hqd", grad_scores, keys, preferred_element_type=jnp.float32
            )
            key_part = jnp.einsum(
                "hqk,qhd->khd", grad_scores, query3, preferred_element_type=jnp.float32
            )
            return (
                acc_now,
                key_part.reshape(block, local_width),
                value_part.reshape(block, local_width),
            )

        def skip(acc_now):
            empty = jnp.zeros((block, local_width), jnp.float32)
            return (acc_now, empty, empty)

        acc_next, key_part, value_part = lax.cond(start <= last_row, backward_work, skip, query_acc)
        return (acc_next, (key_part, value_part))

    query_acc, (key_blocks, value_blocks) = lax.scan(
        backward_block,
        jnp.zeros((heads_here, rows, HEAD_DIM), jnp.float32),
        jnp.arange(blocks, dtype=jnp.int32),
    )
    grad_keys, grad_values = (
        lax.psum_scatter(
            key_blocks.reshape(length, local_width).astype(jnp.bfloat16),
            "ctx",
            scatter_dimension=0,
            tiled=True,
        ).astype(jnp.float32),
        lax.psum_scatter(
            value_blocks.reshape(length, local_width).astype(jnp.bfloat16),
            "ctx",
            scatter_dimension=0,
            tiled=True,
        ).astype(jnp.float32),
    )
    grad_queries = query_acc.transpose(1, 0, 2).reshape(rows, local_width)
    _, pull_query = jax.vjp(
        lambda normed: rope_turn(normed, cosine, sine, factor), query_unit * query_gain_f
    )
    (grad_query_normed,) = pull_query(grad_queries)
    _, pull_key = jax.vjp(
        lambda normed: rope_turn(normed, cosine, sine, 1.0), key_unit * key_gain_f
    )
    (grad_key_normed,) = pull_key(grad_keys)
    query_gain_grad = jnp.sum(grad_query_normed * query_unit, axis=0)
    key_gain_grad = jnp.sum(grad_key_normed * key_unit, axis=0)
    query_scaled = (grad_query_normed * query_gain_f).reshape(rows, local_width)
    key_scaled = (grad_key_normed * key_gain_f).reshape(rows, local_width)
    query_dot, key_dot = lax.psum(
        (jnp.sum(query_raw * query_scaled, axis=-1), jnp.sum(key_raw * key_scaled, axis=-1)), "mp"
    )
    grad_query_raw = (
        query_inv[:, None] * query_scaled
        - query_raw * (query_inv * query_inv * query_inv * query_dot / all_columns)[:, None]
    )
    grad_key_raw = (
        key_inv[:, None] * key_scaled
        - key_raw * (key_inv * key_inv * key_inv * key_dot / all_columns)[:, None]
    )
    query_half = grad_query_raw.astype(jnp.bfloat16)
    key_half = grad_key_raw.astype(jnp.bfloat16)
    value_half = grad_values.astype(jnp.bfloat16)
    query_grad = contract_first(normed_one, query_half)
    key_grad = contract_first(normed_one, key_half)
    value_grad = contract_first(normed_one, value_half)
    normed_part = (
        contract_last(query_half, query_full)
        + contract_last(key_half, key_full)
        + contract_last(value_half, value_full)
    )
    grad_normed_one = lax.psum(normed_part.astype(jnp.bfloat16), "mp").astype(jnp.float32)
    _, pull_one = jax.vjp(rms_scale, flat, gain_one)
    grad_flat_part, attention_gain_grad = pull_one(grad_normed_one)
    tokens_grad = (grad_hidden + grad_flat_part)[None]
    owned = (
        lax.psum_scatter(query_grad, ("seq", "ctx"), scatter_dimension=0, tiled=True),
        lax.psum_scatter(key_grad, ("seq", "ctx"), scatter_dimension=0, tiled=True),
        lax.psum_scatter(value_grad, ("seq", "ctx"), scatter_dimension=0, tiled=True),
        lax.psum_scatter(output_grad, ("seq", "ctx"), scatter_dimension=1, tiled=True),
        lax.psum_scatter(router_grad, ("seq", "ctx"), scatter_dimension=0, tiled=True),
        lax.psum_scatter(attention_gain_grad, ("seq", "ctx"), scatter_dimension=0, tiled=True),
        lax.psum_scatter(ffn_gain_grad, ("seq", "ctx"), scatter_dimension=0, tiled=True),
        lax.psum_scatter(query_gain_grad, ("seq", "ctx"), scatter_dimension=1, tiled=True),
        lax.psum_scatter(key_gain_grad, ("seq", "ctx"), scatter_dimension=1, tiled=True),
    )
    (
        query_owned,
        key_owned,
        value_owned,
        output_owned,
        router_owned,
        gain_one_owned,
        gain_two_owned,
        query_gain_owned,
        key_gain_owned,
    ) = owned
    return (
        layer_output,
        tokens_grad,
        gain_one_owned,
        query_owned,
        key_owned,
        value_owned,
        query_gain_owned,
        key_gain_owned,
        output_owned,
        gain_two_owned,
        router_owned,
        gate_grad[None],
        up_grad[None],
        down_grad[None],
    )


def fast_body(
    tokens, positions, routes, cotangent, attention_gain, query_weight, key_weight, value_weight,
    query_gain, key_gain, output_weight, ffn_gain, router_weight, gate_weight, up_weight,
    down_weight,
):
    s, z, m = place()
    c = s * 4 + z
    rows, width = tokens.shape[1:]
    cut = width // 2
    half = np.arange(HEAD_DIM // 2).astype(np.float32)
    freq = np.float32(10000.0) ** (-(half * np.float32(2.0) / np.float32(HEAD_DIM)))
    freq = jnp.asarray(np.tile(freq, (8, 2)), F32)
    (normed, out_full, all_top, weights3, info, raw, rows3, squares, mixed, lse, trig, _, hidden,
     normed_two, probs, chosen, share, head_gains, gains) = front(
        0, tokens[0], attention_gain.reshape(1, rows), ffn_gain.reshape(1, rows), positions,
        router_weight.T, query_gain, key_gain, routes[0], query_weight, key_weight, value_weight,
        output_weight, cotangent[0], freq)
    grad_two, prob_out, moe, gate_grad, up_grad, down_grad = experts(
        5, normed_two, share, all_top, gate_weight[0], up_weight[0], down_weight[0])
    _, moe_sum, query_grad, key_grad, value_grad, output_grad, tokens_grad, tail = rear(
        6, grad_two, prob_out, probs, chosen, normed_two, hidden, cotangent[0], info,
        mixed.reshape(8 * rows, HEAD_DIM), rows3, raw, squares, lse, trig, head_gains, weights3,
        tokens[0], gains, out_full, normed, moe)
    layer_output = (hidden + moe_sum.astype(F32)).astype(BF)
    summed = jnp.sum(tail[0], axis=0)
    gain_grads = lax.dynamic_slice_in_dim(tail[0] + tail[1], m * 8, 8, 0)
    gain_grads = lax.dynamic_slice_in_dim(gain_grads, c * 8, 8, 2)
    return (
        layer_output[None],
        tokens_grad[None],
        summed[0],
        query_grad,
        key_grad,
        value_grad,
        gain_grads[:, 2],
        gain_grads[:, 19],
        output_grad.reshape(cut, HEAD_DIM).astype(F32),
        summed[1],
        summed[3:19].T,
        gate_grad[None],
        up_grad[None],
        down_grad[None],
    )


def grid_fits(tokens, router_weight):
    sizes = tuple(lax.axis_size(name) for name in ("seq", "ctx", "mp"))
    return sizes == (4, 4, 2) and tokens.shape == (1, 128, 2048) and router_weight.shape == (128, 16)


def body(*args):
    if grid_fits(args[0], args[12]):
        return fast_body(*args)
    return general_body(*args)


def solution(mesh):
    placed = (
        P("seq", "ctx", None),
        P("seq", "ctx"),
        P("seq", "ctx", None),
        P("seq", "ctx", None),
        P(("seq", "ctx")),
        P(("seq", "ctx"), "mp"),
        P(("seq", "ctx"), "mp"),
        P(("seq", "ctx"), "mp"),
        P("mp", ("seq", "ctx")),
        P("mp", ("seq", "ctx")),
        P("mp", ("seq", "ctx")),
        P(("seq", "ctx")),
        P(("seq", "ctx"), None),
        P(("seq", "ctx"), None, "mp"),
        P(("seq", "ctx"), None, "mp"),
        P(("seq", "ctx"), "mp", None),
    )
    return jax.shard_map(
        body,
        mesh=mesh,
        in_specs=placed,
        out_specs=(
            P("seq", "ctx", None),
            P("seq", "ctx", None),
            P(("seq", "ctx")),
            P(("seq", "ctx"), "mp"),
            P(("seq", "ctx"), "mp"),
            P(("seq", "ctx"), "mp"),
            P("mp", ("seq", "ctx")),
            P("mp", ("seq", "ctx")),
            P("mp", ("seq", "ctx")),
            P(("seq", "ctx")),
            P(("seq", "ctx"), None),
            P(("seq", "ctx"), None, "mp"),
            P(("seq", "ctx"), None, "mp"),
            P(("seq", "ctx"), "mp", None),
        ),
        check_vma=False,
    )
```

```python
import functools

import jax
import jax.numpy as jnp
import numpy as np
from jax import lax
from jax.experimental import pallas as pl
from jax.experimental.pallas import tpu as pltpu
from jax.sharding import PartitionSpec as P

MESH = pl.DeviceIdType.MESH
BF = jnp.bfloat16
F32 = jnp.float32


def place():
    s = lax.axis_index("seq")
    z = lax.axis_index("ctx")
    m = lax.axis_index("mp")
    return s, z, m


def flip_x(s):
    return s + 1 - 2 * lax.rem(s, 2)


def flip_y(s):
    return s + 2 - 4 * lax.div(s, 2)


def remote(src, dst, send, recv, device):
    return pltpu.make_async_remote_copy(
        src_ref=src, dst_ref=dst, send_sem=send, recv_sem=recv,
        device_id=device, device_id_type=MESH,
    )


def signal(device):
    pl.semaphore_signal(
        pltpu.get_barrier_semaphore(), inc=1, device_id=device, device_id_type=MESH
    )


def when(cond, fn):
    if cond is True:
        fn()
    else:
        pl.when(cond)(fn)


def near_planes(z):
    return (z, flip_x(z), 2 - lax.div(z, 2), 3 - 3 * lax.div(z, 2))


def far_planes(z):
    return (3 - 3 * lax.div(z, 2), lax.rem(2 + 3 * z, 5), 1 + lax.rem(z, 2), z)


def span(start, size):
    return pl.ds(pl.multiple_of(start, size), size)


class Part:
    def __init__(self, kind, source, target):
        self.kind = kind
        self.source = source
        self.target = target
        self.whole = kind == "small"

    def own(self, m):
        if self.kind == "rows":
            width = self.source.shape[1] // 2
            return self.source.at[:, span(m * width, width)]
        return self.source

    def piece(self, row, plane, core, half=None):
        ref = self.target
        if self.kind == "small":
            return ref.at[plane * 4 + row, core]
        if self.kind == "line":
            rows = self.source.shape[0]
            return ref.at[span(core * rows, rows), span(plane * 128, 128)]
        if self.kind == "cols":
            rows = self.source.shape[1] // 2
            base = (row * 4 + plane) * 2 * rows + core * rows
            if half is None:
                return ref.at[span(base, rows), :]
            return ref.at[span(base + half * (rows // 2), rows // 2), :]
        if self.kind == "rows":
            rows, width = self.source.shape[0], self.source.shape[1] // 2
            cols = span(core * width, width)
            base = (plane * 4 + row) * rows
        elif self.kind == "chips":
            rows, width = self.source.shape[0], self.source.shape[1] // 2
            cols = span(core * width, width)
            base = (row * 4 + plane) * rows
        else:
            rows = self.source.shape[0]
            cols = span((row * 4 + plane) * 128, 128)
            base = core * rows
        if half is None:
            return ref.at[span(base, rows), cols]
        return ref.at[span(base + half * (rows // 2), rows // 2), cols]

    def mirrored(self):
        return self.kind in ("rows", "chips", "cols")


class Gather:
    Z, X, Y, DX, DY, PO, PX, PY, P0, P1, UP, DN = range(12)

    def __init__(self, parts, send, recv):
        self.parts, self.send, self.recv = parts, send, recv
        s, z, m = place()
        self.s, self.z, self.m = s, z, m
        self.lines = (s, flip_x(s), flip_y(s), 3 - s)
        self.xn, self.yn, self.pn = (self.lines[1], z, m), (self.lines[2], z, m), (s, z, 1 - m)
        self.planes = near_planes(z)
        self.pending = []

    def own(self, k):
        part = self.parts[k]
        if part.kind == "chips":
            width = part.source.shape[1] // 2
            return part.source.at[:, span(self.m * width, width)]
        return part.own(self.m)

    def push(self, cond, k, kind, at, source, target, device, out=None):
        out = kind if out is None else out
        copy = lambda: remote(source, target, self.send.at[k, out, at], self.recv.at[k, kind, at], device)
        when(cond, lambda: copy().start())
        self.pending.append((cond, copy))

    def landed(self, k, kind, at, target):
        remote(target, target, self.send.at[k, kind, at], self.recv.at[k, kind, at], self.pn).wait_recv()

    def fan(self, k, at, source):
        target = self.parts[k].piece(self.s, at, self.m)
        self.push(True, k, self.X, at, source, target, self.xn)
        self.push(True, k, self.Y, at, source, target, self.yn)

    def start(self):
        z, at = self.z, self.z
        for k, part in enumerate(self.parts):
            source, target = self.own(k), part.piece(self.s, at, self.m)
            self.push(z < 3, k, self.Z, at, source, target, (self.s, z + 1, self.m), self.UP)
            self.push(z > 0, k, self.Z, at, source, target, (self.s, z - 1, self.m), self.DN)
            self.fan(k, at, source)
            if not part.mirrored():
                self.push(True, k, self.PO, at, source, target, self.pn)

    def along(self, step):
        z, at = self.z, self.planes[step]
        goal = 3 - z if step == 1 else 3 * z - 3
        inner = jnp.logical_and(z > 0, z < 3)
        for k, part in enumerate(self.parts):
            target = part.piece(self.s, at, self.m)
            self.landed(k, self.Z, at, target)
            self.push(inner, k, self.Z, at, target, target, (self.s, goal, self.m), self.UP)
            self.fan(k, at, target)
            self.push(True, k, self.PO, at, target, target, self.pn)

    def across(self, step):
        at = self.planes[step]
        for k, part in enumerate(self.parts):
            whole = part.piece(self.lines[1], at, self.m)
            half = whole if part.whole else part.piece(self.lines[1], at, self.m, 0)
            self.landed(k, self.X, at, whole)
            self.push(True, k, self.DY, at, half, half, self.yn)
            self.push(True, k, self.PX, at, whole, whole, self.pn)
            whole = part.piece(self.lines[2], at, self.m)
            self.landed(k, self.Y, at, whole)
            if not part.whole:
                half = part.piece(self.lines[2], at, self.m, 1)
                self.push(True, k, self.DX, at, half, half, self.xn)
            self.push(True, k, self.PY, at, whole, whole, self.pn)

    def corner(self, step):
        at, far = self.planes[step], self.lines[3]
        for k, part in enumerate(self.parts):
            half = part.piece(far, at, self.m, None if part.whole else 0)
            self.landed(k, self.DY, at, half)
            self.push(True, k, self.P0, at, half, half, self.pn)
            if not part.whole:
                half = part.piece(far, at, self.m, 1)
                self.landed(k, self.DX, at, half)
                self.push(True, k, self.P1, at, half, half, self.pn)

    def ready(self, step):
        at, other = self.planes[step], 1 - self.m
        for k, part in enumerate(self.parts):
            if step > 0 or not part.mirrored():
                self.landed(k, self.PO, at, part.piece(self.s, at, other))
            self.landed(k, self.PX, at, part.piece(self.lines[1], at, other))
            self.landed(k, self.PY, at, part.piece(self.lines[2], at, other))
            self.landed(k, self.P0, at, part.piece(self.lines[3], at, other, None if part.whole else 0))
            if not part.whole:
                self.landed(k, self.P1, at, part.piece(self.lines[3], at, other, 1))

    def finish(self):
        for cond, copy in self.pending:
            when(cond, lambda copy=copy: copy().wait_send())


class Line(Gather):
    def fan(self, k, at, source):
        pass

    def ready(self, step):
        at = self.planes[step]
        for k, part in enumerate(self.parts):
            self.landed(k, self.PO, at, part.piece(self.s, at, 1 - self.m))


class Spread(Gather):
    def block(self, plane):
        source = self.parts[0].source
        rows = source.shape[1] // 2
        return source.at[plane, span(self.m * rows, rows), :]

    def start(self):
        z = self.z
        target = self.parts[0].piece(self.s, z, self.m)
        for step in (1, 2, 3):
            plane = lax.rem(z + step, 4)
            out = (self.UP, self.DN, self.Z)[step - 1]
            self.push(True, 0, self.Z, z, self.block(plane), target, (self.s, plane, self.m), out)
        self.fan(0, z, self.block(z))

    def along(self, step):
        at = self.planes[step]
        target = self.parts[0].piece(self.s, at, self.m)
        self.landed(0, self.Z, at, target)
        self.fan(0, at, target)
        self.push(True, 0, self.PO, at, target, target, self.pn)


def call_chips():
    s, z, m = place()
    c = s * 4 + z
    for step in range(1, 16):
        j = lax.rem(c + step, 16)
        signal((lax.div(j, 4), lax.rem(j, 4), m))
    signal((s, z, 1 - m))


def add_rows(put, sources, count, step=16):
    def run(r, _):
        at = span(r * step, step)
        total = sources[0](at)
        for source in sources[1:]:
            total = total + source(at)
        put(at, total)
        return 0
    lax.fori_loop(0, count // step, run, 0)


def shifted(at, base, step=16):
    return pl.ds(pl.multiple_of(at.start + base, step), step)


class Reduce:
    def __init__(self, pair, by_plane, src, acc, out, bufs, sems):
        self.pair, self.by_plane, self.src, self.acc, self.out = pair, by_plane, src, acc, out
        (self.buf0, self.bufx, self.bufy, self.bufx2, self.bufy2, self.zbuf, self.zsend, self.fin) = bufs
        self.send, self.recv = sems
        s, z, m = place()
        self.s, self.z, self.m = s, z, m
        self.xn, self.yn, self.pn = (flip_x(s), z, m), (flip_y(s), z, m), (s, z, 1 - m)
        self.lines = (s, flip_x(s), flip_y(s), 3 - s)
        self.rows = self.fin.shape[0]
        self.half = self.rows // 2
        self.width = self.fin.shape[1]
        self.mine = span(m * self.width, self.width)
        self.cols = self.mine if acc.shape[1] > self.width else slice(None)
        self.other = span((1 - m) * self.width, self.width)
        self.pending = []

    def push(self, kind, at, source, target, device):
        copy = lambda: remote(source, target, self.send.at[kind, at], self.recv.at[kind, at], device)
        copy().start()
        self.pending.append(copy)

    def landed(self, kind, at, target):
        remote(target, target, self.send.at[kind, at], self.recv.at[kind, at], self.pn).wait_recv()

    def base(self, at, q, by_plane=None):
        by_plane = self.by_plane if by_plane is None else by_plane
        row = self.lines[q]
        return (at * 4 + row if by_plane else row * 4 + at) * self.rows

    def held(self, at, q):
        return self.base(at, q, self.pair or self.by_plane)

    def swap(self, at):
        for q in (3, 1, 2, 0):
            self.push(q, at, self.src.at[span(self.base(at, q), self.rows), self.other],
                      self.buf0.at[at, q], self.pn)

    def block(self, at, q, lo):
        return self.acc.at[pl.ds(pl.multiple_of(self.held(at, q) + lo, self.half), self.half), self.cols]

    def first(self, at):
        for q in (3, 1, 2, 0):
            if self.pair:
                self.landed(q, at, self.buf0.at[at, q])
                base = self.base(at, q)
                held = self.held(at, q)

                def put(r, v, held=held):
                    self.acc[shifted(r, held), self.cols] = v.astype(BF)
                add_rows(put, [
                    lambda r, base=base: self.src[shifted(r, base), self.mine].astype(F32),
                    lambda r, q=q: self.buf0[at, q, r].astype(F32)], self.rows)
            if q == 3:
                self.push(4, at, self.block(at, 3, 0), self.bufx.at[at, 1], self.xn)
                self.push(5, at, self.block(at, 3, self.half), self.bufy.at[at, 1], self.yn)
            if q == 1:
                self.push(6, at, self.block(at, 1, 0), self.bufx.at[at, 0], self.xn)
            if q == 2:
                self.push(7, at, self.block(at, 2, self.half), self.bufy.at[at, 0], self.yn)

    def local(self, at, q, lo):
        held = self.held(at, q) + lo
        return lambda r: self.acc[shifted(r, held), self.cols].astype(F32)

    def second(self, at):
        self.landed(4, at, self.bufx.at[at, 1])

        def put_x(r, v):
            self.bufx[at, 1, r] = v.astype(BF)
        add_rows(put_x, [self.local(at, 2, 0), lambda r: self.bufx[at, 1, r].astype(F32)], self.half)
        self.push(8, at, self.bufx.at[at, 1], self.bufy2.at[at], self.yn)
        self.landed(5, at, self.bufy.at[at, 1])

        def put_y(r, v):
            self.bufy[at, 1, r] = v.astype(BF)
        add_rows(put_y, [self.local(at, 1, self.half), lambda r: self.bufy[at, 1, r].astype(F32)], self.half)
        self.push(9, at, self.bufy.at[at, 1], self.bufx2.at[at], self.xn)

    def settle(self, at, put_low, put_high):
        half = self.half
        self.landed(6, at, self.bufx.at[at, 0])
        self.landed(8, at, self.bufy2.at[at])
        self.landed(7, at, self.bufy.at[at, 0])
        self.landed(9, at, self.bufx2.at[at])
        add_rows(put_low, [self.local(at, 0, 0), lambda r: self.bufx[at, 0, r].astype(F32),
                           lambda r: self.bufy2[at, r].astype(F32)], half)
        add_rows(put_high, [self.local(at, 0, half), lambda r: self.bufy[at, 0, r].astype(F32),
                            lambda r: self.bufx2[at, r].astype(F32)], half)

    def third(self, at, slot):
        half = self.half

        def low(r, v):
            self.zsend[slot, r] = v.astype(BF)

        def high(r, v):
            self.zsend[slot, shifted(r, half)] = v.astype(BF)
        self.settle(at, low, high)
        copy = lambda: remote(self.zsend.at[slot], self.zbuf.at[self.z], self.send.at[12, slot],
                              self.recv.at[10, self.z], (self.s, at, self.m))
        copy().start()
        self.pending.append(copy)

    def keep(self):
        half = self.half

        def low(r, v):
            self.fin[r] = v

        def high(r, v):
            self.fin[shifted(r, half)] = v
        self.settle(self.z, low, high)

    def close(self):
        mine, other = self.mine, self.other
        others = [lax.rem(self.z + step, 4) for step in (1, 2, 3)]
        for at in others:
            self.landed(10, at, self.zbuf.at[at])

        def put(r, v):
            self.out[r, mine] = v.astype(BF)
        add_rows(put, [lambda r: self.fin[r]] + [
            lambda r, at=at: self.zbuf[at, r].astype(F32) for at in others], self.rows)
        self.push(13, 0, self.out.at[:, mine], self.out.at[:, mine], self.pn)

    def landing(self):
        self.landed(13, 0, self.out.at[:, self.other])

    def finish(self):
        for copy in self.pending:
            copy().wait_send()


def reduce_buffers(pair, rows, width):
    half = rows // 2
    return [
        pltpu.VMEM((4, 4, rows, width) if pair else (1, 1, 16, width), BF),
        pltpu.VMEM((4, 2, half, width), BF),
        pltpu.VMEM((4, 2, half, width), BF),
        pltpu.VMEM((4, half, width), BF),
        pltpu.VMEM((4, half, width), BF),
        pltpu.VMEM((4, rows, width), BF),
        pltpu.VMEM((3, rows, width), BF),
        pltpu.VMEM((rows, width), F32),
        pltpu.SemaphoreType.DMA((14, 4)),
        pltpu.SemaphoreType.DMA((14, 4)),
    ]


def experts_body(two_ref, share_ref, top_ref, gate_ref, up_ref, down_ref,
                 back_out, prob_out, moe_out, dgate_out, dup_out, ddown_out,
                 two_all, shares, top_all, pair_w, down_w, pull, pair_v,
                 acts, dpair, back, prob_v, stage, dstage,
                 buf0, bufx, bufy, bufx2, bufy2, zbuf, zsend, fin, rsend, rrecv,
                 gsend, grecv, psend, precv, load, store, dstore):
    s, z, m = place()
    c = s * 4 + z
    rows = two_ref.shape[0]
    width = two_ref.shape[1]
    hidden = down_w.shape[0]
    block = 4 * rows
    loads = [
        pltpu.make_async_copy(top_ref, top_all, load.at[0]),
        pltpu.make_async_copy(down_ref, down_w, load.at[1]),
        pltpu.make_async_copy(gate_ref, pair_w.at[:, pl.ds(0, hidden)], load.at[2]),
        pltpu.make_async_copy(up_ref, pair_w.at[:, pl.ds(hidden, hidden)], load.at[3]),
    ]
    for copy in loads:
        copy.start()
    call_chips()
    pl.semaphore_wait(pltpu.get_barrier_semaphore(), 16)
    work = Gather([Part("rows", two_ref, two_all), Part("small", share_ref, shares)], gsend, grecv)
    work.start()
    two_all[span((z * 4 + s) * rows, rows), :] = two_ref[...]
    shares[z * 4 + s, m] = share_ref[...]
    total = Reduce(True, True, back, back, back_out,
                   (buf0, bufx, bufy, bufx2, bufy2, zbuf, zsend, fin), (rsend, rrecv))
    planes = work.planes

    def tiles(count, size, fn):
        def run(i, _):
            fn(span(i * size, size))
            return 0
        lax.fori_loop(0, count // size, run, 0)

    def pulls(i):
        at = pl.ds(i * block, block)

        def tile(cols):
            pull[at, cols] = contract_last(top_all[at, :], down_w[cols, :])
        tiles(hidden, 512, tile)

    def enter(side, k):
        at = span(planes[k] * block, block)
        cols = pl.ds(side * hidden, hidden)
        pair_v[:, cols] = jnp.dot(two_all[at, :], pair_w[:, cols], preferred_element_type=F32)

    def middle(k):
        def one(row, _):
            slot = planes[k] * 4 + row
            wide = jnp.broadcast_to(shares[slot, m, pl.ds(c, 1), :], (rows, rows))
            column = jnp.transpose(wide)[:, 0:1]
            base = span(slot * rows, rows)
            here = span(row * rows, rows)
            gate = pair_v[here, pl.ds(0, hidden)]
            up = pair_v[here, pl.ds(hidden, hidden)]
            drawn = pull[base, :]
            sig = jax.nn.sigmoid(gate)
            act = gate * sig * up
            acts[base, :] = (act * column).astype(BF)
            grad = drawn * column
            dpair[base, pl.ds(0, hidden)] = (grad * up * sig * (1.0 + gate * (1.0 - sig))).astype(BF)
            dpair[base, pl.ds(hidden, hidden)] = (grad * gate * sig).astype(BF)
            prob = jnp.sum(act * drawn, axis=1, keepdims=True)
            prob_v[slot] = jnp.transpose(jnp.broadcast_to(prob, (rows, rows)))[0:8, :]
            return 0
        lax.fori_loop(0, 4, one, 0)

    def backs(k):
        at = span(planes[k] * block, block)

        def tile(cols):
            back[at, cols] = contract_last(dpair[at, :], pair_w[cols, :]).astype(BF)
        tiles(width, 1024, tile)
        total.swap(planes[k])

    def saves(i, t):
        cols = pl.ds(t * 1024, 1024)
        return pltpu.make_async_copy(
            stage.at[t], moe_out.at[pl.ds(i * block, block), cols], store.at[t])

    def moes(i):
        at = pl.ds(i * block, block)
        for t in (0, 1):
            if i >= 1:
                saves(i - 1, t).wait()
            cols = pl.ds(t * 1024, 1024)
            stage[t] = jnp.dot(acts[at, :], down_w[:, cols], preferred_element_type=F32).astype(BF)
            saves(i, t).start()

    def keep(i):
        rows_at = span(i * 512, 512)
        slot = lax.rem(i, 2)
        return [
            pltpu.make_async_copy(
                dstage.at[slot, :, pl.ds(side * hidden, hidden)],
                (dgate_out, dup_out)[side].at[rows_at, :],
                dstore.at[slot, side],
            )
            for side in (0, 1)
        ]

    def keep_down(i):
        return pltpu.make_async_copy(
            dstage.at[i], ddown_out.at[:, pl.ds(i * 1024, 1024)], dstore.at[i, 2])

    def grads(low, high):
        def one(i, _):
            def settle():
                for copy in keep(i - 2):
                    copy.wait()
            pl.when(i >= 2)(settle)
            cols = span(i * 512, 512)
            dstage[lax.rem(i, 2)] = contract_first(two_all[:, cols], dpair[...])
            for copy in keep(i):
                copy.start()
            return 0
        lax.fori_loop(low, high, one, 0)

    def downs():
        for i in (2, 3):
            for copy in keep(i):
                copy.wait()
        for i in (0, 1):
            dstage[i] = contract_first(acts[...], top_all[:, pl.ds(i * 1024, 1024)])
            keep_down(i).start()

    loads[0].wait()
    loads[1].wait()
    pulls(0)
    work.along(1)
    work.across(0)
    pulls(1)
    work.along(2)
    work.across(1)
    pulls(2)
    work.along(3)
    work.corner(0)
    pulls(3)
    work.across(2)
    loads[2].wait()
    loads[3].wait()
    work.ready(0)
    enter(0, 0)
    work.corner(1)
    enter(1, 0)
    work.across(3)
    middle(0)
    work.corner(2)
    backs(0)
    work.ready(1)
    enter(0, 1)
    work.corner(3)
    enter(1, 1)
    total.first(planes[0])
    middle(1)
    backs(1)
    total.second(planes[0])
    work.ready(2)
    enter(0, 2)
    total.first(planes[1])
    enter(1, 2)
    middle(2)
    backs(2)
    total.second(planes[1])
    work.ready(3)
    enter(0, 3)
    total.first(planes[2])
    enter(1, 3)
    middle(3)

    def dev(j):
        return (lax.div(j, 4), lax.rem(j, 4), m)

    def send_prob(step):
        j = lax.rem(c + step, 16)
        slot = lax.rem(j, 4) * 4 + lax.div(j, 4)
        return remote(prob_v.at[slot], prob_out.at[m, c], psend.at[step], precv.at[step], dev(j))
    for step in range(1, 16):
        send_prob(step).start()
    prob_out[m, c] = prob_v[z * 4 + s]
    backs(3)
    total.second(planes[2])
    moes(0)
    total.first(planes[3])
    total.keep()
    moes(1)
    total.third(planes[1], 0)
    moes(2)
    total.second(planes[3])
    total.third(planes[2], 1)
    moes(3)
    grads(0, 1)
    total.third(planes[3], 2)
    grads(1, 3)
    for step in range(1, 16):
        j = lax.rem(c + 16 - step, 16)
        target = prob_out.at[m, j]
        remote(target, target, psend.at[step], precv.at[step], dev(j)).wait_recv()
    pair = remote(prob_out.at[m], prob_out.at[m], psend.at[0], precv.at[0], (s, z, 1 - m))
    pair.start()
    grads(3, 4)
    downs()
    total.close()
    for i in (0, 1):
        keep_down(i).wait()
    for t in (0, 1):
        saves(3, t).wait()
    total.landing()
    other = prob_out.at[1 - m]
    remote(other, other, psend.at[0], precv.at[0], (s, z, 1 - m)).wait_recv()
    pair.wait_send()
    for step in range(1, 16):
        send_prob(step).wait_send()
    work.finish()
    total.finish()


def experts(ident, two, share, top, gate, up, down):
    rows, width = two.shape
    hidden = gate.shape[1]
    every = 16 * rows
    block = 4 * rows
    vmem = pl.BlockSpec(memory_space=pltpu.VMEM)
    hbm = pl.BlockSpec(memory_space=pl.ANY)
    return pl.pallas_call(
        experts_body,
        out_shape=(
            jax.ShapeDtypeStruct((rows, width), BF),
            jax.ShapeDtypeStruct((2, 16, 8, rows), F32),
            jax.ShapeDtypeStruct((every, width), BF),
            jax.ShapeDtypeStruct((width, hidden), F32),
            jax.ShapeDtypeStruct((width, hidden), F32),
            jax.ShapeDtypeStruct((hidden, width), F32),
        ),
        in_specs=[vmem, vmem, hbm, hbm, hbm, hbm],
        out_specs=(vmem, vmem, hbm, hbm, hbm, hbm),
        scratch_shapes=[
            pltpu.VMEM((every, width), BF),
            pltpu.VMEM((16, 2) + share.shape, F32),
            pltpu.VMEM((every, width), BF),
            pltpu.VMEM((width, 2 * hidden), BF),
            pltpu.VMEM((hidden, width), BF),
            pltpu.VMEM((every, hidden), F32),
            pltpu.VMEM((block, 2 * hidden), F32),
            pltpu.VMEM((every, hidden), BF),
            pltpu.VMEM((every, 2 * hidden), BF),
            pltpu.VMEM((every, width), BF),
            pltpu.VMEM((16, 8, rows), F32),
            pltpu.VMEM((2, block, 1024), BF),
            pltpu.VMEM((2, 512, 2 * hidden), F32),
        ]
        + reduce_buffers(True, rows, width // 2)
        + [
            pltpu.SemaphoreType.DMA((2, 12, 4)),
            pltpu.SemaphoreType.DMA((2, 12, 4)),
            pltpu.SemaphoreType.DMA((16,)),
            pltpu.SemaphoreType.DMA((16,)),
            pltpu.SemaphoreType.DMA((4,)),
            pltpu.SemaphoreType.DMA((2,)),
            pltpu.SemaphoreType.DMA((2, 3)),
        ],
        compiler_params=pltpu.CompilerParams(collective_id=ident, has_side_effects=True,
                                             vmem_limit_bytes=66900000),
        name="experts_%d" % ident,
    )(two, share, top, gate, up, down)


class Hand:
    def __init__(self, source, target, send, recv):
        s, z, m = place()
        self.c, self.m, self.pn = s * 4 + z, m, (s, z, 1 - m)
        self.source, self.target, self.send, self.recv = source, target, send, recv

    def dev(self, j):
        return (lax.div(j, 4), lax.rem(j, 4), self.m)

    def copy(self, step):
        j = lax.rem(self.c + step, 16)
        return remote(self.source(j), self.target(self.c), self.send.at[step], self.recv.at[step], self.dev(j))

    def start(self):
        for step in range(1, 16):
            self.copy(step).start()

    def collect(self):
        for step in range(1, 16):
            j = lax.rem(self.c + 16 - step, 16)
            remote(self.target(j), self.target(j), self.send.at[step], self.recv.at[step], self.pn).wait_recv()

    def finish(self):
        for step in range(1, 16):
            self.copy(step).wait_send()


class Chips:
    def __init__(self, source, target, send, recv, fsend, frecv, local):
        s, z, m = place()
        self.c, self.m, self.pn = s * 4 + z, m, (s, z, 1 - m)
        self.first = lax.div(self.c, 8) == m
        self.source, self.target = source, target
        self.send, self.recv, self.fsend, self.frecv, self.local = send, recv, fsend, frecv, local

    def copy(self, i):
        j = 8 * self.m + i
        return remote(self.source(i), self.target.at[self.c], self.send.at[i], self.recv.at[self.c],
                      (lax.div(j, 4), lax.rem(j, 4), self.m))

    def mine(self):
        return pltpu.make_async_copy(
            self.source(lax.rem(self.c, 8)), self.target.at[self.c], self.local.at[0])

    def each(self, fn):
        for step in range(8):
            i = lax.rem(self.c + 1 + step, 8)
            pl.when(8 * self.m + i != self.c)(lambda i=i: fn(self.copy(i)))

    def start(self):
        self.each(lambda copy: copy.start())
        pl.when(self.first)(lambda: self.mine().start())

    def forward(self, j):
        return remote(self.target.at[j], self.target.at[j], self.fsend.at[j], self.frecv.at[j], self.pn)

    def collect(self):
        def take():
            self.mine().wait()
            self.forward(self.c).start()
            for step in range(1, 16):
                j = lax.rem(self.c + 16 - step, 16)
                remote(self.target.at[j], self.target.at[j], self.send.at[0], self.recv.at[j],
                       self.pn).wait_recv()
                self.forward(j).start()
        pl.when(self.first)(take)

    def follow(self):
        def wait():
            for j in range(16):
                self.forward(j).wait_recv()
        pl.when(jnp.logical_not(self.first))(wait)

    def finish(self):
        def wait():
            for j in range(16):
                self.forward(j).wait_send()
        pl.when(self.first)(wait)
        self.each(lambda copy: copy.wait_send())


def chips_semaphores():
    return [pltpu.SemaphoreType.DMA((8,))] + [pltpu.SemaphoreType.DMA((16,))] * 3 + [
        pltpu.SemaphoreType.DMA((1,))]


def front_body(tok_ref, one_ref, second_ref, place_ref, router_ref, qg_ref, kg_ref, routes_ref,
               qw_ref, kw_ref, vw_ref, wo_ref, cot_ref, freq_ref,
               n1_out, wo_out, cot_out, w3, info, raw, rows3, squares, mixed, lse, trig, own_mixed,
               hidden, two, probs_out, chosen_out, share_out, heads_out, gain_out,
               info_ref, packed_ref, n1_own, n1_all, wo_all, wide_mixed, gathered, sums, line,
               nsend, nrecv, osend, orecv, csend, crecv,
               isend, irecv, qsend, qrecv, pairs, *chips_sems):
    s, z, m = place()
    c = s * 4 + z
    pn = (s, z, 1 - m)
    rows, width = tok_ref.shape
    dim = 128
    planes = near_planes(z)
    lane = lax.broadcasted_iota(jnp.int32, (rows, dim), 1)
    call_chips()
    info_ref[...] = jnp.zeros_like(info_ref)
    info_ref[0:1, :] = one_ref[...].astype(F32)
    info_ref[1:2, :] = second_ref[...].astype(F32)
    info_ref[2:3, :] = place_ref[...].astype(F32)
    info_ref[4:20, :] = router_ref[...].astype(F32)
    info_ref[24:32, 0:8] = qg_ref[...].astype(F32)
    info_ref[32:40, 0:8] = kg_ref[...].astype(F32)
    for i in range(8):
        for n, ref in enumerate((qw_ref, kw_ref, vw_ref)):
            packed_ref[i, :, pl.ds(n * dim, dim)] = ref[:, pl.ds(i * dim, dim)]
    pl.semaphore_wait(pltpu.get_barrier_semaphore(), 16)
    hand = Hand(lambda j: info_ref, lambda j: info.at[m, j], isend, irecv)
    hand.start()
    weights = Chips(lambda i: packed_ref.at[i], w3, *chips_sems[:5])
    weights.start()
    outer = Gather([Part("heads", wo_ref, wo_all)], osend, orecv)
    outer.start()
    info[m, c] = info_ref[...]

    def square_sum(r, _):
        at = span(r * 16, 16)
        x = tok_ref[at, :].astype(F32)
        mean = jnp.sum(x * x, axis=1, keepdims=True) / width
        line[at, :] = jnp.broadcast_to(lax.rsqrt(mean + eps), (16, dim))
        return 0
    lax.fori_loop(0, rows // 16, square_sum, 0)
    hand.collect()
    swap = remote(info.at[m], info.at[m], pairs.at[0], pairs.at[1], pn)
    swap.start()

    def normalize(j, _):
        at = span(j * dim, dim)
        n1_own[:, at] = (tok_ref[:, at].astype(F32) * line[...] * info[m, j, 0:1, :]).astype(BF)
        return 0
    lax.fori_loop(0, 16, normalize, 0)
    first = Gather([Part("rows", n1_own, n1_all)], nsend, nrecv)
    first.start()
    n1_all[span((z * 4 + s) * rows, rows), :] = n1_own[...]

    def tables(b, _):
        spot = jnp.broadcast_to(info[m, 8 * m + b, 2:3, :], (rows, dim))
        angle = jnp.transpose(spot) * freq_ref[0:1, :]
        trig[0, b] = jnp.cos(angle)
        trig[1, b] = jnp.where(lane < dim // 2, -jnp.sin(angle), jnp.sin(angle))
        return 0
    lax.fori_loop(0, 8, tables, 0)
    other = info.at[1 - m]
    remote(other, other, pairs.at[0], pairs.at[1], pn).wait_recv()

    first.along(1)
    first.across(0)
    weights.collect()
    first.along(2)
    first.across(1)
    first.along(3)
    first.corner(0)
    weights.follow()
    first.across(2)
    first.ready(0)

    def project(k):
        value = jnp.dot(n1_all[span((planes[k] * 4 + 2 * m) * rows, 2 * rows), :],
                        w3[...].reshape(width, 3 * dim), preferred_element_type=F32)
        for e in (0, 1):
            part = value[e * rows : (e + 1) * rows, :]
            base = span((e * 4 + planes[k]) * rows, rows)
            raw[base, :] = part[:, : 2 * dim]
            rows3[base, pl.ds(2 * dim, dim)] = part[:, 2 * dim :].astype(BF)
    project(0)
    first.corner(1)
    first.across(3)
    outer.along(1)
    outer.across(0)
    first.ready(1)
    project(1)
    first.corner(2)
    first.ready(2)
    project(2)
    first.corner(3)
    first.ready(3)
    project(3)

    def norms(b, total):
        at = span(b * rows, rows)
        q = raw[at, pl.ds(0, dim)]
        k = raw[at, pl.ds(dim, dim)]
        total = jnp.where(lane == b, jnp.sum(q * q, axis=1, keepdims=True), total)
        return jnp.where(lane == b + 8, jnp.sum(k * k, axis=1, keepdims=True), total)
    total = lax.fori_loop(0, 8, norms, jnp.zeros((rows, dim), F32))
    sums[...] = jnp.transpose(total)[0:16, :]
    share = Hand(lambda j: sums, lambda j: gathered.at[j], qsend, qrecv)
    share.start()
    gathered[c] = sums[...]
    save_n1 = pltpu.make_async_copy(n1_all, n1_out, pairs.at[2])
    save_n1.start()
    wo_own = pltpu.make_async_copy(wo_ref, outer.parts[0].piece(s, z, m), pairs.at[3])
    wo_own.start()
    outer.along(2)
    share.collect()

    def add_up(j, acc):
        return acc + gathered[j]
    summed = lax.fori_loop(1, 16, add_up, gathered[0])
    squares[...] = summed
    wide = jnp.concatenate([lax.rsqrt(summed / width + eps), jnp.zeros((rows - 16, dim), F32)], axis=0)
    line[...] = jnp.transpose(wide)

    def head_gain(which):
        total = jnp.zeros((8, dim), F32)
        lane8 = lax.broadcasted_iota(jnp.int32, (8, dim), 1)
        for j in range(16):
            row = info[lax.div(c, 8), j, pl.ds(24 + 8 * which + lax.rem(c, 8), 1), :]
            moved = pltpu.roll(jnp.broadcast_to(row, (8, dim)), 8 * j, 1)
            total = jnp.where(lax.div(lane8, 8) == j, moved, total)
        return total[0:1, :]
    gains = (head_gain(0), head_gain(1))
    heads_out[...] = jnp.concatenate([gains[0], gains[1], jnp.zeros((6, dim), F32)], axis=0)

    def turn(b, _):
        at = span(b * rows, rows)
        for which, factor in ((0, dim ** (-0.5)), (1, 1.0)):
            pick = jnp.where(lane == b + 8 * which, line[...], 0.0)
            inverse = jnp.sum(pick, axis=1, keepdims=True)
            value = raw[at, pl.ds(which * dim, dim)] * inverse * gains[which]
            value = value * trig[0, b] + pltpu.roll(value, dim // 2, 1) * trig[1, b]
            rows3[at, pl.ds(which * dim, dim)] = (value * factor).astype(BF)
        return 0
    lax.fori_loop(0, 8, turn, 0)
    outer.across(1)
    outer.along(3)

    def attend(b, _):
        seq = span(lax.div(b, 4) * 4 * rows, 4 * rows)
        at = span(b * rows, rows)
        scores = contract_last(rows3[at, pl.ds(0, dim)], rows3[seq, pl.ds(dim, dim)])
        here = lax.broadcasted_iota(jnp.int32, scores.shape, 0) + lax.rem(b, 4) * rows
        allowed = lax.broadcasted_iota(jnp.int32, scores.shape, 1) <= here
        scores = jnp.where(allowed, scores, neg_big)
        top = jnp.max(scores, axis=1, keepdims=True)
        weight = jnp.where(allowed, jnp.exp(scores - top), 0.0)
        count = jnp.sum(weight, axis=1, keepdims=True)
        value = jnp.dot(weight.astype(BF), rows3[seq, pl.ds(2 * dim, dim)], preferred_element_type=F32)
        mixed[b] = (value / count).astype(BF)
        lse[b] = jnp.transpose(jnp.broadcast_to(top + jnp.log(count), (rows, dim)))[0:8, :]
        return 0
    lax.fori_loop(0, 8, attend, 0)
    back = Chips(lambda i: mixed.at[i], own_mixed, *chips_sems[5:])
    back.start()
    outer.corner(0)
    outer.across(2)
    back.collect()
    outer.corner(1)
    outer.across(3)
    cots = Gather([Part("rows", cot_ref, cot_out)], csend, crecv)
    cots.start()
    cot_own = pltpu.make_async_copy(cot_ref, cot_out.at[span((z * 4 + s) * rows, rows)], pairs.at[4])
    cot_own.start()
    outer.corner(2)
    back.follow()
    outer.corner(3)
    wo_own.wait()
    for step in range(4):
        outer.ready(step)
    save_wo = pltpu.make_async_copy(wo_all, wo_out, pairs.at[5])
    save_wo.start()
    cots.along(1)
    cots.across(0)
    for j in range(16):
        wide_mixed[:, pl.ds(j * dim, dim)] = own_mixed[j]

    def outward(j, _):
        at = span(j * 512, 512)
        hidden[:, at] = tok_ref[:, at].astype(F32) + jnp.dot(
            wide_mixed[...], wo_all[:, at], preferred_element_type=F32)
        return 0
    lax.fori_loop(0, 4, outward, 0)
    cots.along(2)
    cots.across(1)

    def square_two(r, _):
        at = span(r * 8, 8)
        x = hidden[at, :]
        mean = jnp.sum(x * x, axis=1, keepdims=True) / width
        line[at, :] = jnp.broadcast_to(lax.rsqrt(mean + eps), (8, dim))
        return 0
    lax.fori_loop(0, rows // 8, square_two, 0)

    def normalize_two(j, _):
        at = span(j * dim, dim)
        two[:, at] = (hidden[:, at] * line[...] * info[m, j, 1:2, :]).astype(BF)
        return 0
    lax.fori_loop(0, 16, normalize_two, 0)
    logits = jnp.zeros((16, rows), F32)
    for j in range(16):
        logits = logits + contract_last(info[m, j, 4:20, :].astype(BF), two[:, pl.ds(j * dim, dim)])
        gain_out[0:1, pl.ds(j * dim, dim)] = info[m, j, 0:1, :]
        gain_out[1:2, pl.ds(j * dim, dim)] = info[m, j, 1:2, :]
    gain_out[2:8, :] = jnp.zeros((6, width), F32)
    logits = jnp.exp(logits - jnp.max(logits, axis=0, keepdims=True))
    probs = logits / jnp.sum(logits, axis=0, keepdims=True)
    picks = jnp.transpose(jnp.concatenate(
        [routes_ref[...].astype(F32), jnp.full((rows, dim - 8), -1.0, F32)], axis=1))
    row16 = lax.broadcasted_iota(jnp.int32, (16, rows), 0).astype(F32)
    chosen = jnp.zeros((16, rows), F32)
    for k in range(8):
        chosen = jnp.where(row16 == picks[k : k + 1, :], 1.0, chosen)
    probs_out[...] = probs
    chosen_out[...] = chosen
    share_out[...] = probs * chosen
    cots.along(3)
    cots.corner(0)
    cots.across(2)
    cots.corner(1)
    cots.across(3)
    cots.corner(2)
    cots.corner(3)
    for step in range(4):
        cots.ready(step)
    for copy in (save_n1, save_wo, cot_own):
        copy.wait()
    swap.wait_send()
    for work in (hand, weights, share, back, first, outer, cots):
        work.finish()


def front(ident, *arrays):
    rows, width = arrays[0].shape
    every = 16 * rows
    mine = every // 2
    vmem = pl.BlockSpec(memory_space=pltpu.VMEM)
    hbm = pl.BlockSpec(memory_space=pl.ANY)

    def shape(*sizes, dtype=F32):
        return jax.ShapeDtypeStruct(sizes, dtype)
    return pl.pallas_call(
        front_body,
        out_shape=(
            shape(every, width, dtype=BF),
            shape(every, width, dtype=BF),
            shape(every, width, dtype=BF),
            shape(16, rows, 384, dtype=BF),
            shape(2, 16, 40, 128),
            shape(mine, 256),
            shape(mine, 384, dtype=BF),
            shape(16, 128),
            shape(8, rows, 128, dtype=BF),
            shape(8, 8, rows),
            shape(2, 8, rows, 128),
            shape(16, rows, 128, dtype=BF),
            shape(rows, width),
            shape(rows, width, dtype=BF),
            shape(16, rows),
            shape(16, rows),
            shape(16, rows),
            shape(8, 128),
            shape(8, width),
        ),
        in_specs=[vmem] * 14,
        out_specs=(hbm, hbm, hbm) + (vmem,) * 16,
        scratch_shapes=[
            pltpu.VMEM((40, 128), F32),
            pltpu.VMEM((8, rows, 384), BF),
            pltpu.VMEM((rows, width), BF),
            pltpu.VMEM((every, width), BF),
            pltpu.VMEM((every, width), BF),
            pltpu.VMEM((rows, width), BF),
            pltpu.VMEM((16, 16, 128), F32),
            pltpu.VMEM((16, 128), F32),
            pltpu.VMEM((rows, 128), F32),
        ]
        + [pltpu.SemaphoreType.DMA((1, 12, 4))] * 6
        + [pltpu.SemaphoreType.DMA((16,))] * 4
        + [pltpu.SemaphoreType.DMA((6,))]
        + chips_semaphores() * 2,
        compiler_params=pltpu.CompilerParams(collective_id=ident, has_side_effects=True,
                                             vmem_limit_bytes=56 << 20),
        name="front_%d" % ident,
    )(*arrays)


class Cores:
    def __init__(self, source, target, send, recv, local):
        s, z, m = place()
        self.c, self.m = s * 4 + z, m
        self.high, self.low = lax.div(self.c, 8), lax.rem(self.c, 8)
        self.same = self.high == m
        self.source, self.target, self.send, self.recv, self.local = source, target, send, recv, local

    def dev(self, i):
        j = 8 * self.m + i
        return (lax.div(j, 4), lax.rem(j, 4), self.high)

    def away(self, i):
        return jnp.logical_not(jnp.logical_and(self.same, self.low == i))

    def copy(self, i):
        return remote(self.source.at[i], self.target.at[self.low], self.send.at[i],
                      self.recv.at[self.low], self.dev(i))

    def mine(self):
        return pltpu.make_async_copy(self.source.at[self.low], self.target.at[self.low], self.local.at[0])

    def start(self, low=0, high=8):
        for i in range(low, high):
            pl.when(self.away(i))(lambda i=i: self.copy(i).start())

            def keep():
                self.mine().start()
            pl.when(jnp.logical_not(self.away(i)))(keep)

    def collect(self):
        for i in range(8):
            pl.when(self.away(i))(lambda i=i: remote(
                self.target.at[i], self.target.at[i], self.send.at[0], self.recv.at[i],
                self.dev(i)).wait_recv())
        pl.when(self.same)(lambda: self.mine().wait())

    def finish(self):
        for i in range(8):
            pl.when(self.away(i))(lambda i=i: self.copy(i).wait_send())


def cores_semaphores():
    return [pltpu.SemaphoreType.DMA((8,))] * 2 + [pltpu.SemaphoreType.DMA((1,))]


def call_all():
    s, z, m = place()
    high = lax.div(s * 4 + z, 8)
    call_chips()

    def cross():
        for i in range(8):
            j = 8 * m + i
            signal((lax.div(j, 4), lax.rem(j, 4), high))
    pl.when(high != m)(cross)


def await_all():
    s, z, m = place()
    high = lax.div(s * 4 + z, 8)
    pl.when(high != m)(lambda: pl.semaphore_wait(pltpu.get_barrier_semaphore(), 24))
    pl.when(high == m)(lambda: pl.semaphore_wait(pltpu.get_barrier_semaphore(), 16))


def rear_body(back_ref, prob_ref, probs_ref, chosen_ref, two_ref, out_ref, cot_ref, info,
              mixed_ref, rows3, raw, squares, lse, trig, gains, w3, tok_ref, gain_ref,
              wo_ref, n1_ref, moe_ref,
              gn_out, moe_out, q_out, k_out, v_out, out_grad, tok_out, tail_out,
              got, ga_ref, hidden_ref, wo_half, n1_half, moe, gn_part, mixed_line, ga_blocks, ga_plane, gm_send, gm, wsend, backs,
              dq, dk, dv, sums, gathered, line, dots, tail, out_mine, out_all,
              a0, a1, a2, a3, a4, a5, a6, a7, asend, arecv,
              b0, b1, b2, b3, b4, b5, b6, b7, bsend, brecv,
              msend, mrecv, csend, crecv, hsend, hrecv, tsend, trecv, psend, precv, osend, orecv, load, *rest):
    s, z, m = place()
    c = s * 4 + z
    pn = (s, z, 1 - m)
    rows, width = tok_ref.shape
    cut = width // 2
    dim = 128
    factor = dim ** (-0.5)
    loads = [
        pltpu.make_async_copy(wo_ref.at[span(m * cut, cut), :], wo_half, load.at[0]),
        pltpu.make_async_copy(moe_ref, moe, load.at[1]),
        pltpu.make_async_copy(n1_ref.at[:, span(m * cut, cut)], n1_half, load.at[2]),
        pltpu.make_async_copy(mixed_ref, mixed_line.at[span(m * cut, cut), span(z * dim, dim)], load.at[3]),
    ]
    for copy in loads:
        copy.start()
    call_all()
    order = far_planes(z)
    outer = Reduce(True, True, moe, moe, moe_out, (a0, a1, a2, a3, a4, a5, a6, a7), (asend, arecv))
    inner = Reduce(False, True, gn_part, gn_part, gn_out, (b0, b1, b2, b3, b4, b5, b6, b7), (bsend, brecv))
    prob = jnp.concatenate(
        [prob_ref[0, j, 0:1, :] + prob_ref[1, j, 0:1, :] for j in range(16)], axis=0)
    prob = prob * chosen_ref[...]
    probs = probs_ref[...]
    logits = (probs * (prob - jnp.sum(probs * prob, axis=0, keepdims=True))).astype(BF)
    tail[...] = jnp.zeros_like(tail)
    for j in range(16):
        at = pl.ds(j * dim, dim)
        tail[j, 3:19, :] = jnp.dot(logits, two_ref[:, at], preferred_element_type=F32)
        hidden_ref[:, at] = back_ref[:, at].astype(F32) + contract_first(
            logits, info[m, j, 4:20, :].astype(BF))

    def second_norm(r, acc):
        at = span(r * 16, 16)
        x = out_ref[at, :]
        grad = hidden_ref[at, :]
        inverse = lax.rsqrt(jnp.sum(x * x, axis=1, keepdims=True) / width + eps)
        scaled = grad * gain_ref[1:2, :]
        dot = jnp.sum(x * scaled, axis=1, keepdims=True) / width
        value = cot_ref[at, :].astype(F32) + (
            inverse * scaled - x * (inverse * inverse * inverse * dot))
        hidden_ref[at, :] = value
        ga_ref[at, :] = value.astype(BF)
        part = grad * x * inverse
        return acc + part[0:8] + part[8:16]
    acc = lax.fori_loop(0, rows // 16, second_norm, jnp.zeros((8, width), F32))
    acc = jnp.sum(acc, axis=0, keepdims=True)
    for j in range(16):
        tail[j, 1:2, :] = acc[:, j * dim : (j + 1) * dim]
    await_all()
    loads[1].wait()
    for at in order:
        outer.swap(at)
    lane = lax.broadcasted_iota(jnp.int32, (rows, dim), 1)
    give = Cores(gm_send, gm, *rest[:3])
    loads[0].wait()
    for t in range(2):
        value = contract_last(ga_ref[...], wo_half[pl.ds(t * 512, 512), :]).astype(BF)
        for i in range(4):
            gm_send[t * 4 + i] = value[:, i * dim : (i + 1) * dim]
        give.start(t * 4, t * 4 + 4)
    strip = Line([Part("line", mixed_ref, mixed_line)], msend, mrecv)
    spread = Spread([Part("cols", ga_blocks, ga_plane)], csend, crecv)

    wide = jnp.concatenate(
        [lax.rsqrt(squares[...] / width + eps), jnp.zeros((rows - 16, dim), F32)], axis=0)
    line[...] = jnp.transpose(wide)
    dk[...] = jnp.zeros_like(dk)
    dv[...] = jnp.zeros_like(dv)
    outer.first(order[0])
    outer.first(order[1])
    give.collect()
    outer.first(order[2])
    outer.first(order[3])

    def attend(b, _):
        seq = span(lax.div(b, 4) * 4 * rows, 4 * rows)
        at = span(b * rows, rows)
        query = rows3[at, pl.ds(0, dim)]
        key = rows3[seq, pl.ds(dim, dim)]
        value = rows3[seq, pl.ds(2 * dim, dim)]
        grad = gm[b]
        top = jnp.transpose(jnp.broadcast_to(lse[b, 0:1, :], (rows, dim)))[:, 0:1]
        delta = jnp.sum(grad.astype(F32) * mixed_ref[at, :].astype(F32), axis=1, keepdims=True)
        scores = contract_last(query, key)
        here = lax.broadcasted_iota(jnp.int32, scores.shape, 0) + lax.rem(b, 4) * rows
        allowed = lax.broadcasted_iota(jnp.int32, scores.shape, 1) <= here
        prob = jnp.where(allowed, jnp.exp(jnp.where(allowed, scores, neg_big) - top), 0.0)
        back = (prob * (contract_last(grad, value) - delta)).astype(BF)
        dv[seq, :] += contract_first(prob.astype(BF), grad)
        dk[seq, :] += contract_first(back, query)
        dq[at, :] = jnp.dot(back, key, preferred_element_type=F32) * factor
        return 0
    lax.fori_loop(0, 4, attend, 0)
    outer.second(order[0])
    outer.second(order[1])
    lax.fori_loop(4, 8, attend, 0)

    def column(source, r):
        return jnp.sum(jnp.where(lane == r, source, 0.0), axis=1, keepdims=True)

    def unturn(b, carry):
        total, gain_q, gain_k = carry
        at = span(b * rows, rows)
        out = []
        for which, grads in ((0, dq), (1, dk)):
            value = grads[at, :]
            value = value * trig[0, b] + pltpu.roll(value * trig[1, b], dim // 2, 1)
            plain = raw[at, pl.ds(which * dim, dim)]
            unit = plain * column(line[...], b + 8 * which)
            out.append(jnp.sum(value * unit, axis=0, keepdims=True))
            value = value * gains[which : which + 1, :]
            grads[at, :] = value
            dot = jnp.sum(plain * value, axis=1, keepdims=True)
            total = jnp.where(lane == b + 8 * which, dot, total)
        return total, gain_q + out[0], gain_k + out[1]
    zero = jnp.zeros((1, dim), F32)
    total, gain_q, gain_k = lax.fori_loop(0, 8, unturn, (jnp.zeros((rows, dim), F32), zero, zero))
    for j in range(16):
        tail[j, 2:3, :] = gain_q
        tail[j, 19:20, :] = gain_k
    sums[...] = jnp.transpose(total)[0:16, :]
    hand = Hand(lambda j: sums, lambda j: gathered.at[j], hsend, hrecv)
    hand.start()
    gathered[c] = sums[...]
    strip.start()
    for p in range(4):
        for q in range(4):
            ga_blocks[p, :, pl.ds(q * dim, dim)] = ga_ref[:, pl.ds((q * 4 + p) * dim, dim)]
    spread.start()
    ga_plane[span(c * rows, rows), :] = ga_blocks[z]
    outer.second(order[2])
    outer.third(order[0], 0)
    outer.second(order[3])
    outer.third(order[1], 1)
    hand.collect()
    summed = lax.fori_loop(1, 16, lambda j, acc: acc + gathered[j], gathered[0])
    dots[...] = jnp.transpose(jnp.concatenate([summed, jnp.zeros((rows - 16, dim), F32)], axis=0))

    def finish_rows(b, _):
        at = span(b * rows, rows)
        base = span((lax.rem(b, 4) * 4 + 2 * m + lax.div(b, 4)) * rows, rows)
        for which, grads in ((0, dq), (1, dk)):
            inverse = column(line[...], b + 8 * which)
            dot = column(dots[...], b + 8 * which)
            value = inverse * grads[at, :] - raw[at, pl.ds(which * dim, dim)] * (
                inverse * inverse * inverse * dot / width)
            backs[base, pl.ds(which * dim, dim)] = value.astype(BF)
        backs[base, pl.ds(2 * dim, dim)] = dv[at, :].astype(BF)
        return 0
    lax.fori_loop(0, 8, finish_rows, 0)

    def pair(at, core):
        part = backs.at[span((at * 4 + 2 * core) * rows, 2 * rows), :]
        return remote(part, part, psend.at[at], precv.at[at], pn)
    for at in range(4):
        pair(at, m).start()
    outer.third(order[2], 2)
    for at in range(4):
        pair(at, 1 - m).wait_recv()
    for at in order:
        here = span(at * 4 * rows, 4 * rows)
        gn_part[here, :] = contract_last(
            backs[here, :], w3[span(m * 8, 8)].reshape(cut, 3 * dim)).astype(BF)
        inner.first(at)
    outer.keep()
    strip.along(1)
    spread.along(1)
    loads[2].wait()

    def weight_tile(t):
        value = contract_first(n1_half[:, pl.ds(t * 256, 256)], backs[...]).astype(BF)
        wsend[2 * t] = value[:rows]
        wsend[2 * t + 1] = value[rows:]
    weight_tile(0)
    weight_tile(1)
    inner.second(order[0])
    weight_tile(2)
    inner.third(order[0], 0)
    inner.second(order[1])
    weight_tile(3)
    outer.close()
    weights = Cores(wsend, got, *rest[3:6])
    weights.start()
    strip.along(2)
    spread.along(2)
    spread.across(0)
    inner.third(order[1], 1)
    inner.second(order[2])
    inner.third(order[2], 2)
    inner.second(order[3])
    inner.keep()
    strip.along(3)
    spread.along(3)
    spread.across(1)
    spread.corner(0)
    inner.close()
    inner.landing()

    def last(r, acc):
        at = span(r * 16, 16)
        x = tok_ref[at, :].astype(F32)
        grad = gn_out[at, :].astype(F32)
        inverse = lax.rsqrt(jnp.sum(x * x, axis=1, keepdims=True) / width + eps)
        scaled = grad * gain_ref[0:1, :]
        dot = jnp.sum(x * scaled, axis=1, keepdims=True) / width
        tok_out[at, :] = hidden_ref[at, :] + inverse * scaled - x * (inverse * inverse * inverse * dot)
        part = grad * x * inverse
        return acc + part[0:8] + part[8:16]
    acc = lax.fori_loop(0, rows // 16, last, jnp.zeros((8, width), F32))
    acc = jnp.sum(acc, axis=0, keepdims=True)
    for j in range(16):
        tail[j, 0:1, :] = acc[:, j * dim : (j + 1) * dim]
    finale = Hand(lambda j: tail.at[j], lambda j: tail_out.at[m, j], tsend, trecv)
    finale.start()
    tail_out[m, c] = tail[c]
    spread.across(2)
    spread.corner(1)
    spread.across(3)
    spread.corner(2)
    spread.corner(3)
    loads[3].wait()
    for step in (1, 2, 3):
        strip.ready(step)
    strip_own = mixed_line.at[span((1 - m) * cut, cut), span(z * dim, dim)]
    strip.landed(0, strip.PO, z, strip_own)
    for step in range(4):
        spread.ready(step)

    value = contract_first(mixed_line[:, span(m * 256, 256)], ga_plane[...]).astype(BF)
    for q in range(4):
        out_mine[q] = value[:, q * dim : (q + 1) * dim]
    high = lax.div(c, 8)
    lower = lax.rem(s, 2)
    cross = remote(out_mine, out_all.at[m], osend.at[0], orecv.at[0], pn)

    def landing(q, core):
        return out_grad.at[q, core]

    def away(step, core):
        q = (None, flip_x(s), flip_y(s), 3 - s)[step]
        source = out_mine if core is None else out_all.at[1 - m]
        who = m if core is None else 1 - m
        at = step * 2 + (0 if core is None else 1)
        return remote(source.at[q], landing(lower, who), osend.at[at], orecv.at[at], (q, z, m))

    def lead():
        for step in (1, 2, 3):
            away(step, None).start()
        out_grad[lower, m] = out_mine[s]
        remote(out_all.at[1 - m], out_all.at[1 - m], osend.at[0], orecv.at[0], pn).wait_recv()
        for step in (1, 2, 3):
            away(step, 1).start()
        out_grad[lower, 1 - m] = out_all[1 - m, s]
    pl.when(high == m)(lead)
    pl.when(high != m)(lambda: cross.start())
    finale.collect()
    pair_tail = remote(tail_out.at[m], tail_out.at[m], osend.at[8], orecv.at[8], pn)
    pair_tail.start()
    weights.collect()
    for j in range(8):
        for n, ref in enumerate((q_out, k_out, v_out)):
            ref[:, pl.ds(j * dim, dim)] = got[j, :, pl.ds(n * dim, dim)].astype(F32)

    def arrive(step):
        q = (None, flip_x(s), flip_y(s), 3 - s)[step]

        def take():
            for second in (0, 1):
                who = 1 - m if second else m
                at = step * 2 + second
                target = landing(lax.rem(q, 2), who)
                remote(target, target, osend.at[at], orecv.at[at], pn).wait_recv()
        pl.when(lax.div(q, 2) == m)(take)
    for step in (1, 2, 3):
        arrive(step)
    other = tail_out.at[1 - m]
    remote(other, other, osend.at[8], orecv.at[8], pn).wait_recv()
    pair_tail.wait_send()
    pl.when(high != m)(lambda: cross.wait_send())

    def sent():
        for step in (1, 2, 3):
            away(step, None).wait_send()
            away(step, 1).wait_send()
    pl.when(high == m)(sent)
    outer.landing()
    for at in range(4):
        pair(at, m).wait_send()
    for work in (give, outer, inner, hand, finale, weights, strip, spread):
        work.finish()


def rear(ident, *arrays):
    rows, width = arrays[0].shape
    every = 16 * rows
    cut = width // 2
    vmem = pl.BlockSpec(memory_space=pltpu.VMEM)
    hbm = pl.BlockSpec(memory_space=pl.ANY)
    return pl.pallas_call(
        rear_body,
        out_shape=(
            jax.ShapeDtypeStruct((rows, width), BF),
            jax.ShapeDtypeStruct((rows, width), BF),
            jax.ShapeDtypeStruct((rows, cut), F32),
            jax.ShapeDtypeStruct((rows, cut), F32),
            jax.ShapeDtypeStruct((rows, cut), F32),
            jax.ShapeDtypeStruct((2, 2, 256, 128), BF),
            jax.ShapeDtypeStruct((rows, width), F32),
            jax.ShapeDtypeStruct((2, 16, 24, 128), F32),
        ),
        in_specs=[vmem] * 18 + [hbm] * 3,
        out_specs=(vmem,) * 8,
        scratch_shapes=[
            pltpu.VMEM((8, rows, 384), BF),
            pltpu.VMEM((rows, width), BF),
            pltpu.VMEM((rows, width), F32),
            pltpu.VMEM((cut, width), BF),
            pltpu.VMEM((every, cut), BF),
            pltpu.VMEM((every, width), BF),
            pltpu.VMEM((every, cut), BF),
            pltpu.VMEM((every, 512), BF),
            pltpu.VMEM((4, rows, 512), BF),
            pltpu.VMEM((every, 512), BF),
            pltpu.VMEM((8, rows, 128), BF),
            pltpu.VMEM((8, rows, 128), BF),
            pltpu.VMEM((8, rows, 384), BF),
            pltpu.VMEM((every, 384), BF),
            pltpu.VMEM((every // 2, 128), F32),
            pltpu.VMEM((every // 2, 128), F32),
            pltpu.VMEM((every // 2, 128), F32),
            pltpu.VMEM((16, 128), F32),
            pltpu.VMEM((16, 16, 128), F32),
            pltpu.VMEM((rows, 128), F32),
            pltpu.VMEM((rows, 128), F32),
            pltpu.VMEM((16, 24, 128), F32),
            pltpu.VMEM((4, 256, 128), BF),
            pltpu.VMEM((2, 4, 256, 128), BF),
        ]
        + reduce_buffers(True, rows, cut)
        + reduce_buffers(False, rows, cut)
        + [pltpu.SemaphoreType.DMA((1, 12, 4))] * 4
        + [pltpu.SemaphoreType.DMA((16,))] * 4
        + [pltpu.SemaphoreType.DMA((4,))] * 2
        + [pltpu.SemaphoreType.DMA((9,))] * 2
        + [pltpu.SemaphoreType.DMA((4,))]
        + cores_semaphores()
        + cores_semaphores(),
        compiler_params=pltpu.CompilerParams(collective_id=ident, has_side_effects=True,
                                             vmem_limit_bytes=66900000),
        name="rear_%d" % ident,
    )(*arrays)


HEADS = 16
HEAD_DIM = 128


eps = 1e-05
neg_big = -1e30


def rms_scale(rows, gain):
    return rows * lax.rsqrt(jnp.mean(rows * rows, axis=-1, keepdims=True) + eps) * gain


def rope_tables(positions):
    half = HEAD_DIM // 2
    freq = 10000.0 ** (-(jnp.arange(half).astype(jnp.float32) * 2.0 / HEAD_DIM))
    angle = positions.astype(jnp.float32)[:, None] * freq[None, :]
    return (jnp.cos(angle), jnp.sin(angle))


def rope_turn(normed, cosine, sine, factor):
    count = normed.shape[0]
    heads = normed.shape[1]
    width = normed.shape[2]
    first = normed[..., : width // 2]
    second = normed[..., width // 2 :]
    cos_rows = cosine[:, None, :]
    sin_rows = sine[:, None, :]
    turned = jnp.concatenate(
        [first * cos_rows - second * sin_rows, second * cos_rows + first * sin_rows], axis=-1
    )
    return (turned * factor).reshape(count, heads * width)


def contract_last(left, right):
    return lax.dot_general(
        left, right, (((1,), (1,)), ((), ())), preferred_element_type=jnp.float32
    )


def contract_first(left, right):
    return lax.dot_general(
        left, right, (((0,), (0,)), ((), ())), preferred_element_type=jnp.float32
    )


def sum_halves(part):
    return lax.psum(part.astype(jnp.bfloat16), "mp").astype(jnp.float32)


def general_body(
    tokens,
    positions,
    routes,
    cotangent,
    attention_gain,
    query_weight,
    key_weight,
    value_weight,
    query_gain,
    key_gain,
    output_weight,
    ffn_gain,
    router_weight,
    gate_weight,
    up_weight,
    down_weight,
):
    gathered = (
        lax.all_gather(query_weight, ("seq", "ctx"), axis=0, tiled=True),
        lax.all_gather(key_weight, ("seq", "ctx"), axis=0, tiled=True),
        lax.all_gather(value_weight, ("seq", "ctx"), axis=0, tiled=True),
        lax.all_gather(output_weight, ("seq", "ctx"), axis=1, tiled=True),
        lax.all_gather(router_weight, ("seq", "ctx"), axis=0, tiled=True),
        lax.all_gather(attention_gain, ("seq", "ctx"), axis=0, tiled=True),
        lax.all_gather(ffn_gain, ("seq", "ctx"), axis=0, tiled=True),
        lax.all_gather(query_gain, ("seq", "ctx"), axis=1, tiled=True),
        lax.all_gather(key_gain, ("seq", "ctx"), axis=1, tiled=True),
    )
    (
        query_full,
        key_full,
        value_full,
        output_full,
        router_full,
        gain_one_half,
        gain_two_half,
        query_gain_full,
        key_gain_full,
    ) = gathered
    rows = tokens.shape[1]
    width = tokens.shape[2]
    heads_here = query_gain.shape[0]
    local_width = query_weight.shape[1]
    all_columns = HEADS * HEAD_DIM
    factor = HEAD_DIM ** (-0.5)
    flat = tokens[0].astype(jnp.float32)
    grad_top = cotangent[0].astype(jnp.float32)
    gain_one = gain_one_half.astype(jnp.float32)
    gain_two = gain_two_half.astype(jnp.float32)
    query_gain_f = query_gain_full.astype(jnp.float32)
    key_gain_f = key_gain_full.astype(jnp.float32)
    normed_one = rms_scale(flat, gain_one).astype(jnp.bfloat16)
    query_raw = jnp.dot(normed_one, query_full, preferred_element_type=jnp.float32)
    key_raw = jnp.dot(normed_one, key_full, preferred_element_type=jnp.float32)
    value_rows = jnp.dot(normed_one, value_full, preferred_element_type=jnp.float32).astype(
        jnp.bfloat16
    )
    query_sq, key_sq = lax.psum(
        (jnp.sum(query_raw * query_raw, axis=-1), jnp.sum(key_raw * key_raw, axis=-1)), "mp"
    )
    query_inv = lax.rsqrt(query_sq / all_columns + eps)
    key_inv = lax.rsqrt(key_sq / all_columns + eps)
    query_unit = (query_raw * query_inv[:, None]).reshape(rows, heads_here, HEAD_DIM)
    key_unit = (key_raw * key_inv[:, None]).reshape(rows, heads_here, HEAD_DIM)
    cosine, sine = rope_tables(positions[0])
    query_rows = rope_turn(query_unit * query_gain_f, cosine, sine, factor).astype(jnp.bfloat16)
    key_rows = rope_turn(key_unit * key_gain_f, cosine, sine, 1.0).astype(jnp.bfloat16)
    keys_all, values_all = (
        lax.all_gather(key_rows, "ctx", axis=0, tiled=True),
        lax.all_gather(value_rows, "ctx", axis=0, tiled=True),
    )
    ctx_count = lax.axis_size("ctx")
    length = rows * ctx_count
    first_row = lax.axis_index("ctx") * rows
    last_row = first_row + rows - 1
    query_pos = first_row + jnp.arange(rows, dtype=jnp.int32)
    block = min(512, length)
    blocks = length // block
    query3 = query_rows.reshape(rows, heads_here, HEAD_DIM)

    def forward_block(carry, index):
        start = index * block

        def forward_work(state):
            top, total, acc = state
            keys = lax.dynamic_slice_in_dim(keys_all, start, block, 0).reshape(
                block, heads_here, HEAD_DIM
            )
            values = lax.dynamic_slice_in_dim(values_all, start, block, 0).reshape(
                block, heads_here, HEAD_DIM
            )
            scores = jnp.einsum("qhd,khd->hqk", query3, keys, preferred_element_type=jnp.float32)
            allowed = (start + jnp.arange(block, dtype=jnp.int32))[None, :] <= query_pos[:, None]
            scores = jnp.where(allowed[None], scores, neg_big)
            new_top = jnp.maximum(top, jnp.max(scores, axis=-1))
            weights = jnp.where(allowed[None], jnp.exp(scores - new_top[..., None]), 0.0)
            fade = jnp.exp(top - new_top)
            total = total * fade + jnp.sum(weights, axis=-1)
            acc = acc * fade[..., None] + jnp.einsum(
                "hqk,khd->hqd",
                weights.astype(jnp.bfloat16),
                values,
                preferred_element_type=jnp.float32,
            )
            return (new_top, total, acc)

        return (lax.cond(start <= last_row, forward_work, lambda state: state, carry), None)

    start_state = (
        jnp.full((heads_here, rows), neg_big, jnp.float32),
        jnp.zeros((heads_here, rows), jnp.float32),
        jnp.zeros((heads_here, rows, HEAD_DIM), jnp.float32),
    )
    (top, total, acc), _ = lax.scan(forward_block, start_state, jnp.arange(blocks, dtype=jnp.int32))
    mixed = (
        (acc / total[..., None]).transpose(1, 0, 2).reshape(rows, local_width).astype(jnp.bfloat16)
    )
    lse = top + jnp.log(total)
    attn = lax.psum(jnp.dot(mixed, output_full, preferred_element_type=jnp.float32), "mp")
    hidden = flat + attn
    normed_two = rms_scale(hidden, gain_two).astype(jnp.bfloat16)
    logits = jnp.dot(normed_two, router_full, preferred_element_type=jnp.float32)
    probs = jax.nn.softmax(logits, axis=-1)
    route_rows = routes[0]
    experts = router_full.shape[1]
    top_count = route_rows.shape[1]
    choose = (route_rows[:, :, None] == jnp.arange(experts, dtype=jnp.int32)[None, None, :]).astype(
        jnp.float32
    )
    share = jnp.sum(choose * probs[:, None, :], axis=-1)
    assign = rows * top_count
    capacity = assign * 3 // (2 * experts)
    expert_of = route_rows.reshape(assign)
    onehot = (expert_of[:, None] == jnp.arange(experts, dtype=jnp.int32)[None, :]).astype(jnp.int32)
    rank = jnp.sum(onehot * jnp.cumsum(onehot, axis=0), axis=1) - 1
    place = expert_of * capacity + rank
    table = (
        jnp.full((experts * capacity,), assign, jnp.int32)
        .at[place]
        .set(jnp.arange(assign, dtype=jnp.int32))
    )
    valid = table < assign
    safe = jnp.minimum(table, assign - 1)
    outgoing = jnp.where(
        valid[:, None], normed_two[safe // top_count], jnp.zeros((), jnp.bfloat16)
    ).reshape(experts, capacity, width)
    gate_here = gate_weight[0]
    up_here = up_weight[0]
    down_here = down_weight[0]
    received = lax.all_to_all(outgoing, ("seq", "ctx"), split_axis=0, concat_axis=0, tiled=True)
    sources = received.shape[0]
    slots = received.shape[1]
    inputs = received.reshape(sources * slots, width)
    gate = jnp.dot(inputs, gate_here, preferred_element_type=jnp.float32)
    up = jnp.dot(inputs, up_here, preferred_element_type=jnp.float32)
    act = (gate * jax.nn.sigmoid(gate) * up).astype(jnp.bfloat16)
    result = jnp.dot(act, down_here, preferred_element_type=jnp.float32).reshape(
        sources, slots, width
    )
    result = sum_halves(result)
    returned = lax.all_to_all(
        result.astype(jnp.bfloat16), ("seq", "ctx"), split_axis=0, concat_axis=0, tiled=True
    ).astype(result.dtype)
    per_assign = returned.reshape(experts * capacity, width)[place].reshape(rows, top_count, width)
    combined = jnp.sum(share[:, :, None] * per_assign, axis=1)
    layer_output = (hidden + combined).astype(jnp.bfloat16)[None]
    grad_share_part = jnp.sum(per_assign * grad_top[:, None, :], axis=-1)
    grad_result = (
        (share[:, :, None] * grad_top[:, None, :]).astype(jnp.bfloat16).reshape(assign, width)
    )
    grad_slots = jnp.where(valid[:, None], grad_result[safe], jnp.zeros((), jnp.bfloat16)).reshape(
        experts, capacity, width
    )
    incoming_rows, incoming_grads = (
        lax.all_to_all(outgoing, ("seq", "ctx"), split_axis=0, concat_axis=0, tiled=True),
        lax.all_to_all(grad_slots, ("seq", "ctx"), split_axis=0, concat_axis=0, tiled=True),
    )
    sources = incoming_rows.shape[0]
    inputs = incoming_rows.reshape(sources * capacity, width)
    grads_in = incoming_grads.reshape(sources * capacity, width)
    gate = jnp.dot(inputs, gate_here, preferred_element_type=jnp.float32)
    up = jnp.dot(inputs, up_here, preferred_element_type=jnp.float32)
    sig = jax.nn.sigmoid(gate)
    act = (gate * sig * up).astype(jnp.bfloat16)
    grad_act = contract_last(grads_in, down_here)
    down_grad = contract_first(act, grads_in)
    grad_gate = (grad_act * up * sig * (1.0 + gate * (1.0 - sig))).astype(jnp.bfloat16)
    grad_up = (grad_act * gate * sig).astype(jnp.bfloat16)
    gate_grad = contract_first(inputs, grad_gate)
    up_grad = contract_first(inputs, grad_up)
    back = (contract_last(grad_gate, gate_here) + contract_last(grad_up, up_here)).reshape(
        sources, capacity, width
    )
    back_home = lax.all_to_all(
        back.astype(jnp.bfloat16), ("seq", "ctx"), split_axis=0, concat_axis=0, tiled=True
    ).astype(back.dtype)
    moe_part = jnp.sum(
        back_home.reshape(experts * capacity, width)[place].reshape(rows, top_count, width), axis=1
    )
    share_send = jnp.zeros_like(grad_share_part)
    grad_norm_moe, share_summed = lax.psum((moe_part, share_send), "mp")
    grad_share = grad_share_part + share_summed
    grad_prob = jnp.sum(choose * grad_share[:, :, None], axis=1)
    grad_logits = (probs * (grad_prob - jnp.sum(probs * grad_prob, axis=-1, keepdims=True))).astype(
        jnp.bfloat16
    )
    router_grad = contract_first(normed_two, grad_logits)
    grad_normed_two = grad_norm_moe + contract_last(grad_logits, router_full)
    _, pull_two = jax.vjp(rms_scale, hidden, gain_two)
    grad_hidden_part, ffn_gain_grad = pull_two(grad_normed_two)
    grad_hidden = grad_top + grad_hidden_part
    grad_attn = grad_hidden.astype(jnp.bfloat16)
    output_grad = contract_first(mixed, grad_attn)
    grad_mixed = contract_last(grad_attn, output_full).astype(jnp.bfloat16)
    grad3 = grad_mixed.reshape(rows, heads_here, HEAD_DIM)
    delta = jnp.sum(
        grad3.astype(jnp.float32) * mixed.reshape(rows, heads_here, HEAD_DIM).astype(jnp.float32),
        axis=-1,
    ).T

    def backward_block(query_acc, index):
        start = index * block

        def backward_work(acc_now):
            keys = lax.dynamic_slice_in_dim(keys_all, start, block, 0).reshape(
                block, heads_here, HEAD_DIM
            )
            values = lax.dynamic_slice_in_dim(values_all, start, block, 0).reshape(
                block, heads_here, HEAD_DIM
            )
            scores = jnp.einsum("qhd,khd->hqk", query3, keys, preferred_element_type=jnp.float32)
            allowed = (start + jnp.arange(block, dtype=jnp.int32))[None, :] <= query_pos[:, None]
            scores = jnp.where(allowed[None], scores, neg_big)
            prob = jnp.where(allowed[None], jnp.exp(scores - lse[..., None]), 0.0)
            value_part = jnp.einsum(
                "hqk,qhd->khd", prob.astype(jnp.bfloat16), grad3, preferred_element_type=jnp.float32
            )
            grad_prob_block = jnp.einsum(
                "qhd,khd->hqk", grad3, values, preferred_element_type=jnp.float32
            )
            grad_scores = (prob * (grad_prob_block - delta[..., None])).astype(jnp.bfloat16)
            acc_now = acc_now + jnp.einsum(
                "hqk,khd->hqd", grad_scores, keys, preferred_element_type=jnp.float32
            )
            key_part = jnp.einsum(
                "hqk,qhd->khd", grad_scores, query3, preferred_element_type=jnp.float32
            )
            return (
                acc_now,
                key_part.reshape(block, local_width),
                value_part.reshape(block, local_width),
            )

        def skip(acc_now):
            empty = jnp.zeros((block, local_width), jnp.float32)
            return (acc_now, empty, empty)

        acc_next, key_part, value_part = lax.cond(start <= last_row, backward_work, skip, query_acc)
        return (acc_next, (key_part, value_part))

    query_acc, (key_blocks, value_blocks) = lax.scan(
        backward_block,
        jnp.zeros((heads_here, rows, HEAD_DIM), jnp.float32),
        jnp.arange(blocks, dtype=jnp.int32),
    )
    grad_keys, grad_values = (
        lax.psum_scatter(
            key_blocks.reshape(length, local_width).astype(jnp.bfloat16),
            "ctx",
            scatter_dimension=0,
            tiled=True,
        ).astype(jnp.float32),
        lax.psum_scatter(
            value_blocks.reshape(length, local_width).astype(jnp.bfloat16),
            "ctx",
            scatter_dimension=0,
            tiled=True,
        ).astype(jnp.float32),
    )
    grad_queries = query_acc.transpose(1, 0, 2).reshape(rows, local_width)
    _, pull_query = jax.vjp(
        lambda normed: rope_turn(normed, cosine, sine, factor), query_unit * query_gain_f
    )
    (grad_query_normed,) = pull_query(grad_queries)
    _, pull_key = jax.vjp(
        lambda normed: rope_turn(normed, cosine, sine, 1.0), key_unit * key_gain_f
    )
    (grad_key_normed,) = pull_key(grad_keys)
    query_gain_grad = jnp.sum(grad_query_normed * query_unit, axis=0)
    key_gain_grad = jnp.sum(grad_key_normed * key_unit, axis=0)
    query_scaled = (grad_query_normed * query_gain_f).reshape(rows, local_width)
    key_scaled = (grad_key_normed * key_gain_f).reshape(rows, local_width)
    query_dot, key_dot = lax.psum(
        (jnp.sum(query_raw * query_scaled, axis=-1), jnp.sum(key_raw * key_scaled, axis=-1)), "mp"
    )
    grad_query_raw = (
        query_inv[:, None] * query_scaled
        - query_raw * (query_inv * query_inv * query_inv * query_dot / all_columns)[:, None]
    )
    grad_key_raw = (
        key_inv[:, None] * key_scaled
        - key_raw * (key_inv * key_inv * key_inv * key_dot / all_columns)[:, None]
    )
    query_half = grad_query_raw.astype(jnp.bfloat16)
    key_half = grad_key_raw.astype(jnp.bfloat16)
    value_half = grad_values.astype(jnp.bfloat16)
    query_grad = contract_first(normed_one, query_half)
    key_grad = contract_first(normed_one, key_half)
    value_grad = contract_first(normed_one, value_half)
    normed_part = (
        contract_last(query_half, query_full)
        + contract_last(key_half, key_full)
        + contract_last(value_half, value_full)
    )
    grad_normed_one = lax.psum(normed_part.astype(jnp.bfloat16), "mp").astype(jnp.float32)
    _, pull_one = jax.vjp(rms_scale, flat, gain_one)
    grad_flat_part, attention_gain_grad = pull_one(grad_normed_one)
    tokens_grad = (grad_hidden + grad_flat_part)[None]
    owned = (
        lax.psum_scatter(query_grad, ("seq", "ctx"), scatter_dimension=0, tiled=True),
        lax.psum_scatter(key_grad, ("seq", "ctx"), scatter_dimension=0, tiled=True),
        lax.psum_scatter(value_grad, ("seq", "ctx"), scatter_dimension=0, tiled=True),
        lax.psum_scatter(output_grad, ("seq", "ctx"), scatter_dimension=1, tiled=True),
        lax.psum_scatter(router_grad, ("seq", "ctx"), scatter_dimension=0, tiled=True),
        lax.psum_scatter(attention_gain_grad, ("seq", "ctx"), scatter_dimension=0, tiled=True),
        lax.psum_scatter(ffn_gain_grad, ("seq", "ctx"), scatter_dimension=0, tiled=True),
        lax.psum_scatter(query_gain_grad, ("seq", "ctx"), scatter_dimension=1, tiled=True),
        lax.psum_scatter(key_gain_grad, ("seq", "ctx"), scatter_dimension=1, tiled=True),
    )
    (
        query_owned,
        key_owned,
        value_owned,
        output_owned,
        router_owned,
        gain_one_owned,
        gain_two_owned,
        query_gain_owned,
        key_gain_owned,
    ) = owned
    return (
        layer_output,
        tokens_grad,
        gain_one_owned,
        query_owned,
        key_owned,
        value_owned,
        query_gain_owned,
        key_gain_owned,
        output_owned,
        gain_two_owned,
        router_owned,
        gate_grad[None],
        up_grad[None],
        down_grad[None],
    )


def fast_body(
    tokens, positions, routes, cotangent, attention_gain, query_weight, key_weight, value_weight,
    query_gain, key_gain, output_weight, ffn_gain, router_weight, gate_weight, up_weight,
    down_weight,
):
    s, z, m = place()
    c = s * 4 + z
    rows, width = tokens.shape[1:]
    cut = width // 2
    half = np.arange(HEAD_DIM // 2).astype(np.float32)
    freq = np.float32(10000.0) ** (-(half * np.float32(2.0) / np.float32(HEAD_DIM)))
    freq = jnp.asarray(np.tile(freq, (8, 2)), F32)
    (normed, out_full, all_top, weights3, info, raw, rows3, squares, mixed, lse, trig, _, hidden,
     normed_two, probs, chosen, share, head_gains, gains) = front(
        0, tokens[0], attention_gain.reshape(1, rows), ffn_gain.reshape(1, rows), positions,
        router_weight.T, query_gain, key_gain, routes[0], query_weight, key_weight, value_weight,
        output_weight, cotangent[0], freq)
    grad_two, prob_out, moe, gate_grad, up_grad, down_grad = experts(
        5, normed_two, share, all_top, gate_weight[0], up_weight[0], down_weight[0])
    _, moe_sum, query_grad, key_grad, value_grad, output_grad, tokens_grad, tail = rear(
        6, grad_two, prob_out, probs, chosen, normed_two, hidden, cotangent[0], info,
        mixed.reshape(8 * rows, HEAD_DIM), rows3, raw, squares, lse, trig, head_gains, weights3,
        tokens[0], gains, out_full, normed, moe)
    layer_output = (hidden + moe_sum.astype(F32)).astype(BF)
    summed = jnp.sum(tail[0], axis=0)
    gain_grads = lax.dynamic_slice_in_dim(tail[0] + tail[1], m * 8, 8, 0)
    gain_grads = lax.dynamic_slice_in_dim(gain_grads, c * 8, 8, 2)
    return (
        layer_output[None],
        tokens_grad[None],
        summed[0],
        query_grad,
        key_grad,
        value_grad,
        gain_grads[:, 2],
        gain_grads[:, 19],
        output_grad.reshape(cut, HEAD_DIM).astype(F32),
        summed[1],
        summed[3:19].T,
        gate_grad[None],
        up_grad[None],
        down_grad[None],
    )


def grid_fits(tokens, router_weight):
    sizes = tuple(lax.axis_size(name) for name in ("seq", "ctx", "mp"))
    return sizes == (4, 4, 2) and tokens.shape == (1, 128, 2048) and router_weight.shape == (128, 16)


def body(*args):
    if grid_fits(args[0], args[12]):
        return fast_body(*args)
    return general_body(*args)


def solution(mesh):
    placed = (
        P("seq", "ctx", None),
        P("seq", "ctx"),
        P("seq", "ctx", None),
        P("seq", "ctx", None),
        P(("seq", "ctx")),
        P(("seq", "ctx"), "mp"),
        P(("seq", "ctx"), "mp"),
        P(("seq", "ctx"), "mp"),
        P("mp", ("seq", "ctx")),
        P("mp", ("seq", "ctx")),
        P("mp", ("seq", "ctx")),
        P(("seq", "ctx")),
        P(("seq", "ctx"), None),
        P(("seq", "ctx"), None, "mp"),
        P(("seq", "ctx"), None, "mp"),
        P(("seq", "ctx"), "mp", None),
    )
    return jax.shard_map(
        body,
        mesh=mesh,
        in_specs=placed,
        out_specs=(
            P("seq", "ctx", None),
            P("seq", "ctx", None),
            P(("seq", "ctx")),
            P(("seq", "ctx"), "mp"),
            P(("seq", "ctx"), "mp"),
            P(("seq", "ctx"), "mp"),
            P("mp", ("seq", "ctx")),
            P("mp", ("seq", "ctx")),
            P("mp", ("seq", "ctx")),
            P(("seq", "ctx")),
            P(("seq", "ctx"), None),
            P(("seq", "ctx"), None, "mp"),
            P(("seq", "ctx"), None, "mp"),
            P(("seq", "ctx"), "mp", None),
        ),
        check_vma=False,
    )
```

```python
import functools

import jax
import jax.numpy as jnp
import numpy as np
from jax import lax
from jax.experimental import pallas as pl
from jax.experimental.pallas import tpu as pltpu
from jax.sharding import PartitionSpec as P

MESH = pl.DeviceIdType.MESH
BF = jnp.bfloat16
F32 = jnp.float32


def place():
    s = lax.axis_index("seq")
    z = lax.axis_index("ctx")
    m = lax.axis_index("mp")
    return s, z, m


def flip_x(s):
    return s + 1 - 2 * lax.rem(s, 2)


def flip_y(s):
    return s + 2 - 4 * lax.div(s, 2)


def remote(src, dst, send, recv, device):
    return pltpu.make_async_remote_copy(
        src_ref=src, dst_ref=dst, send_sem=send, recv_sem=recv,
        device_id=device, device_id_type=MESH,
    )


def signal(device):
    pl.semaphore_signal(
        pltpu.get_barrier_semaphore(), inc=1, device_id=device, device_id_type=MESH
    )


def when(cond, fn):
    if cond is True:
        fn()
    else:
        pl.when(cond)(fn)


def near_planes(z):
    return (z, flip_x(z), 2 - lax.div(z, 2), 3 - 3 * lax.div(z, 2))


def far_planes(z):
    return (3 - 3 * lax.div(z, 2), lax.rem(2 + 3 * z, 5), 1 + lax.rem(z, 2), z)


def span(start, size):
    return pl.ds(pl.multiple_of(start, size), size)


class Part:
    def __init__(self, kind, source, target):
        self.kind = kind
        self.source = source
        self.target = target
        self.whole = kind == "small"

    def own(self, m):
        if self.kind == "rows":
            width = self.source.shape[1] // 2
            return self.source.at[:, span(m * width, width)]
        return self.source

    def piece(self, row, plane, core, half=None):
        ref = self.target
        if self.kind == "small":
            return ref.at[plane * 4 + row, core]
        if self.kind == "line":
            rows = self.source.shape[0]
            return ref.at[span(core * rows, rows), span(plane * 128, 128)]
        if self.kind == "cols":
            rows = self.source.shape[1] // 2
            base = (row * 4 + plane) * 2 * rows + core * rows
            if half is None:
                return ref.at[span(base, rows), :]
            return ref.at[span(base + half * (rows // 2), rows // 2), :]
        if self.kind == "rows":
            rows, width = self.source.shape[0], self.source.shape[1] // 2
            cols = span(core * width, width)
            base = (plane * 4 + row) * rows
        elif self.kind == "chips":
            rows, width = self.source.shape[0], self.source.shape[1] // 2
            cols = span(core * width, width)
            base = (row * 4 + plane) * rows
        else:
            rows = self.source.shape[0]
            cols = span((row * 4 + plane) * 128, 128)
            base = core * rows
        if half is None:
            return ref.at[span(base, rows), cols]
        return ref.at[span(base + half * (rows // 2), rows // 2), cols]

    def mirrored(self):
        return self.kind in ("rows", "chips", "cols")


class Gather:
    Z, X, Y, DX, DY, PO, PX, PY, P0, P1, UP, DN = range(12)

    def __init__(self, parts, send, recv):
        self.parts, self.send, self.recv = parts, send, recv
        s, z, m = place()
        self.s, self.z, self.m = s, z, m
        self.lines = (s, flip_x(s), flip_y(s), 3 - s)
        self.xn, self.yn, self.pn = (self.lines[1], z, m), (self.lines[2], z, m), (s, z, 1 - m)
        self.planes = near_planes(z)
        self.pending = []

    def own(self, k):
        part = self.parts[k]
        if part.kind == "chips":
            width = part.source.shape[1] // 2
            return part.source.at[:, span(self.m * width, width)]
        return part.own(self.m)

    def push(self, cond, k, kind, at, source, target, device, out=None):
        out = kind if out is None else out
        copy = lambda: remote(source, target, self.send.at[k, out, at], self.recv.at[k, kind, at], device)
        when(cond, lambda: copy().start())
        self.pending.append((cond, copy))

    def landed(self, k, kind, at, target):
        remote(target, target, self.send.at[k, kind, at], self.recv.at[k, kind, at], self.pn).wait_recv()

    def fan(self, k, at, source):
        target = self.parts[k].piece(self.s, at, self.m)
        self.push(True, k, self.X, at, source, target, self.xn)
        self.push(True, k, self.Y, at, source, target, self.yn)

    def start(self):
        z, at = self.z, self.z
        for k, part in enumerate(self.parts):
            source, target = self.own(k), part.piece(self.s, at, self.m)
            self.push(z < 3, k, self.Z, at, source, target, (self.s, z + 1, self.m), self.UP)
            self.push(z > 0, k, self.Z, at, source, target, (self.s, z - 1, self.m), self.DN)
            self.fan(k, at, source)
            if not part.mirrored():
                self.push(True, k, self.PO, at, source, target, self.pn)

    def along(self, step):
        z, at = self.z, self.planes[step]
        goal = 3 - z if step == 1 else 3 * z - 3
        inner = jnp.logical_and(z > 0, z < 3)
        for k, part in enumerate(self.parts):
            target = part.piece(self.s, at, self.m)
            self.landed(k, self.Z, at, target)
            self.push(inner, k, self.Z, at, target, target, (self.s, goal, self.m), self.UP)
            self.fan(k, at, target)
            self.push(True, k, self.PO, at, target, target, self.pn)

    def across(self, step):
        at = self.planes[step]
        for k, part in enumerate(self.parts):
            whole = part.piece(self.lines[1], at, self.m)
            half = whole if part.whole else part.piece(self.lines[1], at, self.m, 0)
            self.landed(k, self.X, at, whole)
            self.push(True, k, self.DY, at, half, half, self.yn)
            self.push(True, k, self.PX, at, whole, whole, self.pn)
            whole = part.piece(self.lines[2], at, self.m)
            self.landed(k, self.Y, at, whole)
            if not part.whole:
                half = part.piece(self.lines[2], at, self.m, 1)
                self.push(True, k, self.DX, at, half, half, self.xn)
            self.push(True, k, self.PY, at, whole, whole, self.pn)

    def corner(self, step):
        at, far = self.planes[step], self.lines[3]
        for k, part in enumerate(self.parts):
            half = part.piece(far, at, self.m, None if part.whole else 0)
            self.landed(k, self.DY, at, half)
            self.push(True, k, self.P0, at, half, half, self.pn)
            if not part.whole:
                half = part.piece(far, at, self.m, 1)
                self.landed(k, self.DX, at, half)
                self.push(True, k, self.P1, at, half, half, self.pn)

    def ready(self, step):
        at, other = self.planes[step], 1 - self.m
        for k, part in enumerate(self.parts):
            if step > 0 or not part.mirrored():
                self.landed(k, self.PO, at, part.piece(self.s, at, other))
            self.landed(k, self.PX, at, part.piece(self.lines[1], at, other))
            self.landed(k, self.PY, at, part.piece(self.lines[2], at, other))
            self.landed(k, self.P0, at, part.piece(self.lines[3], at, other, None if part.whole else 0))
            if not part.whole:
                self.landed(k, self.P1, at, part.piece(self.lines[3], at, other, 1))

    def finish(self):
        for cond, copy in self.pending:
            when(cond, lambda copy=copy: copy().wait_send())


class Line(Gather):
    def fan(self, k, at, source):
        pass

    def ready(self, step):
        at = self.planes[step]
        for k, part in enumerate(self.parts):
            self.landed(k, self.PO, at, part.piece(self.s, at, 1 - self.m))


class Spread(Gather):
    def block(self, plane):
        source = self.parts[0].source
        rows = source.shape[1] // 2
        return source.at[plane, span(self.m * rows, rows), :]

    def start(self):
        z = self.z
        target = self.parts[0].piece(self.s, z, self.m)
        for step in (1, 2, 3):
            plane = lax.rem(z + step, 4)
            out = (self.UP, self.DN, self.Z)[step - 1]
            self.push(True, 0, self.Z, z, self.block(plane), target, (self.s, plane, self.m), out)
        self.fan(0, z, self.block(z))

    def along(self, step):
        at = self.planes[step]
        target = self.parts[0].piece(self.s, at, self.m)
        self.landed(0, self.Z, at, target)
        self.fan(0, at, target)
        self.push(True, 0, self.PO, at, target, target, self.pn)


def call_chips():
    s, z, m = place()
    c = s * 4 + z
    for step in range(1, 16):
        j = lax.rem(c + step, 16)
        signal((lax.div(j, 4), lax.rem(j, 4), m))
    signal((s, z, 1 - m))


def add_rows(put, sources, count, step=16):
    def run(r, _):
        at = span(r * step, step)
        total = sources[0](at)
        for source in sources[1:]:
            total = total + source(at)
        put(at, total)
        return 0
    lax.fori_loop(0, count // step, run, 0)


def shifted(at, base, step=16):
    return pl.ds(pl.multiple_of(at.start + base, step), step)


class Reduce:
    def __init__(self, pair, by_plane, src, acc, out, bufs, sems):
        self.pair, self.by_plane, self.src, self.acc, self.out = pair, by_plane, src, acc, out
        (self.buf0, self.bufx, self.bufy, self.bufx2, self.bufy2, self.zbuf, self.zsend, self.fin) = bufs
        self.send, self.recv = sems
        s, z, m = place()
        self.s, self.z, self.m = s, z, m
        self.xn, self.yn, self.pn = (flip_x(s), z, m), (flip_y(s), z, m), (s, z, 1 - m)
        self.lines = (s, flip_x(s), flip_y(s), 3 - s)
        self.rows = self.fin.shape[0]
        self.half = self.rows // 2
        self.width = self.fin.shape[1]
        self.mine = span(m * self.width, self.width)
        self.cols = self.mine if acc.shape[1] > self.width else slice(None)
        self.other = span((1 - m) * self.width, self.width)
        self.pending = []

    def push(self, kind, at, source, target, device):
        copy = lambda: remote(source, target, self.send.at[kind, at], self.recv.at[kind, at], device)
        copy().start()
        self.pending.append(copy)

    def landed(self, kind, at, target):
        remote(target, target, self.send.at[kind, at], self.recv.at[kind, at], self.pn).wait_recv()

    def base(self, at, q, by_plane=None):
        by_plane = self.by_plane if by_plane is None else by_plane
        row = self.lines[q]
        return (at * 4 + row if by_plane else row * 4 + at) * self.rows

    def held(self, at, q):
        return self.base(at, q, self.pair or self.by_plane)

    def swap(self, at):
        for q in (3, 1, 2, 0):
            self.push(q, at, self.src.at[span(self.base(at, q), self.rows), self.other],
                      self.buf0.at[at, q], self.pn)

    def block(self, at, q, lo):
        return self.acc.at[pl.ds(pl.multiple_of(self.held(at, q) + lo, self.half), self.half), self.cols]

    def first(self, at):
        for q in (3, 1, 2, 0):
            if self.pair:
                self.landed(q, at, self.buf0.at[at, q])
                base = self.base(at, q)
                held = self.held(at, q)

                def put(r, v, held=held):
                    self.acc[shifted(r, held), self.cols] = v.astype(BF)
                add_rows(put, [
                    lambda r, base=base: self.src[shifted(r, base), self.mine].astype(F32),
                    lambda r, q=q: self.buf0[at, q, r].astype(F32)], self.rows)
            if q == 3:
                self.push(4, at, self.block(at, 3, 0), self.bufx.at[at, 1], self.xn)
                self.push(5, at, self.block(at, 3, self.half), self.bufy.at[at, 1], self.yn)
            if q == 1:
                self.push(6, at, self.block(at, 1, 0), self.bufx.at[at, 0], self.xn)
            if q == 2:
                self.push(7, at, self.block(at, 2, self.half), self.bufy.at[at, 0], self.yn)

    def local(self, at, q, lo):
        held = self.held(at, q) + lo
        return lambda r: self.acc[shifted(r, held), self.cols].astype(F32)

    def second(self, at):
        self.landed(4, at, self.bufx.at[at, 1])

        def put_x(r, v):
            self.bufx[at, 1, r] = v.astype(BF)
        add_rows(put_x, [self.local(at, 2, 0), lambda r: self.bufx[at, 1, r].astype(F32)], self.half)
        self.push(8, at, self.bufx.at[at, 1], self.bufy2.at[at], self.yn)
        self.landed(5, at, self.bufy.at[at, 1])

        def put_y(r, v):
            self.bufy[at, 1, r] = v.astype(BF)
        add_rows(put_y, [self.local(at, 1, self.half), lambda r: self.bufy[at, 1, r].astype(F32)], self.half)
        self.push(9, at, self.bufy.at[at, 1], self.bufx2.at[at], self.xn)

    def settle(self, at, put_low, put_high):
        half = self.half
        self.landed(6, at, self.bufx.at[at, 0])
        self.landed(8, at, self.bufy2.at[at])
        self.landed(7, at, self.bufy.at[at, 0])
        self.landed(9, at, self.bufx2.at[at])
        add_rows(put_low, [self.local(at, 0, 0), lambda r: self.bufx[at, 0, r].astype(F32),
                           lambda r: self.bufy2[at, r].astype(F32)], half)
        add_rows(put_high, [self.local(at, 0, half), lambda r: self.bufy[at, 0, r].astype(F32),
                            lambda r: self.bufx2[at, r].astype(F32)], half)

    def third(self, at, slot):
        half = self.half

        def low(r, v):
            self.zsend[slot, r] = v.astype(BF)

        def high(r, v):
            self.zsend[slot, shifted(r, half)] = v.astype(BF)
        self.settle(at, low, high)
        copy = lambda: remote(self.zsend.at[slot], self.zbuf.at[self.z], self.send.at[12, slot],
                              self.recv.at[10, self.z], (self.s, at, self.m))
        copy().start()
        self.pending.append(copy)

    def keep(self):
        half = self.half

        def low(r, v):
            self.fin[r] = v

        def high(r, v):
            self.fin[shifted(r, half)] = v
        self.settle(self.z, low, high)

    def close(self):
        mine, other = self.mine, self.other
        others = [lax.rem(self.z + step, 4) for step in (1, 2, 3)]
        for at in others:
            self.landed(10, at, self.zbuf.at[at])

        def put(r, v):
            self.out[r, mine] = v.astype(BF)
        add_rows(put, [lambda r: self.fin[r]] + [
            lambda r, at=at: self.zbuf[at, r].astype(F32) for at in others], self.rows)
        self.push(13, 0, self.out.at[:, mine], self.out.at[:, mine], self.pn)

    def landing(self):
        self.landed(13, 0, self.out.at[:, self.other])

    def finish(self):
        for copy in self.pending:
            copy().wait_send()


def reduce_buffers(pair, rows, width):
    half = rows // 2
    return [
        pltpu.VMEM((4, 4, rows, width) if pair else (1, 1, 16, width), BF),
        pltpu.VMEM((4, 2, half, width), BF),
        pltpu.VMEM((4, 2, half, width), BF),
        pltpu.VMEM((4, half, width), BF),
        pltpu.VMEM((4, half, width), BF),
        pltpu.VMEM((4, rows, width), BF),
        pltpu.VMEM((3, rows, width), BF),
        pltpu.VMEM((rows, width), F32),
        pltpu.SemaphoreType.DMA((14, 4)),
        pltpu.SemaphoreType.DMA((14, 4)),
    ]


def experts_body(two_ref, share_ref, top_ref, gate_ref, up_ref, down_ref,
                 back_out, prob_out, moe_out, dgate_out, dup_out, ddown_out,
                 two_all, shares, top_all, pair_w, down_w, pull, pair_v,
                 acts, dpair, back, prob_v, stage, dstage,
                 buf0, bufx, bufy, bufx2, bufy2, zbuf, zsend, fin, rsend, rrecv,
                 gsend, grecv, psend, precv, load, store, dstore):
    s, z, m = place()
    c = s * 4 + z
    rows = two_ref.shape[0]
    width = two_ref.shape[1]
    hidden = down_w.shape[0]
    block = 4 * rows
    loads = [
        pltpu.make_async_copy(top_ref, top_all, load.at[0]),
        pltpu.make_async_copy(down_ref, down_w, load.at[1]),
        pltpu.make_async_copy(gate_ref, pair_w.at[:, pl.ds(0, hidden)], load.at[2]),
        pltpu.make_async_copy(up_ref, pair_w.at[:, pl.ds(hidden, hidden)], load.at[3]),
    ]
    for copy in loads:
        copy.start()
    call_chips()
    pl.semaphore_wait(pltpu.get_barrier_semaphore(), 16)
    work = Gather([Part("rows", two_ref, two_all), Part("small", share_ref, shares)], gsend, grecv)
    work.start()
    two_all[span((z * 4 + s) * rows, rows), :] = two_ref[...]
    shares[z * 4 + s, m] = share_ref[...]
    total = Reduce(True, True, back, back, back_out,
                   (buf0, bufx, bufy, bufx2, bufy2, zbuf, zsend, fin), (rsend, rrecv))
    planes = work.planes

    def tiles(count, size, fn):
        def run(i, _):
            fn(span(i * size, size))
            return 0
        lax.fori_loop(0, count // size, run, 0)

    def pulls(i):
        at = pl.ds(i * block, block)

        def tile(cols):
            pull[at, cols] = contract_last(top_all[at, :], down_w[cols, :])
        tiles(hidden, 256, tile)

    def enter(side, k):
        at = span(planes[k] * block, block)
        cols = pl.ds(side * hidden, hidden)
        pair_v[:, cols] = jnp.dot(two_all[at, :], pair_w[:, cols], preferred_element_type=F32)

    def middle(k):
        def one(row, _):
            slot = planes[k] * 4 + row
            wide = jnp.broadcast_to(shares[slot, m, pl.ds(c, 1), :], (rows, rows))
            column = jnp.transpose(wide)[:, 0:1]
            base = span(slot * rows, rows)
            here = span(row * rows, rows)
            gate = pair_v[here, pl.ds(0, hidden)]
            up = pair_v[here, pl.ds(hidden, hidden)]
            drawn = pull[base, :]
            sig = jax.nn.sigmoid(gate)
            act = gate * sig * up
            acts[base, :] = (act * column).astype(BF)
            grad = drawn * column
            dpair[base, pl.ds(0, hidden)] = (grad * up * sig * (1.0 + gate * (1.0 - sig))).astype(BF)
            dpair[base, pl.ds(hidden, hidden)] = (grad * gate * sig).astype(BF)
            prob = jnp.sum(act * drawn, axis=1, keepdims=True)
            prob_v[slot] = jnp.transpose(jnp.broadcast_to(prob, (rows, rows)))[0:8, :]
            return 0
        lax.fori_loop(0, 4, one, 0)

    def backs(k):
        at = span(planes[k] * block, block)

        def tile(cols):
            back[at, cols] = contract_last(dpair[at, :], pair_w[cols, :]).astype(BF)
        tiles(width, 512, tile)
        total.swap(planes[k])

    def saves(i, t):
        return pltpu.make_async_copy(
            stage.at[t], moe_out.at[pl.ds(i * block, block), span(t * 1024, 1024)], store.at[t])

    def moes(i):
        at = pl.ds(i * block, block)

        def one(t, _):
            if i >= 1:
                saves(i - 1, t).wait()
            cols = span(t * 1024, 1024)
            stage[t] = jnp.dot(acts[at, :], down_w[:, cols], preferred_element_type=F32).astype(BF)
            saves(i, t).start()
            return 0
        lax.fori_loop(0, 2, one, 0)

    def keep(i):
        rows_at = span(i * 512, 512)
        slot = lax.rem(i, 2)
        return [
            pltpu.make_async_copy(
                dstage.at[slot, :, pl.ds(side * hidden, hidden)],
                (dgate_out, dup_out)[side].at[rows_at, :],
                dstore.at[slot, side],
            )
            for side in (0, 1)
        ]

    def keep_down(i):
        return pltpu.make_async_copy(
            dstage.at[i], ddown_out.at[:, span(i * 1024, 1024)], dstore.at[i, 2])

    def grads(low, high):
        def one(i, _):
            def settle():
                for copy in keep(i - 2):
                    copy.wait()
            pl.when(i >= 2)(settle)
            cols = span(i * 512, 512)

            def side(n, _):
                here = span(n * hidden, hidden)
                dstage[lax.rem(i, 2), :, here] = contract_first(two_all[:, cols], dpair[:, here])
                return 0
            lax.fori_loop(0, 2, side, 0)
            for copy in keep(i):
                copy.start()
            return 0
        lax.fori_loop(low, high, one, 0)

    def downs():
        for i in (2, 3):
            for copy in keep(i):
                copy.wait()

        def one(i, _):
            dstage[i] = contract_first(acts[...], top_all[:, span(i * 1024, 1024)])
            keep_down(i).start()
            return 0
        lax.fori_loop(0, 2, one, 0)

    loads[0].wait()
    loads[1].wait()
    pulls(0)
    work.along(1)
    work.across(0)
    pulls(1)
    work.along(2)
    work.across(1)
    pulls(2)
    work.along(3)
    work.corner(0)
    pulls(3)
    work.across(2)
    loads[2].wait()
    loads[3].wait()
    work.ready(0)
    enter(0, 0)
    work.corner(1)
    enter(1, 0)
    work.across(3)
    middle(0)
    work.corner(2)
    backs(0)
    work.ready(1)
    enter(0, 1)
    work.corner(3)
    enter(1, 1)
    total.first(planes[0])
    middle(1)
    backs(1)
    total.second(planes[0])
    work.ready(2)
    enter(0, 2)
    total.first(planes[1])
    enter(1, 2)
    middle(2)
    backs(2)
    total.second(planes[1])
    work.ready(3)
    enter(0, 3)
    total.first(planes[2])
    enter(1, 3)
    middle(3)

    def dev(j):
        return (lax.div(j, 4), lax.rem(j, 4), m)

    def send_prob(step):
        j = lax.rem(c + step, 16)
        slot = lax.rem(j, 4) * 4 + lax.div(j, 4)
        return remote(prob_v.at[slot], prob_out.at[m, c], psend.at[step], precv.at[step], dev(j))
    for step in range(1, 16):
        send_prob(step).start()
    prob_out[m, c] = prob_v[z * 4 + s]
    backs(3)
    total.second(planes[2])
    moes(0)
    total.first(planes[3])
    total.keep()
    moes(1)
    total.third(planes[1], 0)
    moes(2)
    total.second(planes[3])
    total.third(planes[2], 1)
    moes(3)
    grads(0, 1)
    total.third(planes[3], 2)
    for step in range(1, 16):
        j = lax.rem(c + 16 - step, 16)
        target = prob_out.at[m, j]
        remote(target, target, psend.at[step], precv.at[step], dev(j)).wait_recv()
    pair = remote(prob_out.at[m], prob_out.at[m], psend.at[0], precv.at[0], (s, z, 1 - m))
    pair.start()
    grads(1, 4)
    downs()
    total.close()
    for i in (0, 1):
        keep_down(i).wait()
    for t in (0, 1):
        saves(3, t).wait()
    total.landing()
    other = prob_out.at[1 - m]
    remote(other, other, psend.at[0], precv.at[0], (s, z, 1 - m)).wait_recv()
    pair.wait_send()
    for step in range(1, 16):
        send_prob(step).wait_send()
    work.finish()
    total.finish()


def experts(ident, two, share, top, gate, up, down):
    rows, width = two.shape
    hidden = gate.shape[1]
    every = 16 * rows
    block = 4 * rows
    vmem = pl.BlockSpec(memory_space=pltpu.VMEM)
    hbm = pl.BlockSpec(memory_space=pl.ANY)
    return pl.pallas_call(
        experts_body,
        out_shape=(
            jax.ShapeDtypeStruct((rows, width), BF),
            jax.ShapeDtypeStruct((2, 16, 8, rows), F32),
            jax.ShapeDtypeStruct((every, width), BF),
            jax.ShapeDtypeStruct((width, hidden), F32),
            jax.ShapeDtypeStruct((width, hidden), F32),
            jax.ShapeDtypeStruct((hidden, width), F32),
        ),
        in_specs=[vmem, vmem, hbm, hbm, hbm, hbm],
        out_specs=(vmem, vmem, hbm, hbm, hbm, hbm),
        scratch_shapes=[
            pltpu.VMEM((every, width), BF),
            pltpu.VMEM((16, 2) + share.shape, F32),
            pltpu.VMEM((every, width), BF),
            pltpu.VMEM((width, 2 * hidden), BF),
            pltpu.VMEM((hidden, width), BF),
            pltpu.VMEM((every, hidden), F32),
            pltpu.VMEM((block, 2 * hidden), F32),
            pltpu.VMEM((every, hidden), BF),
            pltpu.VMEM((every, 2 * hidden), BF),
            pltpu.VMEM((every, width), BF),
            pltpu.VMEM((16, 8, rows), F32),
            pltpu.VMEM((2, block, 1024), BF),
            pltpu.VMEM((2, 512, 2 * hidden), F32),
        ]
        + reduce_buffers(True, rows, width // 2)
        + [
            pltpu.SemaphoreType.DMA((2, 12, 4)),
            pltpu.SemaphoreType.DMA((2, 12, 4)),
            pltpu.SemaphoreType.DMA((16,)),
            pltpu.SemaphoreType.DMA((16,)),
            pltpu.SemaphoreType.DMA((4,)),
            pltpu.SemaphoreType.DMA((2,)),
            pltpu.SemaphoreType.DMA((2, 3)),
        ],
        compiler_params=pltpu.CompilerParams(collective_id=ident, has_side_effects=True,
                                             vmem_limit_bytes=66900000),
        name="experts_%d" % ident,
    )(two, share, top, gate, up, down)


class Hand:
    def __init__(self, source, target, send, recv):
        s, z, m = place()
        self.c, self.m, self.pn = s * 4 + z, m, (s, z, 1 - m)
        self.source, self.target, self.send, self.recv = source, target, send, recv

    def dev(self, j):
        return (lax.div(j, 4), lax.rem(j, 4), self.m)

    def copy(self, step):
        j = lax.rem(self.c + step, 16)
        return remote(self.source(j), self.target(self.c), self.send.at[step], self.recv.at[step], self.dev(j))

    def start(self):
        for step in range(1, 16):
            self.copy(step).start()

    def collect(self):
        for step in range(1, 16):
            j = lax.rem(self.c + 16 - step, 16)
            remote(self.target(j), self.target(j), self.send.at[step], self.recv.at[step], self.pn).wait_recv()

    def finish(self):
        for step in range(1, 16):
            self.copy(step).wait_send()


class Chips:
    def __init__(self, source, target, send, recv, fsend, frecv, local):
        s, z, m = place()
        self.c, self.m, self.pn = s * 4 + z, m, (s, z, 1 - m)
        self.first = lax.div(self.c, 8) == m
        self.source, self.target = source, target
        self.send, self.recv, self.fsend, self.frecv, self.local = send, recv, fsend, frecv, local

    def copy(self, i):
        j = 8 * self.m + i
        return remote(self.source(i), self.target.at[self.c], self.send.at[i], self.recv.at[self.c],
                      (lax.div(j, 4), lax.rem(j, 4), self.m))

    def mine(self):
        return pltpu.make_async_copy(
            self.source(lax.rem(self.c, 8)), self.target.at[self.c], self.local.at[0])

    def each(self, fn):
        for step in range(8):
            i = lax.rem(self.c + 1 + step, 8)
            pl.when(8 * self.m + i != self.c)(lambda i=i: fn(self.copy(i)))

    def start(self):
        self.each(lambda copy: copy.start())
        pl.when(self.first)(lambda: self.mine().start())

    def forward(self, j):
        return remote(self.target.at[j], self.target.at[j], self.fsend.at[j], self.frecv.at[j], self.pn)

    def collect(self):
        def take():
            self.mine().wait()
            self.forward(self.c).start()
            for step in range(1, 16):
                j = lax.rem(self.c + 16 - step, 16)
                remote(self.target.at[j], self.target.at[j], self.send.at[0], self.recv.at[j],
                       self.pn).wait_recv()
                self.forward(j).start()
        pl.when(self.first)(take)

    def follow(self):
        def wait():
            for j in range(16):
                self.forward(j).wait_recv()
        pl.when(jnp.logical_not(self.first))(wait)

    def finish(self):
        def wait():
            for j in range(16):
                self.forward(j).wait_send()
        pl.when(self.first)(wait)
        self.each(lambda copy: copy.wait_send())


def chips_semaphores():
    return [pltpu.SemaphoreType.DMA((8,))] + [pltpu.SemaphoreType.DMA((16,))] * 3 + [
        pltpu.SemaphoreType.DMA((1,))]


def front_body(tok_ref, one_ref, second_ref, place_ref, router_ref, qg_ref, kg_ref, routes_ref,
               qw_ref, kw_ref, vw_ref, wo_ref, cot_ref, freq_ref,
               n1_out, wo_out, cot_out, w3, info, raw, rows3, squares, mixed, lse, trig, own_mixed,
               hidden, two, probs_out, chosen_out, share_out, heads_out, gain_out,
               info_ref, packed_ref, n1_own, n1_all, wo_all, wide_mixed, gathered, sums, line,
               nsend, nrecv, osend, orecv, csend, crecv,
               isend, irecv, qsend, qrecv, pairs, *chips_sems):
    s, z, m = place()
    c = s * 4 + z
    pn = (s, z, 1 - m)
    rows, width = tok_ref.shape
    dim = 128
    planes = near_planes(z)
    lane = lax.broadcasted_iota(jnp.int32, (rows, dim), 1)
    call_chips()
    info_ref[...] = jnp.zeros_like(info_ref)
    info_ref[0:1, :] = one_ref[...].astype(F32)
    info_ref[1:2, :] = second_ref[...].astype(F32)
    info_ref[2:3, :] = place_ref[...].astype(F32)
    info_ref[4:20, :] = router_ref[...].astype(F32)
    info_ref[24:32, 0:8] = qg_ref[...].astype(F32)
    info_ref[32:40, 0:8] = kg_ref[...].astype(F32)
    for i in range(8):
        for n, ref in enumerate((qw_ref, kw_ref, vw_ref)):
            packed_ref[i, :, pl.ds(n * dim, dim)] = ref[:, pl.ds(i * dim, dim)]
    pl.semaphore_wait(pltpu.get_barrier_semaphore(), 16)
    hand = Hand(lambda j: info_ref, lambda j: info.at[m, j], isend, irecv)
    hand.start()
    weights = Chips(lambda i: packed_ref.at[i], w3, *chips_sems[:5])
    weights.start()
    outer = Gather([Part("heads", wo_ref, wo_all)], osend, orecv)
    outer.start()
    info[m, c] = info_ref[...]

    def square_sum(r, _):
        at = span(r * 16, 16)
        x = tok_ref[at, :].astype(F32)
        mean = jnp.sum(x * x, axis=1, keepdims=True) / width
        line[at, :] = jnp.broadcast_to(lax.rsqrt(mean + eps), (16, dim))
        return 0
    lax.fori_loop(0, rows // 16, square_sum, 0)
    hand.collect()
    swap = remote(info.at[m], info.at[m], pairs.at[0], pairs.at[1], pn)
    swap.start()

    def normalize(j, _):
        at = span(j * dim, dim)
        n1_own[:, at] = (tok_ref[:, at].astype(F32) * line[...] * info[m, j, 0:1, :]).astype(BF)
        return 0
    lax.fori_loop(0, 16, normalize, 0)
    first = Gather([Part("rows", n1_own, n1_all)], nsend, nrecv)
    first.start()
    n1_all[span((z * 4 + s) * rows, rows), :] = n1_own[...]

    def tables(b, _):
        spot = jnp.broadcast_to(info[m, 8 * m + b, 2:3, :], (rows, dim))
        angle = jnp.transpose(spot) * freq_ref[0:1, :]
        trig[0, b] = jnp.cos(angle)
        trig[1, b] = jnp.where(lane < dim // 2, -jnp.sin(angle), jnp.sin(angle))
        return 0
    lax.fori_loop(0, 8, tables, 0)
    other = info.at[1 - m]
    remote(other, other, pairs.at[0], pairs.at[1], pn).wait_recv()

    first.along(1)
    first.across(0)
    weights.collect()
    first.along(2)
    first.across(1)
    first.along(3)
    first.corner(0)
    weights.follow()
    first.across(2)
    first.ready(0)

    def project(k):
        def one(e, _):
            value = jnp.dot(n1_all[span((planes[k] * 4 + 2 * m + e) * rows, rows), :],
                            w3[...].reshape(width, 3 * dim), preferred_element_type=F32)
            base = span((e * 4 + planes[k]) * rows, rows)
            raw[base, :] = value[:, : 2 * dim]
            rows3[base, pl.ds(2 * dim, dim)] = value[:, 2 * dim :].astype(BF)
            return 0
        lax.fori_loop(0, 2, one, 0)
    project(0)
    first.corner(1)
    first.across(3)
    outer.along(1)
    outer.across(0)
    first.ready(1)
    project(1)
    first.corner(2)
    first.ready(2)
    project(2)
    first.corner(3)
    first.ready(3)
    project(3)

    def norms(b, total):
        at = span(b * rows, rows)
        q = raw[at, pl.ds(0, dim)]
        k = raw[at, pl.ds(dim, dim)]
        total = jnp.where(lane == b, jnp.sum(q * q, axis=1, keepdims=True), total)
        return jnp.where(lane == b + 8, jnp.sum(k * k, axis=1, keepdims=True), total)
    total = lax.fori_loop(0, 8, norms, jnp.zeros((rows, dim), F32))
    sums[...] = jnp.transpose(total)[0:16, :]
    share = Hand(lambda j: sums, lambda j: gathered.at[j], qsend, qrecv)
    share.start()
    gathered[c] = sums[...]
    save_n1 = pltpu.make_async_copy(n1_all, n1_out, pairs.at[2])
    save_n1.start()
    wo_own = pltpu.make_async_copy(wo_ref, outer.parts[0].piece(s, z, m), pairs.at[3])
    wo_own.start()
    outer.along(2)
    share.collect()

    def add_up(j, acc):
        return acc + gathered[j]
    summed = lax.fori_loop(1, 16, add_up, gathered[0])
    squares[...] = summed
    wide = jnp.concatenate([lax.rsqrt(summed / width + eps), jnp.zeros((rows - 16, dim), F32)], axis=0)
    line[...] = jnp.transpose(wide)

    def head_gain(which):
        total = jnp.zeros((8, dim), F32)
        lane8 = lax.broadcasted_iota(jnp.int32, (8, dim), 1)
        for j in range(16):
            row = info[lax.div(c, 8), j, pl.ds(24 + 8 * which + lax.rem(c, 8), 1), :]
            moved = pltpu.roll(jnp.broadcast_to(row, (8, dim)), 8 * j, 1)
            total = jnp.where(lax.div(lane8, 8) == j, moved, total)
        return total[0:1, :]
    gains = (head_gain(0), head_gain(1))
    heads_out[...] = jnp.concatenate([gains[0], gains[1], jnp.zeros((6, dim), F32)], axis=0)

    def turn(b, _):
        at = span(b * rows, rows)
        for which, factor in ((0, dim ** (-0.5)), (1, 1.0)):
            pick = jnp.where(lane == b + 8 * which, line[...], 0.0)
            inverse = jnp.sum(pick, axis=1, keepdims=True)
            value = raw[at, pl.ds(which * dim, dim)] * inverse * gains[which]
            value = value * trig[0, b] + pltpu.roll(value, dim // 2, 1) * trig[1, b]
            rows3[at, pl.ds(which * dim, dim)] = (value * factor).astype(BF)
        return 0
    lax.fori_loop(0, 8, turn, 0)
    outer.across(1)
    outer.along(3)

    def attend(b, _):
        seq = span(lax.div(b, 4) * 4 * rows, 4 * rows)
        at = span(b * rows, rows)
        scores = contract_last(rows3[at, pl.ds(0, dim)], rows3[seq, pl.ds(dim, dim)])
        here = lax.broadcasted_iota(jnp.int32, scores.shape, 0) + lax.rem(b, 4) * rows
        allowed = lax.broadcasted_iota(jnp.int32, scores.shape, 1) <= here
        scores = jnp.where(allowed, scores, neg_big)
        top = jnp.max(scores, axis=1, keepdims=True)
        weight = jnp.where(allowed, jnp.exp(scores - top), 0.0)
        count = jnp.sum(weight, axis=1, keepdims=True)
        value = jnp.dot(weight.astype(BF), rows3[seq, pl.ds(2 * dim, dim)], preferred_element_type=F32)
        mixed[b] = (value / count).astype(BF)
        lse[b] = jnp.transpose(jnp.broadcast_to(top + jnp.log(count), (rows, dim)))[0:8, :]
        return 0
    lax.fori_loop(0, 8, attend, 0)
    back = Chips(lambda i: mixed.at[i], own_mixed, *chips_sems[5:])
    back.start()
    outer.corner(0)
    outer.across(2)
    back.collect()
    outer.corner(1)
    outer.across(3)
    cots = Gather([Part("rows", cot_ref, cot_out)], csend, crecv)
    cots.start()
    cot_own = pltpu.make_async_copy(cot_ref, cot_out.at[span((z * 4 + s) * rows, rows)], pairs.at[4])
    cot_own.start()
    outer.corner(2)
    back.follow()
    outer.corner(3)
    wo_own.wait()
    for step in range(4):
        outer.ready(step)
    save_wo = pltpu.make_async_copy(wo_all, wo_out, pairs.at[5])
    save_wo.start()
    cots.along(1)
    cots.across(0)
    for j in range(16):
        wide_mixed[:, pl.ds(j * dim, dim)] = own_mixed[j]

    def outward(j, _):
        at = span(j * 512, 512)
        hidden[:, at] = tok_ref[:, at].astype(F32) + jnp.dot(
            wide_mixed[...], wo_all[:, at], preferred_element_type=F32)
        return 0
    lax.fori_loop(0, 4, outward, 0)
    cots.along(2)
    cots.across(1)

    def square_two(r, _):
        at = span(r * 8, 8)
        x = hidden[at, :]
        mean = jnp.sum(x * x, axis=1, keepdims=True) / width
        line[at, :] = jnp.broadcast_to(lax.rsqrt(mean + eps), (8, dim))
        return 0
    lax.fori_loop(0, rows // 8, square_two, 0)

    def normalize_two(j, _):
        at = span(j * dim, dim)
        two[:, at] = (hidden[:, at] * line[...] * info[m, j, 1:2, :]).astype(BF)
        return 0
    lax.fori_loop(0, 16, normalize_two, 0)
    logits = jnp.zeros((16, rows), F32)
    for j in range(16):
        logits = logits + contract_last(info[m, j, 4:20, :].astype(BF), two[:, pl.ds(j * dim, dim)])
        gain_out[0:1, pl.ds(j * dim, dim)] = info[m, j, 0:1, :]
        gain_out[1:2, pl.ds(j * dim, dim)] = info[m, j, 1:2, :]
    gain_out[2:8, :] = jnp.zeros((6, width), F32)
    logits = jnp.exp(logits - jnp.max(logits, axis=0, keepdims=True))
    probs = logits / jnp.sum(logits, axis=0, keepdims=True)
    picks = jnp.transpose(jnp.concatenate(
        [routes_ref[...].astype(F32), jnp.full((rows, dim - 8), -1.0, F32)], axis=1))
    row16 = lax.broadcasted_iota(jnp.int32, (16, rows), 0).astype(F32)
    chosen = jnp.zeros((16, rows), F32)
    for k in range(8):
        chosen = jnp.where(row16 == picks[k : k + 1, :], 1.0, chosen)
    probs_out[...] = probs
    chosen_out[...] = chosen
    share_out[...] = probs * chosen
    cots.along(3)
    cots.corner(0)
    cots.across(2)
    cots.corner(1)
    cots.across(3)
    cots.corner(2)
    cots.corner(3)
    for step in range(4):
        cots.ready(step)
    for copy in (save_n1, save_wo, cot_own):
        copy.wait()
    swap.wait_send()
    for work in (hand, weights, share, back, first, outer, cots):
        work.finish()


def front(ident, *arrays):
    rows, width = arrays[0].shape
    every = 16 * rows
    mine = every // 2
    vmem = pl.BlockSpec(memory_space=pltpu.VMEM)
    hbm = pl.BlockSpec(memory_space=pl.ANY)

    def shape(*sizes, dtype=F32):
        return jax.ShapeDtypeStruct(sizes, dtype)
    return pl.pallas_call(
        front_body,
        out_shape=(
            shape(every, width, dtype=BF),
            shape(every, width, dtype=BF),
            shape(every, width, dtype=BF),
            shape(16, rows, 384, dtype=BF),
            shape(2, 16, 40, 128),
            shape(mine, 256),
            shape(mine, 384, dtype=BF),
            shape(16, 128),
            shape(8, rows, 128, dtype=BF),
            shape(8, 8, rows),
            shape(2, 8, rows, 128),
            shape(16, rows, 128, dtype=BF),
            shape(rows, width),
            shape(rows, width, dtype=BF),
            shape(16, rows),
            shape(16, rows),
            shape(16, rows),
            shape(8, 128),
            shape(8, width),
        ),
        in_specs=[vmem] * 14,
        out_specs=(hbm, hbm, hbm) + (vmem,) * 16,
        scratch_shapes=[
            pltpu.VMEM((40, 128), F32),
            pltpu.VMEM((8, rows, 384), BF),
            pltpu.VMEM((rows, width), BF),
            pltpu.VMEM((every, width), BF),
            pltpu.VMEM((every, width), BF),
            pltpu.VMEM((rows, width), BF),
            pltpu.VMEM((16, 16, 128), F32),
            pltpu.VMEM((16, 128), F32),
            pltpu.VMEM((rows, 128), F32),
        ]
        + [pltpu.SemaphoreType.DMA((1, 12, 4))] * 6
        + [pltpu.SemaphoreType.DMA((16,))] * 4
        + [pltpu.SemaphoreType.DMA((6,))]
        + chips_semaphores() * 2,
        compiler_params=pltpu.CompilerParams(collective_id=ident, has_side_effects=True,
                                             vmem_limit_bytes=56 << 20),
        name="front_%d" % ident,
    )(*arrays)


class Cores:
    def __init__(self, source, target, send, recv, local):
        s, z, m = place()
        self.c, self.m = s * 4 + z, m
        self.high, self.low = lax.div(self.c, 8), lax.rem(self.c, 8)
        self.same = self.high == m
        self.source, self.target, self.send, self.recv, self.local = source, target, send, recv, local

    def dev(self, i):
        j = 8 * self.m + i
        return (lax.div(j, 4), lax.rem(j, 4), self.high)

    def away(self, i):
        return jnp.logical_not(jnp.logical_and(self.same, self.low == i))

    def copy(self, i):
        return remote(self.source.at[i], self.target.at[self.low], self.send.at[i],
                      self.recv.at[self.low], self.dev(i))

    def mine(self):
        return pltpu.make_async_copy(self.source.at[self.low], self.target.at[self.low], self.local.at[0])

    def start(self, low=0, high=8):
        for i in range(low, high):
            pl.when(self.away(i))(lambda i=i: self.copy(i).start())

            def keep():
                self.mine().start()
            pl.when(jnp.logical_not(self.away(i)))(keep)

    def collect(self):
        for i in range(8):
            pl.when(self.away(i))(lambda i=i: remote(
                self.target.at[i], self.target.at[i], self.send.at[0], self.recv.at[i],
                self.dev(i)).wait_recv())
        pl.when(self.same)(lambda: self.mine().wait())

    def finish(self):
        for i in range(8):
            pl.when(self.away(i))(lambda i=i: self.copy(i).wait_send())


def cores_semaphores():
    return [pltpu.SemaphoreType.DMA((8,))] * 2 + [pltpu.SemaphoreType.DMA((1,))]


def call_all():
    s, z, m = place()
    high = lax.div(s * 4 + z, 8)
    call_chips()

    def cross():
        for i in range(8):
            j = 8 * m + i
            signal((lax.div(j, 4), lax.rem(j, 4), high))
    pl.when(high != m)(cross)


def await_all():
    s, z, m = place()
    high = lax.div(s * 4 + z, 8)
    pl.when(high != m)(lambda: pl.semaphore_wait(pltpu.get_barrier_semaphore(), 24))
    pl.when(high == m)(lambda: pl.semaphore_wait(pltpu.get_barrier_semaphore(), 16))


def rear_body(back_ref, prob_ref, probs_ref, chosen_ref, two_ref, out_ref, cot_ref, info,
              mixed_ref, rows3, raw, squares, lse, trig, gains, w3, tok_ref, gain_ref,
              wo_ref, n1_ref, moe_ref,
              gn_out, moe_out, q_out, k_out, v_out, out_grad, tok_out, tail_out,
              got, ga_ref, hidden_ref, wo_half, n1_half, moe, gn_part, mixed_line, ga_blocks, ga_plane, gm_send, gm, wsend, backs,
              dq, dk, dv, sums, gathered, line, dots, tail, out_mine, out_all,
              a0, a1, a2, a3, a4, a5, a6, a7, asend, arecv,
              b0, b1, b2, b3, b4, b5, b6, b7, bsend, brecv,
              msend, mrecv, csend, crecv, hsend, hrecv, tsend, trecv, psend, precv, osend, orecv, load, *rest):
    s, z, m = place()
    c = s * 4 + z
    pn = (s, z, 1 - m)
    rows, width = tok_ref.shape
    cut = width // 2
    dim = 128
    factor = dim ** (-0.5)
    loads = [
        pltpu.make_async_copy(wo_ref.at[span(m * cut, cut), :], wo_half, load.at[0]),
        pltpu.make_async_copy(moe_ref, moe, load.at[1]),
        pltpu.make_async_copy(n1_ref.at[:, span(m * cut, cut)], n1_half, load.at[2]),
        pltpu.make_async_copy(mixed_ref, mixed_line.at[span(m * cut, cut), span(z * dim, dim)], load.at[3]),
    ]
    for copy in loads:
        copy.start()
    call_all()
    order = far_planes(z)
    outer = Reduce(True, True, moe, moe, moe_out, (a0, a1, a2, a3, a4, a5, a6, a7), (asend, arecv))
    inner = Reduce(False, True, gn_part, gn_part, gn_out, (b0, b1, b2, b3, b4, b5, b6, b7), (bsend, brecv))
    prob = jnp.concatenate(
        [prob_ref[0, j, 0:1, :] + prob_ref[1, j, 0:1, :] for j in range(16)], axis=0)
    prob = prob * chosen_ref[...]
    probs = probs_ref[...]
    logits = (probs * (prob - jnp.sum(probs * prob, axis=0, keepdims=True))).astype(BF)
    tail[...] = jnp.zeros_like(tail)
    for j in range(16):
        at = pl.ds(j * dim, dim)
        tail[j, 3:19, :] = jnp.dot(logits, two_ref[:, at], preferred_element_type=F32)
        hidden_ref[:, at] = back_ref[:, at].astype(F32) + contract_first(
            logits, info[m, j, 4:20, :].astype(BF))

    def second_norm(r, acc):
        at = span(r * 16, 16)
        x = out_ref[at, :]
        grad = hidden_ref[at, :]
        inverse = lax.rsqrt(jnp.sum(x * x, axis=1, keepdims=True) / width + eps)
        scaled = grad * gain_ref[1:2, :]
        dot = jnp.sum(x * scaled, axis=1, keepdims=True) / width
        value = cot_ref[at, :].astype(F32) + (
            inverse * scaled - x * (inverse * inverse * inverse * dot))
        hidden_ref[at, :] = value
        ga_ref[at, :] = value.astype(BF)
        part = grad * x * inverse
        return acc + part[0:8] + part[8:16]
    acc = lax.fori_loop(0, rows // 16, second_norm, jnp.zeros((8, width), F32))
    acc = jnp.sum(acc, axis=0, keepdims=True)
    for j in range(16):
        tail[j, 1:2, :] = acc[:, j * dim : (j + 1) * dim]
    await_all()
    loads[1].wait()
    for at in order:
        outer.swap(at)
    lane = lax.broadcasted_iota(jnp.int32, (rows, dim), 1)
    give = Cores(gm_send, gm, *rest[:3])
    loads[0].wait()
    def mix(t, _):
        value = contract_last(ga_ref[...], wo_half[span(t * 512, 512), :]).astype(BF)
        for i in range(4):
            gm_send[t * 4 + i] = value[:, i * dim : (i + 1) * dim]
        return 0
    lax.fori_loop(0, 2, mix, 0)
    give.start()
    strip = Line([Part("line", mixed_ref, mixed_line)], msend, mrecv)
    spread = Spread([Part("cols", ga_blocks, ga_plane)], csend, crecv)

    wide = jnp.concatenate(
        [lax.rsqrt(squares[...] / width + eps), jnp.zeros((rows - 16, dim), F32)], axis=0)
    line[...] = jnp.transpose(wide)
    dk[...] = jnp.zeros_like(dk)
    dv[...] = jnp.zeros_like(dv)
    outer.first(order[0])
    outer.first(order[1])
    give.collect()
    outer.first(order[2])
    outer.first(order[3])

    def attend(b, _):
        seq = span(lax.div(b, 4) * 4 * rows, 4 * rows)
        at = span(b * rows, rows)
        query = rows3[at, pl.ds(0, dim)]
        key = rows3[seq, pl.ds(dim, dim)]
        value = rows3[seq, pl.ds(2 * dim, dim)]
        grad = gm[b]
        top = jnp.transpose(jnp.broadcast_to(lse[b, 0:1, :], (rows, dim)))[:, 0:1]
        delta = jnp.sum(grad.astype(F32) * mixed_ref[at, :].astype(F32), axis=1, keepdims=True)
        scores = contract_last(query, key)
        here = lax.broadcasted_iota(jnp.int32, scores.shape, 0) + lax.rem(b, 4) * rows
        allowed = lax.broadcasted_iota(jnp.int32, scores.shape, 1) <= here
        prob = jnp.where(allowed, jnp.exp(jnp.where(allowed, scores, neg_big) - top), 0.0)
        back = (prob * (contract_last(grad, value) - delta)).astype(BF)
        dv[seq, :] += contract_first(prob.astype(BF), grad)
        dk[seq, :] += contract_first(back, query)
        dq[at, :] = jnp.dot(back, key, preferred_element_type=F32) * factor
        return 0
    lax.fori_loop(0, 4, attend, 0)
    outer.second(order[0])
    outer.second(order[1])
    lax.fori_loop(4, 8, attend, 0)

    def column(source, r):
        return jnp.sum(jnp.where(lane == r, source, 0.0), axis=1, keepdims=True)

    def unturn(b, carry):
        total, gain_q, gain_k = carry
        at = span(b * rows, rows)
        out = []
        for which, grads in ((0, dq), (1, dk)):
            value = grads[at, :]
            value = value * trig[0, b] + pltpu.roll(value * trig[1, b], dim // 2, 1)
            plain = raw[at, pl.ds(which * dim, dim)]
            unit = plain * column(line[...], b + 8 * which)
            out.append(jnp.sum(value * unit, axis=0, keepdims=True))
            value = value * gains[which : which + 1, :]
            grads[at, :] = value
            dot = jnp.sum(plain * value, axis=1, keepdims=True)
            total = jnp.where(lane == b + 8 * which, dot, total)
        return total, gain_q + out[0], gain_k + out[1]
    zero = jnp.zeros((1, dim), F32)
    total, gain_q, gain_k = lax.fori_loop(0, 8, unturn, (jnp.zeros((rows, dim), F32), zero, zero))
    for j in range(16):
        tail[j, 2:3, :] = gain_q
        tail[j, 19:20, :] = gain_k
    sums[...] = jnp.transpose(total)[0:16, :]
    hand = Hand(lambda j: sums, lambda j: gathered.at[j], hsend, hrecv)
    hand.start()
    gathered[c] = sums[...]
    strip.start()
    for p in range(4):
        for q in range(4):
            ga_blocks[p, :, pl.ds(q * dim, dim)] = ga_ref[:, pl.ds((q * 4 + p) * dim, dim)]
    spread.start()
    ga_plane[span(c * rows, rows), :] = ga_blocks[z]
    outer.second(order[2])
    outer.third(order[0], 0)
    outer.second(order[3])
    outer.third(order[1], 1)
    hand.collect()
    summed = lax.fori_loop(1, 16, lambda j, acc: acc + gathered[j], gathered[0])
    dots[...] = jnp.transpose(jnp.concatenate([summed, jnp.zeros((rows - 16, dim), F32)], axis=0))

    def finish_rows(b, _):
        at = span(b * rows, rows)
        base = span((lax.rem(b, 4) * 4 + 2 * m + lax.div(b, 4)) * rows, rows)
        for which, grads in ((0, dq), (1, dk)):
            inverse = column(line[...], b + 8 * which)
            dot = column(dots[...], b + 8 * which)
            value = inverse * grads[at, :] - raw[at, pl.ds(which * dim, dim)] * (
                inverse * inverse * inverse * dot / width)
            backs[base, pl.ds(which * dim, dim)] = value.astype(BF)
        backs[base, pl.ds(2 * dim, dim)] = dv[at, :].astype(BF)
        return 0
    lax.fori_loop(0, 8, finish_rows, 0)

    def pair(at, core):
        part = backs.at[span((at * 4 + 2 * core) * rows, 2 * rows), :]
        return remote(part, part, psend.at[at], precv.at[at], pn)
    for at in range(4):
        pair(at, m).start()
    outer.third(order[2], 2)
    for at in range(4):
        pair(at, 1 - m).wait_recv()
    for at in order:
        def chunk(t, _, at=at):
            here = span((at * 2 + t) * 2 * rows, 2 * rows)
            gn_part[here, :] = contract_last(
                backs[here, :], w3[span(m * 8, 8)].reshape(cut, 3 * dim)).astype(BF)
            return 0
        lax.fori_loop(0, 2, chunk, 0)
        inner.first(at)
    outer.keep()
    strip.along(1)
    spread.along(1)
    loads[2].wait()

    def weight_tile(n):
        def one(t, _):
            wsend[t] = contract_first(n1_half[:, span(t * dim, dim)], backs[...]).astype(BF)
            return 0
        lax.fori_loop(2 * n, 2 * n + 2, one, 0)
    weight_tile(0)
    weight_tile(1)
    inner.second(order[0])
    weight_tile(2)
    inner.third(order[0], 0)
    inner.second(order[1])
    weight_tile(3)
    outer.close()
    weights = Cores(wsend, got, *rest[3:6])
    weights.start()
    strip.along(2)
    spread.along(2)
    spread.across(0)
    inner.third(order[1], 1)
    inner.second(order[2])
    inner.third(order[2], 2)
    inner.second(order[3])
    inner.keep()
    strip.along(3)
    spread.along(3)
    spread.across(1)
    spread.corner(0)
    inner.close()
    inner.landing()

    def last(r, acc):
        at = span(r * 16, 16)
        x = tok_ref[at, :].astype(F32)
        grad = gn_out[at, :].astype(F32)
        inverse = lax.rsqrt(jnp.sum(x * x, axis=1, keepdims=True) / width + eps)
        scaled = grad * gain_ref[0:1, :]
        dot = jnp.sum(x * scaled, axis=1, keepdims=True) / width
        tok_out[at, :] = hidden_ref[at, :] + inverse * scaled - x * (inverse * inverse * inverse * dot)
        part = grad * x * inverse
        return acc + part[0:8] + part[8:16]
    acc = lax.fori_loop(0, rows // 16, last, jnp.zeros((8, width), F32))
    acc = jnp.sum(acc, axis=0, keepdims=True)
    for j in range(16):
        tail[j, 0:1, :] = acc[:, j * dim : (j + 1) * dim]
    finale = Hand(lambda j: tail.at[j], lambda j: tail_out.at[m, j], tsend, trecv)
    finale.start()
    tail_out[m, c] = tail[c]
    spread.across(2)
    spread.corner(1)
    spread.across(3)
    spread.corner(2)
    spread.corner(3)
    loads[3].wait()
    for step in (1, 2, 3):
        strip.ready(step)
    strip_own = mixed_line.at[span((1 - m) * cut, cut), span(z * dim, dim)]
    strip.landed(0, strip.PO, z, strip_own)
    for step in range(4):
        spread.ready(step)

    value = contract_first(mixed_line[:, span(m * 256, 256)], ga_plane[...]).astype(BF)
    for q in range(4):
        out_mine[q] = value[:, q * dim : (q + 1) * dim]
    high = lax.div(c, 8)
    lower = lax.rem(s, 2)
    cross = remote(out_mine, out_all.at[m], osend.at[0], orecv.at[0], pn)

    def landing(q, core):
        return out_grad.at[q, core]

    def away(step, core):
        q = (None, flip_x(s), flip_y(s), 3 - s)[step]
        source = out_mine if core is None else out_all.at[1 - m]
        who = m if core is None else 1 - m
        at = step * 2 + (0 if core is None else 1)
        return remote(source.at[q], landing(lower, who), osend.at[at], orecv.at[at], (q, z, m))

    def lead():
        for step in (1, 2, 3):
            away(step, None).start()
        out_grad[lower, m] = out_mine[s]
        remote(out_all.at[1 - m], out_all.at[1 - m], osend.at[0], orecv.at[0], pn).wait_recv()
        for step in (1, 2, 3):
            away(step, 1).start()
        out_grad[lower, 1 - m] = out_all[1 - m, s]
    pl.when(high == m)(lead)
    pl.when(high != m)(lambda: cross.start())
    finale.collect()
    pair_tail = remote(tail_out.at[m], tail_out.at[m], osend.at[8], orecv.at[8], pn)
    pair_tail.start()
    weights.collect()
    for j in range(8):
        for n, ref in enumerate((q_out, k_out, v_out)):
            ref[:, pl.ds(j * dim, dim)] = got[j, :, pl.ds(n * dim, dim)].astype(F32)

    def arrive(step):
        q = (None, flip_x(s), flip_y(s), 3 - s)[step]

        def take():
            for second in (0, 1):
                who = 1 - m if second else m
                at = step * 2 + second
                target = landing(lax.rem(q, 2), who)
                remote(target, target, osend.at[at], orecv.at[at], pn).wait_recv()
        pl.when(lax.div(q, 2) == m)(take)
    for step in (1, 2, 3):
        arrive(step)
    other = tail_out.at[1 - m]
    remote(other, other, osend.at[8], orecv.at[8], pn).wait_recv()
    pair_tail.wait_send()
    pl.when(high != m)(lambda: cross.wait_send())

    def sent():
        for step in (1, 2, 3):
            away(step, None).wait_send()
            away(step, 1).wait_send()
    pl.when(high == m)(sent)
    outer.landing()
    for at in range(4):
        pair(at, m).wait_send()
    for work in (give, outer, inner, hand, finale, weights, strip, spread):
        work.finish()


def rear(ident, *arrays):
    rows, width = arrays[0].shape
    every = 16 * rows
    cut = width // 2
    vmem = pl.BlockSpec(memory_space=pltpu.VMEM)
    hbm = pl.BlockSpec(memory_space=pl.ANY)
    return pl.pallas_call(
        rear_body,
        out_shape=(
            jax.ShapeDtypeStruct((rows, width), BF),
            jax.ShapeDtypeStruct((rows, width), BF),
            jax.ShapeDtypeStruct((rows, cut), F32),
            jax.ShapeDtypeStruct((rows, cut), F32),
            jax.ShapeDtypeStruct((rows, cut), F32),
            jax.ShapeDtypeStruct((2, 2, 256, 128), BF),
            jax.ShapeDtypeStruct((rows, width), F32),
            jax.ShapeDtypeStruct((2, 16, 24, 128), F32),
        ),
        in_specs=[vmem] * 18 + [hbm] * 3,
        out_specs=(vmem,) * 8,
        scratch_shapes=[
            pltpu.VMEM((8, rows, 384), BF),
            pltpu.VMEM((rows, width), BF),
            pltpu.VMEM((rows, width), F32),
            pltpu.VMEM((cut, width), BF),
            pltpu.VMEM((every, cut), BF),
            pltpu.VMEM((every, width), BF),
            pltpu.VMEM((every, cut), BF),
            pltpu.VMEM((every, 512), BF),
            pltpu.VMEM((4, rows, 512), BF),
            pltpu.VMEM((every, 512), BF),
            pltpu.VMEM((8, rows, 128), BF),
            pltpu.VMEM((8, rows, 128), BF),
            pltpu.VMEM((8, rows, 384), BF),
            pltpu.VMEM((every, 384), BF),
            pltpu.VMEM((every // 2, 128), F32),
            pltpu.VMEM((every // 2, 128), F32),
            pltpu.VMEM((every // 2, 128), F32),
            pltpu.VMEM((16, 128), F32),
            pltpu.VMEM((16, 16, 128), F32),
            pltpu.VMEM((rows, 128), F32),
            pltpu.VMEM((rows, 128), F32),
            pltpu.VMEM((16, 24, 128), F32),
            pltpu.VMEM((4, 256, 128), BF),
            pltpu.VMEM((2, 4, 256, 128), BF),
        ]
        + reduce_buffers(True, rows, cut)
        + reduce_buffers(False, rows, cut)
        + [pltpu.SemaphoreType.DMA((1, 12, 4))] * 4
        + [pltpu.SemaphoreType.DMA((16,))] * 4
        + [pltpu.SemaphoreType.DMA((4,))] * 2
        + [pltpu.SemaphoreType.DMA((9,))] * 2
        + [pltpu.SemaphoreType.DMA((4,))]
        + cores_semaphores()
        + cores_semaphores(),
        compiler_params=pltpu.CompilerParams(collective_id=ident, has_side_effects=True,
                                             vmem_limit_bytes=66900000),
        name="rear_%d" % ident,
    )(*arrays)


HEADS = 16
HEAD_DIM = 128


eps = 1e-05
neg_big = -1e30


def rms_scale(rows, gain):
    return rows * lax.rsqrt(jnp.mean(rows * rows, axis=-1, keepdims=True) + eps) * gain


def rope_tables(positions):
    half = HEAD_DIM // 2
    freq = 10000.0 ** (-(jnp.arange(half).astype(jnp.float32) * 2.0 / HEAD_DIM))
    angle = positions.astype(jnp.float32)[:, None] * freq[None, :]
    return (jnp.cos(angle), jnp.sin(angle))


def rope_turn(normed, cosine, sine, factor):
    count = normed.shape[0]
    heads = normed.shape[1]
    width = normed.shape[2]
    first = normed[..., : width // 2]
    second = normed[..., width // 2 :]
    cos_rows = cosine[:, None, :]
    sin_rows = sine[:, None, :]
    turned = jnp.concatenate(
        [first * cos_rows - second * sin_rows, second * cos_rows + first * sin_rows], axis=-1
    )
    return (turned * factor).reshape(count, heads * width)


def contract_last(left, right):
    return lax.dot_general(
        left, right, (((1,), (1,)), ((), ())), preferred_element_type=jnp.float32
    )


def contract_first(left, right):
    return lax.dot_general(
        left, right, (((0,), (0,)), ((), ())), preferred_element_type=jnp.float32
    )


def sum_halves(part):
    return lax.psum(part.astype(jnp.bfloat16), "mp").astype(jnp.float32)


def general_body(
    tokens,
    positions,
    routes,
    cotangent,
    attention_gain,
    query_weight,
    key_weight,
    value_weight,
    query_gain,
    key_gain,
    output_weight,
    ffn_gain,
    router_weight,
    gate_weight,
    up_weight,
    down_weight,
):
    gathered = (
        lax.all_gather(query_weight, ("seq", "ctx"), axis=0, tiled=True),
        lax.all_gather(key_weight, ("seq", "ctx"), axis=0, tiled=True),
        lax.all_gather(value_weight, ("seq", "ctx"), axis=0, tiled=True),
        lax.all_gather(output_weight, ("seq", "ctx"), axis=1, tiled=True),
        lax.all_gather(router_weight, ("seq", "ctx"), axis=0, tiled=True),
        lax.all_gather(attention_gain, ("seq", "ctx"), axis=0, tiled=True),
        lax.all_gather(ffn_gain, ("seq", "ctx"), axis=0, tiled=True),
        lax.all_gather(query_gain, ("seq", "ctx"), axis=1, tiled=True),
        lax.all_gather(key_gain, ("seq", "ctx"), axis=1, tiled=True),
    )
    (
        query_full,
        key_full,
        value_full,
        output_full,
        router_full,
        gain_one_half,
        gain_two_half,
        query_gain_full,
        key_gain_full,
    ) = gathered
    rows = tokens.shape[1]
    width = tokens.shape[2]
    heads_here = query_gain.shape[0]
    local_width = query_weight.shape[1]
    all_columns = HEADS * HEAD_DIM
    factor = HEAD_DIM ** (-0.5)
    flat = tokens[0].astype(jnp.float32)
    grad_top = cotangent[0].astype(jnp.float32)
    gain_one = gain_one_half.astype(jnp.float32)
    gain_two = gain_two_half.astype(jnp.float32)
    query_gain_f = query_gain_full.astype(jnp.float32)
    key_gain_f = key_gain_full.astype(jnp.float32)
    normed_one = rms_scale(flat, gain_one).astype(jnp.bfloat16)
    query_raw = jnp.dot(normed_one, query_full, preferred_element_type=jnp.float32)
    key_raw = jnp.dot(normed_one, key_full, preferred_element_type=jnp.float32)
    value_rows = jnp.dot(normed_one, value_full, preferred_element_type=jnp.float32).astype(
        jnp.bfloat16
    )
    query_sq, key_sq = lax.psum(
        (jnp.sum(query_raw * query_raw, axis=-1), jnp.sum(key_raw * key_raw, axis=-1)), "mp"
    )
    query_inv = lax.rsqrt(query_sq / all_columns + eps)
    key_inv = lax.rsqrt(key_sq / all_columns + eps)
    query_unit = (query_raw * query_inv[:, None]).reshape(rows, heads_here, HEAD_DIM)
    key_unit = (key_raw * key_inv[:, None]).reshape(rows, heads_here, HEAD_DIM)
    cosine, sine = rope_tables(positions[0])
    query_rows = rope_turn(query_unit * query_gain_f, cosine, sine, factor).astype(jnp.bfloat16)
    key_rows = rope_turn(key_unit * key_gain_f, cosine, sine, 1.0).astype(jnp.bfloat16)
    keys_all, values_all = (
        lax.all_gather(key_rows, "ctx", axis=0, tiled=True),
        lax.all_gather(value_rows, "ctx", axis=0, tiled=True),
    )
    ctx_count = lax.axis_size("ctx")
    length = rows * ctx_count
    first_row = lax.axis_index("ctx") * rows
    last_row = first_row + rows - 1
    query_pos = first_row + jnp.arange(rows, dtype=jnp.int32)
    block = min(512, length)
    blocks = length // block
    query3 = query_rows.reshape(rows, heads_here, HEAD_DIM)

    def forward_block(carry, index):
        start = index * block

        def forward_work(state):
            top, total, acc = state
            keys = lax.dynamic_slice_in_dim(keys_all, start, block, 0).reshape(
                block, heads_here, HEAD_DIM
            )
            values = lax.dynamic_slice_in_dim(values_all, start, block, 0).reshape(
                block, heads_here, HEAD_DIM
            )
            scores = jnp.einsum("qhd,khd->hqk", query3, keys, preferred_element_type=jnp.float32)
            allowed = (start + jnp.arange(block, dtype=jnp.int32))[None, :] <= query_pos[:, None]
            scores = jnp.where(allowed[None], scores, neg_big)
            new_top = jnp.maximum(top, jnp.max(scores, axis=-1))
            weights = jnp.where(allowed[None], jnp.exp(scores - new_top[..., None]), 0.0)
            fade = jnp.exp(top - new_top)
            total = total * fade + jnp.sum(weights, axis=-1)
            acc = acc * fade[..., None] + jnp.einsum(
                "hqk,khd->hqd",
                weights.astype(jnp.bfloat16),
                values,
                preferred_element_type=jnp.float32,
            )
            return (new_top, total, acc)

        return (lax.cond(start <= last_row, forward_work, lambda state: state, carry), None)

    start_state = (
        jnp.full((heads_here, rows), neg_big, jnp.float32),
        jnp.zeros((heads_here, rows), jnp.float32),
        jnp.zeros((heads_here, rows, HEAD_DIM), jnp.float32),
    )
    (top, total, acc), _ = lax.scan(forward_block, start_state, jnp.arange(blocks, dtype=jnp.int32))
    mixed = (
        (acc / total[..., None]).transpose(1, 0, 2).reshape(rows, local_width).astype(jnp.bfloat16)
    )
    lse = top + jnp.log(total)
    attn = lax.psum(jnp.dot(mixed, output_full, preferred_element_type=jnp.float32), "mp")
    hidden = flat + attn
    normed_two = rms_scale(hidden, gain_two).astype(jnp.bfloat16)
    logits = jnp.dot(normed_two, router_full, preferred_element_type=jnp.float32)
    probs = jax.nn.softmax(logits, axis=-1)
    route_rows = routes[0]
    experts = router_full.shape[1]
    top_count = route_rows.shape[1]
    choose = (route_rows[:, :, None] == jnp.arange(experts, dtype=jnp.int32)[None, None, :]).astype(
        jnp.float32
    )
    share = jnp.sum(choose * probs[:, None, :], axis=-1)
    assign = rows * top_count
    capacity = assign * 3 // (2 * experts)
    expert_of = route_rows.reshape(assign)
    onehot = (expert_of[:, None] == jnp.arange(experts, dtype=jnp.int32)[None, :]).astype(jnp.int32)
    rank = jnp.sum(onehot * jnp.cumsum(onehot, axis=0), axis=1) - 1
    place = expert_of * capacity + rank
    table = (
        jnp.full((experts * capacity,), assign, jnp.int32)
        .at[place]
        .set(jnp.arange(assign, dtype=jnp.int32))
    )
    valid = table < assign
    safe = jnp.minimum(table, assign - 1)
    outgoing = jnp.where(
        valid[:, None], normed_two[safe // top_count], jnp.zeros((), jnp.bfloat16)
    ).reshape(experts, capacity, width)
    gate_here = gate_weight[0]
    up_here = up_weight[0]
    down_here = down_weight[0]
    received = lax.all_to_all(outgoing, ("seq", "ctx"), split_axis=0, concat_axis=0, tiled=True)
    sources = received.shape[0]
    slots = received.shape[1]
    inputs = received.reshape(sources * slots, width)
    gate = jnp.dot(inputs, gate_here, preferred_element_type=jnp.float32)
    up = jnp.dot(inputs, up_here, preferred_element_type=jnp.float32)
    act = (gate * jax.nn.sigmoid(gate) * up).astype(jnp.bfloat16)
    result = jnp.dot(act, down_here, preferred_element_type=jnp.float32).reshape(
        sources, slots, width
    )
    result = sum_halves(result)
    returned = lax.all_to_all(
        result.astype(jnp.bfloat16), ("seq", "ctx"), split_axis=0, concat_axis=0, tiled=True
    ).astype(result.dtype)
    per_assign = returned.reshape(experts * capacity, width)[place].reshape(rows, top_count, width)
    combined = jnp.sum(share[:, :, None] * per_assign, axis=1)
    layer_output = (hidden + combined).astype(jnp.bfloat16)[None]
    grad_share_part = jnp.sum(per_assign * grad_top[:, None, :], axis=-1)
    grad_result = (
        (share[:, :, None] * grad_top[:, None, :]).astype(jnp.bfloat16).reshape(assign, width)
    )
    grad_slots = jnp.where(valid[:, None], grad_result[safe], jnp.zeros((), jnp.bfloat16)).reshape(
        experts, capacity, width
    )
    incoming_rows, incoming_grads = (
        lax.all_to_all(outgoing, ("seq", "ctx"), split_axis=0, concat_axis=0, tiled=True),
        lax.all_to_all(grad_slots, ("seq", "ctx"), split_axis=0, concat_axis=0, tiled=True),
    )
    sources = incoming_rows.shape[0]
    inputs = incoming_rows.reshape(sources * capacity, width)
    grads_in = incoming_grads.reshape(sources * capacity, width)
    gate = jnp.dot(inputs, gate_here, preferred_element_type=jnp.float32)
    up = jnp.dot(inputs, up_here, preferred_element_type=jnp.float32)
    sig = jax.nn.sigmoid(gate)
    act = (gate * sig * up).astype(jnp.bfloat16)
    grad_act = contract_last(grads_in, down_here)
    down_grad = contract_first(act, grads_in)
    grad_gate = (grad_act * up * sig * (1.0 + gate * (1.0 - sig))).astype(jnp.bfloat16)
    grad_up = (grad_act * gate * sig).astype(jnp.bfloat16)
    gate_grad = contract_first(inputs, grad_gate)
    up_grad = contract_first(inputs, grad_up)
    back = (contract_last(grad_gate, gate_here) + contract_last(grad_up, up_here)).reshape(
        sources, capacity, width
    )
    back_home = lax.all_to_all(
        back.astype(jnp.bfloat16), ("seq", "ctx"), split_axis=0, concat_axis=0, tiled=True
    ).astype(back.dtype)
    moe_part = jnp.sum(
        back_home.reshape(experts * capacity, width)[place].reshape(rows, top_count, width), axis=1
    )
    share_send = jnp.zeros_like(grad_share_part)
    grad_norm_moe, share_summed = lax.psum((moe_part, share_send), "mp")
    grad_share = grad_share_part + share_summed
    grad_prob = jnp.sum(choose * grad_share[:, :, None], axis=1)
    grad_logits = (probs * (grad_prob - jnp.sum(probs * grad_prob, axis=-1, keepdims=True))).astype(
        jnp.bfloat16
    )
    router_grad = contract_first(normed_two, grad_logits)
    grad_normed_two = grad_norm_moe + contract_last(grad_logits, router_full)
    _, pull_two = jax.vjp(rms_scale, hidden, gain_two)
    grad_hidden_part, ffn_gain_grad = pull_two(grad_normed_two)
    grad_hidden = grad_top + grad_hidden_part
    grad_attn = grad_hidden.astype(jnp.bfloat16)
    output_grad = contract_first(mixed, grad_attn)
    grad_mixed = contract_last(grad_attn, output_full).astype(jnp.bfloat16)
    grad3 = grad_mixed.reshape(rows, heads_here, HEAD_DIM)
    delta = jnp.sum(
        grad3.astype(jnp.float32) * mixed.reshape(rows, heads_here, HEAD_DIM).astype(jnp.float32),
        axis=-1,
    ).T

    def backward_block(query_acc, index):
        start = index * block

        def backward_work(acc_now):
            keys = lax.dynamic_slice_in_dim(keys_all, start, block, 0).reshape(
                block, heads_here, HEAD_DIM
            )
            values = lax.dynamic_slice_in_dim(values_all, start, block, 0).reshape(
                block, heads_here, HEAD_DIM
            )
            scores = jnp.einsum("qhd,khd->hqk", query3, keys, preferred_element_type=jnp.float32)
            allowed = (start + jnp.arange(block, dtype=jnp.int32))[None, :] <= query_pos[:, None]
            scores = jnp.where(allowed[None], scores, neg_big)
            prob = jnp.where(allowed[None], jnp.exp(scores - lse[..., None]), 0.0)
            value_part = jnp.einsum(
                "hqk,qhd->khd", prob.astype(jnp.bfloat16), grad3, preferred_element_type=jnp.float32
            )
            grad_prob_block = jnp.einsum(
                "qhd,khd->hqk", grad3, values, preferred_element_type=jnp.float32
            )
            grad_scores = (prob * (grad_prob_block - delta[..., None])).astype(jnp.bfloat16)
            acc_now = acc_now + jnp.einsum(
                "hqk,khd->hqd", grad_scores, keys, preferred_element_type=jnp.float32
            )
            key_part = jnp.einsum(
                "hqk,qhd->khd", grad_scores, query3, preferred_element_type=jnp.float32
            )
            return (
                acc_now,
                key_part.reshape(block, local_width),
                value_part.reshape(block, local_width),
            )

        def skip(acc_now):
            empty = jnp.zeros((block, local_width), jnp.float32)
            return (acc_now, empty, empty)

        acc_next, key_part, value_part = lax.cond(start <= last_row, backward_work, skip, query_acc)
        return (acc_next, (key_part, value_part))

    query_acc, (key_blocks, value_blocks) = lax.scan(
        backward_block,
        jnp.zeros((heads_here, rows, HEAD_DIM), jnp.float32),
        jnp.arange(blocks, dtype=jnp.int32),
    )
    grad_keys, grad_values = (
        lax.psum_scatter(
            key_blocks.reshape(length, local_width).astype(jnp.bfloat16),
            "ctx",
            scatter_dimension=0,
            tiled=True,
        ).astype(jnp.float32),
        lax.psum_scatter(
            value_blocks.reshape(length, local_width).astype(jnp.bfloat16),
            "ctx",
            scatter_dimension=0,
            tiled=True,
        ).astype(jnp.float32),
    )
    grad_queries = query_acc.transpose(1, 0, 2).reshape(rows, local_width)
    _, pull_query = jax.vjp(
        lambda normed: rope_turn(normed, cosine, sine, factor), query_unit * query_gain_f
    )
    (grad_query_normed,) = pull_query(grad_queries)
    _, pull_key = jax.vjp(
        lambda normed: rope_turn(normed, cosine, sine, 1.0), key_unit * key_gain_f
    )
    (grad_key_normed,) = pull_key(grad_keys)
    query_gain_grad = jnp.sum(grad_query_normed * query_unit, axis=0)
    key_gain_grad = jnp.sum(grad_key_normed * key_unit, axis=0)
    query_scaled = (grad_query_normed * query_gain_f).reshape(rows, local_width)
    key_scaled = (grad_key_normed * key_gain_f).reshape(rows, local_width)
    query_dot, key_dot = lax.psum(
        (jnp.sum(query_raw * query_scaled, axis=-1), jnp.sum(key_raw * key_scaled, axis=-1)), "mp"
    )
    grad_query_raw = (
        query_inv[:, None] * query_scaled
        - query_raw * (query_inv * query_inv * query_inv * query_dot / all_columns)[:, None]
    )
    grad_key_raw = (
        key_inv[:, None] * key_scaled
        - key_raw * (key_inv * key_inv * key_inv * key_dot / all_columns)[:, None]
    )
    query_half = grad_query_raw.astype(jnp.bfloat16)
    key_half = grad_key_raw.astype(jnp.bfloat16)
    value_half = grad_values.astype(jnp.bfloat16)
    query_grad = contract_first(normed_one, query_half)
    key_grad = contract_first(normed_one, key_half)
    value_grad = contract_first(normed_one, value_half)
    normed_part = (
        contract_last(query_half, query_full)
        + contract_last(key_half, key_full)
        + contract_last(value_half, value_full)
    )
    grad_normed_one = lax.psum(normed_part.astype(jnp.bfloat16), "mp").astype(jnp.float32)
    _, pull_one = jax.vjp(rms_scale, flat, gain_one)
    grad_flat_part, attention_gain_grad = pull_one(grad_normed_one)
    tokens_grad = (grad_hidden + grad_flat_part)[None]
    owned = (
        lax.psum_scatter(query_grad, ("seq", "ctx"), scatter_dimension=0, tiled=True),
        lax.psum_scatter(key_grad, ("seq", "ctx"), scatter_dimension=0, tiled=True),
        lax.psum_scatter(value_grad, ("seq", "ctx"), scatter_dimension=0, tiled=True),
        lax.psum_scatter(output_grad, ("seq", "ctx"), scatter_dimension=1, tiled=True),
        lax.psum_scatter(router_grad, ("seq", "ctx"), scatter_dimension=0, tiled=True),
        lax.psum_scatter(attention_gain_grad, ("seq", "ctx"), scatter_dimension=0, tiled=True),
        lax.psum_scatter(ffn_gain_grad, ("seq", "ctx"), scatter_dimension=0, tiled=True),
        lax.psum_scatter(query_gain_grad, ("seq", "ctx"), scatter_dimension=1, tiled=True),
        lax.psum_scatter(key_gain_grad, ("seq", "ctx"), scatter_dimension=1, tiled=True),
    )
    (
        query_owned,
        key_owned,
        value_owned,
        output_owned,
        router_owned,
        gain_one_owned,
        gain_two_owned,
        query_gain_owned,
        key_gain_owned,
    ) = owned
    return (
        layer_output,
        tokens_grad,
        gain_one_owned,
        query_owned,
        key_owned,
        value_owned,
        query_gain_owned,
        key_gain_owned,
        output_owned,
        gain_two_owned,
        router_owned,
        gate_grad[None],
        up_grad[None],
        down_grad[None],
    )


def fast_body(
    tokens, positions, routes, cotangent, attention_gain, query_weight, key_weight, value_weight,
    query_gain, key_gain, output_weight, ffn_gain, router_weight, gate_weight, up_weight,
    down_weight,
):
    s, z, m = place()
    c = s * 4 + z
    rows, width = tokens.shape[1:]
    cut = width // 2
    half = np.arange(HEAD_DIM // 2).astype(np.float32)
    freq = np.float32(10000.0) ** (-(half * np.float32(2.0) / np.float32(HEAD_DIM)))
    freq = jnp.asarray(np.tile(freq, (8, 2)), F32)
    (normed, out_full, all_top, weights3, info, raw, rows3, squares, mixed, lse, trig, _, hidden,
     normed_two, probs, chosen, share, head_gains, gains) = front(
        0, tokens[0], attention_gain.reshape(1, rows), ffn_gain.reshape(1, rows), positions,
        router_weight.T, query_gain, key_gain, routes[0], query_weight, key_weight, value_weight,
        output_weight, cotangent[0], freq)
    grad_two, prob_out, moe, gate_grad, up_grad, down_grad = experts(
        5, normed_two, share, all_top, gate_weight[0], up_weight[0], down_weight[0])
    _, moe_sum, query_grad, key_grad, value_grad, output_grad, tokens_grad, tail = rear(
        6, grad_two, prob_out, probs, chosen, normed_two, hidden, cotangent[0], info,
        mixed.reshape(8 * rows, HEAD_DIM), rows3, raw, squares, lse, trig, head_gains, weights3,
        tokens[0], gains, out_full, normed, moe)
    layer_output = (hidden + moe_sum.astype(F32)).astype(BF)
    summed = jnp.sum(tail[0], axis=0)
    gain_grads = lax.dynamic_slice_in_dim(tail[0] + tail[1], m * 8, 8, 0)
    gain_grads = lax.dynamic_slice_in_dim(gain_grads, c * 8, 8, 2)
    return (
        layer_output[None],
        tokens_grad[None],
        summed[0],
        query_grad,
        key_grad,
        value_grad,
        gain_grads[:, 2],
        gain_grads[:, 19],
        output_grad.reshape(cut, HEAD_DIM).astype(F32),
        summed[1],
        summed[3:19].T,
        gate_grad[None],
        up_grad[None],
        down_grad[None],
    )


def grid_fits(tokens, router_weight):
    sizes = tuple(lax.axis_size(name) for name in ("seq", "ctx", "mp"))
    return sizes == (4, 4, 2) and tokens.shape == (1, 128, 2048) and router_weight.shape == (128, 16)


def body(*args):
    if grid_fits(args[0], args[12]):
        return fast_body(*args)
    return general_body(*args)


def solution(mesh):
    placed = (
        P("seq", "ctx", None),
        P("seq", "ctx"),
        P("seq", "ctx", None),
        P("seq", "ctx", None),
        P(("seq", "ctx")),
        P(("seq", "ctx"), "mp"),
        P(("seq", "ctx"), "mp"),
        P(("seq", "ctx"), "mp"),
        P("mp", ("seq", "ctx")),
        P("mp", ("seq", "ctx")),
        P("mp", ("seq", "ctx")),
        P(("seq", "ctx")),
        P(("seq", "ctx"), None),
        P(("seq", "ctx"), None, "mp"),
        P(("seq", "ctx"), None, "mp"),
        P(("seq", "ctx"), "mp", None),
    )
    return jax.shard_map(
        body,
        mesh=mesh,
        in_specs=placed,
        out_specs=(
            P("seq", "ctx", None),
            P("seq", "ctx", None),
            P(("seq", "ctx")),
            P(("seq", "ctx"), "mp"),
            P(("seq", "ctx"), "mp"),
            P(("seq", "ctx"), "mp"),
            P("mp", ("seq", "ctx")),
            P("mp", ("seq", "ctx")),
            P("mp", ("seq", "ctx")),
            P(("seq", "ctx")),
            P(("seq", "ctx"), None),
            P(("seq", "ctx"), None, "mp"),
            P(("seq", "ctx"), None, "mp"),
            P(("seq", "ctx"), "mp", None),
        ),
        check_vma=False,
    )
```
